128 devices in a mesh: dp: 1, wy: 16 (over z, y), wx: 8 (over x, core).
Axes of the slice: x: 4, y: 4, z: 4, core: 2. Of those that a mesh axis runs over, the one named last changes fastest.
Arguments:
- x_tokens: bfloat16 [128, 256, 2048], P(('dp', 'wy', 'wx'))
- gamma_ln: float32 [2, 2048], replicated
- w_q: bfloat16 [2, 2048, 2048], P(None, 'wx', 'wy')
- w_kv: bfloat16 [2, 2048, 2, 128], P(None, 'wx')
- w_gu: bfloat16 [2, 2048, 2, 8192], P(None, 'wx', None, 'wy')
- w_o: bfloat16 [2, 2048, 2048], P(None, 'wy', 'wx')
- w_d: bfloat16 [2, 8192, 2048], P(None, 'wy', 'wx')
Outputs:
- output 1: bfloat16 [128, 256, 2048], P(('dp', 'wy', 'wx'))
- output 2: bfloat16 [2, 128, 256, 128], P(None, ('dp', 'wy', 'wx'))
- output 3: bfloat16 [2, 128, 256, 128], P(None, ('dp', 'wy', 'wx'))
All inputs are finite; a program needn't handle non-finite values.
Results may differ from the reference program's by a relative error of at most 0.0150521.
Values are sent between devices in bfloat16 or wider.
A program may use at most 1 GiB of HBM per device.

```python
import jax
import jax.numpy as jnp
from jax import lax

D_MODEL = 2048
NUM_HEADS = 16
HEAD_DIM = 128
D_FF = 8192
SEQ_LEN = 256
BATCH_SEQS = 128
N_LAYERS = 2
LN_EPS = 1e-6
ROPE_BASE = 10000.0
Q_WIDTH = NUM_HEADS * HEAD_DIM


def setup_inputs(seed: int = 0, part: int = 0) -> dict:
    base_key = jax.random.key(seed)
    keys_all = jax.random.split(base_key, 7)
    x_key = jax.random.fold_in(keys_all[0], part)
    x_tokens = jax.random.normal(x_key, (BATCH_SEQS, SEQ_LEN, D_MODEL), jnp.float32).astype(jnp.bfloat16)
    gamma_ln = 1.0 + 0.5 * jax.random.normal(keys_all[1], (N_LAYERS, D_MODEL), jnp.float32)
    w_q = (2.5 * D_MODEL ** -0.5) * jax.random.normal(keys_all[2], (N_LAYERS, D_MODEL, Q_WIDTH), jnp.float32)
    w_kv = D_MODEL ** -0.5 * jax.random.normal(keys_all[3], (N_LAYERS, D_MODEL, 2, HEAD_DIM), jnp.float32)
    w_gu = D_MODEL ** -0.5 * jax.random.normal(keys_all[4], (N_LAYERS, D_MODEL, 2, D_FF), jnp.float32)
    w_o = Q_WIDTH ** -0.5 * jax.random.normal(keys_all[5], (N_LAYERS, Q_WIDTH, D_MODEL), jnp.float32)
    w_d = D_FF ** -0.5 * jax.random.normal(keys_all[6], (N_LAYERS, D_FF, D_MODEL), jnp.float32)
    return {'x_tokens': x_tokens, 'gamma_ln': gamma_ln, 'w_q': w_q.astype(jnp.bfloat16), 'w_kv': w_kv.astype(jnp.bfloat16), 'w_gu': w_gu.astype(jnp.bfloat16), 'w_o': w_o.astype(jnp.bfloat16), 'w_d': w_d.astype(jnp.bfloat16)}


def rope_tables():
    half_dim = HEAD_DIM // 2
    inv_freq = ROPE_BASE ** (-2.0 * jnp.arange(half_dim, dtype=jnp.float32) / HEAD_DIM)
    angles = jnp.arange(SEQ_LEN, dtype=jnp.float32)[:, None] * inv_freq[None, :]
    return jnp.cos(angles), jnp.sin(angles)


def rotate(values_in, cos_tab, sin_tab):
    half_dim = HEAD_DIM // 2
    first_half = values_in[..., :half_dim]
    second_half = values_in[..., half_dim:]
    return jnp.concatenate([first_half * cos_tab - second_half * sin_tab, second_half * cos_tab + first_half * sin_tab], axis=-1)


def one_prompt(prompt, gamma_ln, w_q, w_kv, w_gu, w_o, w_d):
    cos_tab, sin_tab = rope_tables()
    allowed = jnp.arange(SEQ_LEN)[:, None] >= jnp.arange(SEQ_LEN)[None, :]

    def layer_step(resid, layer_weights):
        g_scale, wq_l, wkv_l, wgu_l, wo_l, wd_l = layer_weights
        resid_f = resid.astype(jnp.float32)
        centered = resid_f - jnp.mean(resid_f, axis=-1, keepdims=True)
        variance = jnp.mean(centered * centered, axis=-1, keepdims=True)
        normed = (centered * lax.rsqrt(variance + LN_EPS) * g_scale).astype(jnp.bfloat16)
        q_proj = jnp.dot(normed, wq_l, preferred_element_type=jnp.float32).astype(jnp.bfloat16)
        kv_proj = jnp.dot(normed, wkv_l.reshape(D_MODEL, 2 * HEAD_DIM), preferred_element_type=jnp.float32).astype(jnp.bfloat16)
        gu_proj = jnp.dot(normed, wgu_l.reshape(D_MODEL, 2 * D_FF), preferred_element_type=jnp.float32).astype(jnp.bfloat16)
        q_rot = rotate(q_proj.astype(jnp.float32).reshape(SEQ_LEN, NUM_HEADS, HEAD_DIM), cos_tab[:, None, :], sin_tab[:, None, :]).astype(jnp.bfloat16)
        k_rot = rotate(kv_proj[:, :HEAD_DIM].astype(jnp.float32), cos_tab, sin_tab).astype(jnp.bfloat16)
        v_val = kv_proj[:, HEAD_DIM:]
        scores = jnp.einsum('she,te->hst', q_rot.astype(jnp.float32), k_rot.astype(jnp.float32)) * HEAD_DIM ** -0.5
        scores = jnp.where(allowed[None, :, :], scores, -jnp.inf)
        attn_probs = jax.nn.softmax(scores, axis=-1).astype(jnp.bfloat16)
        attended = jnp.einsum('hst,te->she', attn_probs.astype(jnp.float32), v_val.astype(jnp.float32)).astype(jnp.bfloat16)
        hidden = (jax.nn.silu(gu_proj[:, :D_FF].astype(jnp.float32)) * gu_proj[:, D_FF:].astype(jnp.float32)).astype(jnp.bfloat16)
        mixed = jnp.dot(attended.reshape(SEQ_LEN, Q_WIDTH), wo_l, preferred_element_type=jnp.float32) + jnp.dot(hidden, wd_l, preferred_element_type=jnp.float32)
        return (resid_f + mixed).astype(jnp.bfloat16), (k_rot, v_val)

    y_seq, caches = lax.scan(layer_step, prompt, (gamma_ln, w_q, w_kv, w_gu, w_o, w_d))
    return y_seq, caches[0], caches[1]


def reference(x_tokens, gamma_ln, w_q, w_kv, w_gu, w_o, w_d):
    def per_prompt(prompt):
        return one_prompt(prompt, gamma_ln, w_q, w_kv, w_gu, w_o, w_d)
    y_out, k_all, v_all = lax.map(per_prompt, x_tokens)
    return y_out, jnp.swapaxes(k_all, 0, 1), jnp.swapaxes(v_all, 0, 1)
```

```python
import jax
import jax.numpy as jnp
from jax import lax
from jax.sharding import PartitionSpec as P

LN_EPS = 1e-6
ROPE_BASE = 10000.0


def rope_tables(seq_len, head_dim):
    half_dim = head_dim // 2
    inv_freq = ROPE_BASE ** (-2.0 * jnp.arange(half_dim, dtype=jnp.float32) / head_dim)
    angles = jnp.arange(seq_len, dtype=jnp.float32)[:, None] * inv_freq[None, :]
    return jnp.cos(angles), jnp.sin(angles)


def rotate(values_in, cos_tab, sin_tab):
    half_dim = values_in.shape[-1] // 2
    first_half = values_in[..., :half_dim].astype(jnp.float32)
    second_half = values_in[..., half_dim:].astype(jnp.float32)
    rotated = jnp.concatenate([first_half * cos_tab - second_half * sin_tab, second_half * cos_tab + first_half * sin_tab], axis=-1)
    return rotated.astype(jnp.bfloat16)


def layer_norm(resid, g_scale):
    resid_f = resid.astype(jnp.float32)
    centered = resid_f - jnp.mean(resid_f, axis=-1, keepdims=True)
    variance = jnp.mean(centered * centered, axis=-1, keepdims=True)
    return (centered * lax.rsqrt(variance + LN_EPS) * g_scale).astype(jnp.bfloat16)


def causal_attention(q_rot, k_rot, v_val):
    seq_len = q_rot.shape[1]
    score_scale = q_rot.shape[-1] ** -0.5
    scores = jnp.einsum('bshe,bte->bhst', q_rot, k_rot, preferred_element_type=jnp.float32) * score_scale
    allowed = jnp.arange(seq_len)[:, None] >= jnp.arange(seq_len)[None, :]
    scores = jnp.where(allowed, scores, -jnp.inf)
    attn_probs = jax.nn.softmax(scores, axis=-1).astype(jnp.bfloat16)
    attended = jnp.einsum('bhst,bte->bshe', attn_probs, v_val, preferred_element_type=jnp.float32)
    return attended.astype(jnp.bfloat16)


def solution(mesh):
    batch_axes = ('dp', 'wy', 'wx')
    in_specs = (P(batch_axes), P(), P(None, 'wx', 'wy'), P(None, 'wx'), P(None, 'wx', None, 'wy'), P(None, 'wy', 'wx'), P(None, 'wy', 'wx'))
    out_specs = (P(batch_axes), P(None, batch_axes), P(None, batch_axes))
    n_wy, n_wx = mesh.shape['wy'], mesh.shape['wx']
    per = n_wy // n_wx
    perm = []
    for iy in range(n_wy):
        for ix in range(n_wx):
            perm.append((iy * n_wx + ix, ((iy % per) * n_wx + ix) * n_wx + iy // per))

    def device_step(x_tokens, gamma_ln, w_q, w_kv, w_gu, w_o, w_d):
        seq_len, d_model = x_tokens.shape[1], x_tokens.shape[2]
        head_dim = w_kv.shape[-1]
        d_loc = w_q.shape[1]
        f_loc = w_gu.shape[-1]
        n_layers = w_q.shape[0]
        cos_tab, sin_tab = rope_tables(seq_len, head_dim)
        iy = lax.axis_index('wy')
        ix = lax.axis_index('wx')
        weights_a, weights_b = [], []
        for layer_idx in range(n_layers):
            kv_half = lax.dynamic_index_in_dim(w_kv[layer_idx], lax.rem(iy, per), axis=1, keepdims=False)
            pack_a = jnp.concatenate([w_gu[layer_idx].reshape(d_loc, 2 * f_loc), w_q[layer_idx], kv_half], axis=1)
            pack_b = jnp.concatenate([w_d[layer_idx], w_o[layer_idx]], axis=0)
            pack_a = lax.ppermute(pack_a, ('wy', 'wx'), perm)
            pack_b = lax.ppermute(pack_b, ('wy', 'wx'), perm)
            full_a = lax.all_gather(pack_a, 'wy', axis=0, tiled=True)
            full_b = lax.all_gather(pack_b, 'wy', axis=0, tiled=True)
            weights_a.append(full_a.reshape(per, d_model, 2 * f_loc + 2 * head_dim))
            weights_b.append(full_b.reshape(per, n_wx, f_loc + head_dim, d_loc))
        resid = x_tokens[0]
        key_list = []
        value_list = []
        for layer_idx in range(n_layers):
            wa, wb = weights_a[layer_idx], weights_b[layer_idx]
            normed = layer_norm(resid, gamma_ln[layer_idx])
            h_all = lax.all_gather(normed, 'wx', axis=0, tiled=True)
            proj = [jnp.dot(h_all, wa[hh], preferred_element_type=jnp.float32).astype(jnp.bfloat16) for hh in range(per)]
            q_all = jnp.stack([p[:, 2 * f_loc:2 * f_loc + head_dim] for p in proj], axis=1).reshape(n_wx, seq_len, per, head_dim)
            k_all = proj[0][:, 2 * f_loc + head_dim:].reshape(n_wx, seq_len, head_dim)
            v_all = proj[1][:, 2 * f_loc + head_dim:].reshape(n_wx, seq_len, head_dim)
            q_rot = rotate(q_all, cos_tab[:, None, :], sin_tab[:, None, :])
            k_rot = rotate(k_all, cos_tab, sin_tab)
            attended = causal_attention(q_rot, k_rot, v_all)
            total = None
            for hh in range(per):
                g_f = proj[hh][:, :f_loc].astype(jnp.float32)
                u_f = proj[hh][:, f_loc:2 * f_loc].astype(jnp.float32)
                hidden = (jax.nn.silu(g_f) * u_f).astype(jnp.bfloat16)
                lhs = jnp.concatenate([hidden, attended[:, :, hh].reshape(n_wx * seq_len, head_dim)], axis=1)
                rhs = jnp.transpose(wb[hh], (1, 0, 2)).reshape(f_loc + head_dim, d_model)
                part = jnp.dot(lhs, rhs, preferred_element_type=jnp.float32)
                total = part if total is None else total + part
            mixed = lax.psum_scatter(total, 'wx', scatter_dimension=0, tiled=True)
            resid = (resid.astype(jnp.float32) + mixed).astype(jnp.bfloat16)
            key_list.append(lax.dynamic_index_in_dim(k_rot, ix, axis=0, keepdims=True))
            value_list.append(lax.dynamic_index_in_dim(v_all, ix, axis=0, keepdims=True))
        return resid[None], jnp.stack(key_list), jnp.stack(value_list)

    return jax.shard_map(device_step, mesh=mesh, in_specs=in_specs, out_specs=out_specs, check_vma=False)
```

```python
import functools

import jax
import jax.numpy as jnp
from jax import lax
from jax.experimental import pallas as pl
from jax.experimental.pallas import tpu as pltpu
from jax.sharding import PartitionSpec as P

LN_EPS = 1e-6
ROPE_BASE = 10000.0
MESH = pl.DeviceIdType.MESH
VMEM_LIMIT = 60 * 1024 * 1024


def rope_tables(seq_len, head_dim):
    half_dim = head_dim // 2
    inv_freq = ROPE_BASE ** (-2.0 * jnp.arange(half_dim, dtype=jnp.float32) / head_dim)
    angles = jnp.arange(seq_len, dtype=jnp.float32)[:, None] * inv_freq[None, :]
    cos, sin = jnp.cos(angles), jnp.sin(angles)
    return jnp.concatenate([cos, cos], axis=1), jnp.concatenate([-sin, sin], axis=1)


def layer_norm(resid, g_scale):
    resid_f = resid.astype(jnp.float32)
    centered = resid_f - jnp.mean(resid_f, axis=-1, keepdims=True)
    variance = jnp.mean(centered * centered, axis=-1, keepdims=True)
    return (centered * lax.rsqrt(variance + LN_EPS) * g_scale).astype(jnp.bfloat16)


def ring_ids(n_wx):
    me = lax.axis_index('wx')
    chip, core = lax.div(me, 2), lax.rem(me, 2)
    n_chip = n_wx // 2

    def at(step, other=0):
        return lax.rem(chip + step, n_chip) * 2 + (lax.rem(core + other, 2))

    return me, chip, core, at


def entry_barrier(peers):
    barrier = pltpu.get_barrier_semaphore()
    for peer in peers:
        pl.semaphore_signal(barrier, inc=1, device_id={'wx': peer}, device_id_type=MESH)
    pl.semaphore_wait(barrier, len(peers))


def gather_copies(n_wx, hall, send_sem, recv_sem):
    me, chip, core, at = ring_ids(n_wx)
    half = hall.shape[1] // 2
    right, left, partner = at(1), at(3), at(0, 1)
    top, bottom, whole = pl.ds(0, half), pl.ds(half, half), pl.ds(0, 2 * half)

    def copy(num, block, rows, target):
        ref = hall.at[block, rows]
        return pltpu.make_async_remote_copy(
            src_ref=ref, dst_ref=ref, send_sem=send_sem.at[num], recv_sem=recv_sem.at[num],
            device_id={'wx': target}, device_id_type=MESH)

    return [
        copy(0, me, whole, partner),
        copy(1, me, top, right), copy(2, me, bottom, left),
        copy(3, me, bottom, right), copy(4, me, top, left),
        copy(5, left, top, right), copy(6, right, bottom, left),
        copy(7, left, whole, partner), copy(8, right, whole, partner),
        copy(9, at(2), top, partner), copy(10, at(2), bottom, partner),
    ]


def arrivals(n_wx, hall, send_sem, recv_sem):
    me, chip, core, at = ring_ids(n_wx)
    half = hall.shape[1] // 2
    top, bottom, whole = pl.ds(0, half), pl.ds(half, half), pl.ds(0, 2 * half)

    def copy(num, block, rows):
        ref = hall.at[block, rows]
        return pltpu.make_async_remote_copy(
            src_ref=ref, dst_ref=ref, send_sem=send_sem.at[num], recv_sem=recv_sem.at[num],
            device_id={'wx': at(0, 1)}, device_id_type=MESH)

    return [
        copy(0, at(0, 1), whole),
        copy(1, at(3), top), copy(2, at(1), bottom), copy(3, at(3), bottom), copy(4, at(1), top),
        copy(5, at(2), top), copy(6, at(2), bottom),
        copy(7, at(3, 1), whole), copy(8, at(1, 1), whole),
        copy(9, at(2, 1), top), copy(10, at(2, 1), bottom),
    ]


def gather_kernel(n_wx, h_ref, out_ref, hall, send_sem, recv_sem, local_sem, out_sem):
    me, chip, core, at = ring_ids(n_wx)
    load = pltpu.make_async_copy(h_ref, hall.at[me], local_sem)
    load.start()
    entry_barrier([at(1), at(3), at(0, 1)])
    sends = gather_copies(n_wx, hall, send_sem, recv_sem)
    lands = arrivals(n_wx, hall, send_sem, recv_sem)
    outs = []

    def put(block):
        out = pltpu.make_async_copy(hall.at[block], out_ref.at[block], out_sem.at[len(outs)])
        out.start()
        outs.append(out)

    load.wait()
    for num in range(5):
        sends[num].start()
    put(me)
    lands[0].wait_recv()
    put(at(0, 1))
    lands[1].wait_recv()
    sends[5].start()
    lands[2].wait_recv()
    sends[6].start()
    lands[3].wait_recv()
    sends[7].start()
    put(at(3))
    lands[4].wait_recv()
    sends[8].start()
    put(at(1))
    lands[7].wait_recv()
    put(at(3, 1))
    lands[8].wait_recv()
    put(at(1, 1))
    lands[5].wait_recv()
    sends[9].start()
    lands[6].wait_recv()
    sends[10].start()
    put(at(2))
    lands[9].wait_recv()
    lands[10].wait_recv()
    put(at(2, 1))
    for num in range(11):
        sends[num].wait_send()
    for out in outs:
        out.wait()


def gather_h(h, n_wx):
    seq, d_model = h.shape
    return pl.pallas_call(
        functools.partial(gather_kernel, n_wx),
        out_shape=jax.ShapeDtypeStruct((n_wx, seq, d_model), h.dtype),
        in_specs=[pl.BlockSpec(memory_space=pl.ANY)],
        out_specs=pl.BlockSpec(memory_space=pl.ANY),
        scratch_shapes=[
            pltpu.VMEM((n_wx, seq, d_model), h.dtype),
            pltpu.SemaphoreType.DMA((11,)), pltpu.SemaphoreType.DMA((11,)),
            pltpu.SemaphoreType.DMA, pltpu.SemaphoreType.DMA((n_wx,)),
        ],
        compiler_params=pltpu.CompilerParams(collective_id=0, has_side_effects=True, vmem_limit_bytes=VMEM_LIMIT),
        cost_estimate=pl.CostEstimate(flops=20_000_000_000, bytes_accessed=16 * 2**20, transcendentals=0),
        name='gather_h',
    )(h)


def up_step(hall, wa, mo, kv_out, xt, cos, sin, f_loc, head_dim):
    seq, d_model = hall.shape[1], hall.shape[2]
    rows = pl.ds(pl.multiple_of(xt * 2 * seq, 2 * seq), 2 * seq)
    h = hall[pl.ds(xt * 2, 2)].reshape(2 * seq, d_model)
    width = f_loc + head_dim
    narrow = []
    for hh in range(2):
        qkv = jnp.dot(h, wa[hh, :, 2 * f_loc:], preferred_element_type=jnp.float32)
        narrow.append(qkv.astype(jnp.bfloat16))
    for hh in range(2):
        g_f = jnp.dot(h, wa[hh, :, :f_loc], preferred_element_type=jnp.float32).astype(jnp.bfloat16).astype(jnp.float32)
        u_f = jnp.dot(h, wa[hh, :, f_loc:2 * f_loc], preferred_element_type=jnp.float32).astype(jnp.bfloat16).astype(jnp.float32)
        hidden = g_f * (1.0 / (1.0 + jnp.exp(-g_f))) * u_f
        mo[rows, hh * width:hh * width + f_loc] = hidden.astype(jnp.bfloat16)

    def rot(val):
        val_f = val.astype(jnp.float32)
        return (val_f * cos + pltpu.roll(val_f, head_dim // 2, 1) * sin).astype(jnp.bfloat16)

    allowed = lax.broadcasted_iota(jnp.int32, (seq, seq), 0) >= lax.broadcasted_iota(jnp.int32, (seq, seq), 1)
    for b in range(2):
        part = slice(b * seq, (b + 1) * seq)
        k_rot = rot(narrow[0][part, head_dim:])
        v_val = narrow[1][part, head_dim:]
        kv_out[b, 0] = k_rot
        kv_out[b, 1] = v_val
        for hh in range(2):
            q_rot = rot(narrow[hh][part, :head_dim])
            scores = lax.dot_general(q_rot, k_rot, (((1,), (1,)), ((), ())), preferred_element_type=jnp.float32) * head_dim ** -0.5
            scores = jnp.where(allowed, scores, -jnp.inf)
            top = jnp.max(scores, axis=-1, keepdims=True)
            expd = jnp.exp(scores - top)
            probs = (expd / jnp.sum(expd, axis=-1, keepdims=True)).astype(jnp.bfloat16)
            att = jnp.dot(probs, v_val, preferred_element_type=jnp.float32)
            mo[pl.ds(pl.multiple_of(xt * 2 * seq, 2 * seq) + b * seq, seq), hh * width + f_loc:(hh + 1) * width] = att.astype(jnp.bfloat16)


def up_kernel(n_wx, f_loc, head_dim, hall_ref, wa_ref, cos_ref, sin_ref, mo_ref, k_ref, v_ref, hall, wa, mo, kv, h_sem, w_sem, out_sem, kv_sem):
    me, chip, core, at = ring_ids(n_wx)
    n_chip = n_wx // 2
    seq = hall.shape[1]
    w_loads = [pltpu.make_async_copy(wa_ref.at[hh], wa.at[hh], w_sem.at[hh]) for hh in range(2)]

    def h_load(xt):
        return pltpu.make_async_copy(hall_ref.at[pl.ds(xt * 2, 2)], hall.at[pl.ds(xt * 2, 2)], h_sem.at[xt])

    def out_copy(xt):
        rows = pl.ds(pl.multiple_of(xt * 2 * seq, 2 * seq), 2 * seq)
        return pltpu.make_async_copy(mo.at[rows], mo_ref.at[rows], out_sem.at[xt])

    h_load(0).start()
    for load in w_loads:
        load.start()
    for xt in range(1, n_chip):
        h_load(xt).start()
    for load in w_loads:
        load.wait()

    def body(xt, carry):
        h_load(xt).wait()
        up_step(hall, wa, mo, kv.at[xt], xt, cos_ref[...], sin_ref[...], f_loc, head_dim)
        out_copy(xt).start()
        return carry

    lax.fori_loop(0, n_chip, body, 0)
    k_copy = pltpu.make_async_copy(kv.at[chip, core, 0], k_ref, kv_sem.at[0])
    v_copy = pltpu.make_async_copy(kv.at[chip, core, 1], v_ref, kv_sem.at[1])
    k_copy.start()
    v_copy.start()
    for xt in range(n_chip):
        out_copy(xt).wait()
    k_copy.wait()
    v_copy.wait()


def up_project(h_all, wa, cos, sin, f_loc, head_dim):
    n_wx, seq, d_model = h_all.shape
    n_chip = n_wx // 2
    width = 2 * (f_loc + head_dim)
    return pl.pallas_call(
        functools.partial(up_kernel, n_wx, f_loc, head_dim),
        out_shape=(
            jax.ShapeDtypeStruct((n_wx * seq, width), jnp.bfloat16),
            jax.ShapeDtypeStruct((seq, head_dim), jnp.bfloat16),
            jax.ShapeDtypeStruct((seq, head_dim), jnp.bfloat16),
        ),
        in_specs=[pl.BlockSpec(memory_space=pl.ANY), pl.BlockSpec(memory_space=pl.ANY),
                  pl.BlockSpec(memory_space=pltpu.VMEM), pl.BlockSpec(memory_space=pltpu.VMEM)],
        out_specs=[pl.BlockSpec(memory_space=pl.ANY)] * 3,
        scratch_shapes=[
            pltpu.VMEM((n_wx, seq, d_model), jnp.bfloat16),
            pltpu.VMEM(wa.shape, jnp.bfloat16),
            pltpu.VMEM((n_wx * seq, width), jnp.bfloat16),
            pltpu.VMEM((n_chip, 2, 2, seq, head_dim), jnp.bfloat16),
            pltpu.SemaphoreType.DMA((n_chip,)), pltpu.SemaphoreType.DMA((2,)),
            pltpu.SemaphoreType.DMA((n_chip,)), pltpu.SemaphoreType.DMA((2,)),
        ],
        compiler_params=pltpu.CompilerParams(vmem_limit_bytes=VMEM_LIMIT),
        cost_estimate=pl.CostEstimate(flops=22_000_000_000, bytes_accessed=24 * 2**20, transcendentals=0),
        name='up_project',
    )(h_all, wa, cos, sin)


N_COL = 4


def down_kernel(n_wx, mo_ref, wb_ref, resid_ref, out_ref, mo, wb, given, taken, acc, landed,
                mo_sem, wb_sem, pair_send, pair_recv, ring_send, ring_recv):
    me, chip, core, at = ring_ids(n_wx)
    n_chip = n_wx // 2
    right, left, partner = at(1), at(3), at(0, 1)
    seq = resid_ref.shape[0]
    n_hh, n_w, k_loc, col_w = wb_ref.shape
    col = wb.shape[1] // N_COL

    def step_of(i):
        phase, j = lax.div(i, 4), lax.rem(i, 4)
        odd, slot = lax.rem(j, 2), lax.div(j, 2)
        off = jnp.where(phase == 0, 2, jnp.where(phase == 3, 0, 1 + 2 * odd))
        q = jnp.where(phase == 3, j, jnp.where(phase == 1, (1 - odd) * 2 + slot, odd * 2 + slot))
        return lax.rem(chip + off, n_chip), q, odd

    def mo_load(off):
        rows = pl.ds(pl.multiple_of(lax.rem(chip + off, n_chip) * 2 * seq, 2 * seq), 2 * seq)
        return pltpu.make_async_copy(mo_ref.at[rows], mo.at[rows], mo_sem.at[off])

    def wb_load(hh, w):
        return pltpu.make_async_copy(
            wb_ref.at[hh, w], wb.at[pl.ds(hh * k_loc, k_loc), pl.ds(w * col_w, col_w)], wb_sem.at[hh * n_w + w])

    def pair_copy(i):
        return pltpu.make_async_remote_copy(
            src_ref=given.at[i], dst_ref=taken.at[i], send_sem=pair_send.at[i], recv_sem=pair_recv.at[i],
            device_id={'wx': partner}, device_id_type=MESH)

    def ring_copy(k, odd):
        return pltpu.make_async_remote_copy(
            src_ref=acc.at[k], dst_ref=landed.at[k], send_sem=ring_send.at[k], recv_sem=ring_recv.at[k],
            device_id={'wx': jnp.where(odd == 0, right, left)}, device_id_type=MESH)

    mo_load(2).start()
    for hh in range(n_hh):
        for w in range(n_w):
            wb_load(hh, w).start()
    for off in (1, 3, 0):
        mo_load(off).start()
    entry_barrier([right, left, partner])
    mo_load(2).wait()
    for hh in range(n_hh):
        for w in range(n_w):
            wb_load(hh, w).wait()
    for off in (1, 3, 0):
        mo_load(off).wait()

    def dot_of(i, which):
        xt, q, _ = step_of(i)
        rows = pl.ds(pl.multiple_of((xt * 2 + which) * seq, seq), seq)
        cols = pl.ds(pl.multiple_of(q * col, col), col)
        return jnp.dot(mo[rows, :], wb[:, cols], preferred_element_type=jnp.float32)

    def body(i, carry):
        given[i] = dot_of(i, 1 - core)

        @pl.when(i > 0)
        def _():
            pair_copy(i - 1).wait_recv()
            acc[i - 1] = acc[i - 1] + taken[i - 1]

        acc[i] = dot_of(i, core)
        pair_copy(i).start()

        @pl.when((i > 0) & (i <= 8))
        def _():
            ring_copy(i - 1, lax.rem(i - 1, 2)).start()

        return carry

    n_step = 4 * N_COL
    lax.fori_loop(0, n_step, body, 0)
    pair_copy(n_step - 1).wait_recv()
    acc[n_step - 1] = acc[n_step - 1] + taken[n_step - 1]
    for pair in range(2):
        for odd in range(2):
            k = 8 + pair * 2 + odd
            ring_copy(k - 8, odd).wait_recv()
            acc[k] = acc[k] + landed[k - 8]
        for q in (pair, pair + 2):
            cols = slice(q * col, (q + 1) * col)
            acc[12 + q] = acc[12 + q] + resid_ref[:, cols].astype(jnp.float32)
        for odd in range(2):
            ring_copy(8 + pair * 2 + odd, odd).start()
    for q, (raw, comb) in ((0, (5, 8)), (2, (4, 9)), (1, (7, 10)), (3, (6, 11))):
        ring_copy(raw, raw % 2).wait_recv()
        ring_copy(comb, comb % 2).wait_recv()
        cols = slice(q * col, (q + 1) * col)
        out_ref[:, cols] = (acc[12 + q] + (landed[raw] + landed[comb])).astype(jnp.bfloat16)
    for i in range(n_step):
        pair_copy(i).wait_send()
    for k in range(12):
        ring_copy(k, k % 2).wait_send()


def down_project(mo, wb, resid, n_wx):
    seq, d_model = resid.shape
    col = d_model // N_COL
    n_hh, n_w, k_loc, col_w = wb.shape
    n_step = 4 * N_COL
    return pl.pallas_call(
        functools.partial(down_kernel, n_wx),
        out_shape=jax.ShapeDtypeStruct((seq, d_model), jnp.bfloat16),
        in_specs=[pl.BlockSpec(memory_space=pl.ANY), pl.BlockSpec(memory_space=pl.ANY), pl.BlockSpec(memory_space=pltpu.VMEM)],
        out_specs=pl.BlockSpec(memory_space=pltpu.VMEM),
        scratch_shapes=[
            pltpu.VMEM(mo.shape, jnp.bfloat16),
            pltpu.VMEM((n_hh * k_loc, n_w * col_w), jnp.bfloat16),
            pltpu.VMEM((n_step, seq, col), jnp.float32),
            pltpu.VMEM((n_step, seq, col), jnp.float32),
            pltpu.VMEM((n_step, seq, col), jnp.float32),
            pltpu.VMEM((12, seq, col), jnp.float32),
            pltpu.SemaphoreType.DMA((4,)), pltpu.SemaphoreType.DMA((n_hh * n_w,)),
            pltpu.SemaphoreType.DMA((n_step,)), pltpu.SemaphoreType.DMA((n_step,)),
            pltpu.SemaphoreType.DMA((12,)), pltpu.SemaphoreType.DMA((12,)),
        ],
        compiler_params=pltpu.CompilerParams(collective_id=1, has_side_effects=True, vmem_limit_bytes=VMEM_LIMIT),
        cost_estimate=pl.CostEstimate(flops=40_000_000_000, bytes_accessed=16 * 2**20, transcendentals=0),
        name='down_project',
    )(mo, wb, resid)


def solution(mesh):
    batch_axes = ('dp', 'wy', 'wx')
    in_specs = (P(batch_axes), P(), P(None, 'wx', 'wy'), P(None, 'wx'), P(None, 'wx', None, 'wy'), P(None, 'wy', 'wx'), P(None, 'wy', 'wx'))
    out_specs = (P(batch_axes), P(None, batch_axes), P(None, batch_axes))
    n_wy, n_wx = mesh.shape['wy'], mesh.shape['wx']
    per = n_wy // n_wx
    perm = []
    for iy in range(n_wy):
        for ix in range(n_wx):
            perm.append((iy * n_wx + ix, ((iy % per) * n_wx + ix) * n_wx + iy // per))

    def device_step(x_tokens, gamma_ln, w_q, w_kv, w_gu, w_o, w_d):
        seq_len, d_model = x_tokens.shape[1], x_tokens.shape[2]
        head_dim = w_kv.shape[-1]
        d_loc = w_q.shape[1]
        f_loc = w_gu.shape[-1]
        n_layers = w_q.shape[0]
        cos_tab, sin_tab = rope_tables(seq_len, head_dim)
        iy = lax.axis_index('wy')
        weights_a, weights_b = [], []
        for layer_idx in range(n_layers):
            kv_half = lax.dynamic_index_in_dim(w_kv[layer_idx], lax.rem(iy, per), axis=1, keepdims=False)
            pack_a = jnp.concatenate([w_gu[layer_idx].reshape(d_loc, 2 * f_loc), w_q[layer_idx], kv_half], axis=1)
            pack_b = jnp.concatenate([w_d[layer_idx], w_o[layer_idx]], axis=0)
            pack_a = lax.ppermute(pack_a, ('wy', 'wx'), perm)
            pack_b = lax.ppermute(pack_b, ('wy', 'wx'), perm)
            full_a = lax.all_gather(pack_a, 'wy', axis=0, tiled=True)
            full_b = lax.all_gather(pack_b, 'wy', axis=0, tiled=True)
            weights_a.append(full_a.reshape(per, d_model, 2 * f_loc + 2 * head_dim))
            weights_b.append(full_b.reshape(per, n_wx, f_loc + head_dim, d_loc))
        resid = x_tokens[0]
        key_list = []
        value_list = []
        for layer_idx in range(n_layers):
            normed = layer_norm(resid, gamma_ln[layer_idx])
            h_all = gather_h(normed, n_wx)
            mo, k_rot, v_val = up_project(h_all, weights_a[layer_idx], cos_tab, sin_tab, f_loc, head_dim)
            resid = down_project(mo, weights_b[layer_idx], resid, n_wx)
            key_list.append(k_rot[None])
            value_list.append(v_val[None])
        return resid[None], jnp.stack(key_list), jnp.stack(value_list)

    return jax.shard_map(device_step, mesh=mesh, in_specs=in_specs, out_specs=out_specs, check_vma=False)
```

```python
import functools

import jax
import jax.numpy as jnp
from jax import lax
from jax.experimental import pallas as pl
from jax.experimental.pallas import tpu as pltpu
from jax.sharding import PartitionSpec as P

LN_EPS = 1e-6
ROPE_BASE = 10000.0
MESH = pl.DeviceIdType.MESH
VMEM_LIMIT = 60 * 1024 * 1024


def rope_tables(seq_len, head_dim):
    half_dim = head_dim // 2
    inv_freq = ROPE_BASE ** (-2.0 * jnp.arange(half_dim, dtype=jnp.float32) / head_dim)
    angles = jnp.arange(seq_len, dtype=jnp.float32)[:, None] * inv_freq[None, :]
    cos, sin = jnp.cos(angles), jnp.sin(angles)
    return jnp.concatenate([cos, cos], axis=1), jnp.concatenate([-sin, sin], axis=1)


def layer_norm(resid, g_scale):
    resid_f = resid.astype(jnp.float32)
    centered = resid_f - jnp.mean(resid_f, axis=-1, keepdims=True)
    variance = jnp.mean(centered * centered, axis=-1, keepdims=True)
    return (centered * lax.rsqrt(variance + LN_EPS) * g_scale).astype(jnp.bfloat16)


def ring_ids(n_wx):
    me = lax.axis_index('wx')
    chip, core = lax.div(me, 2), lax.rem(me, 2)
    n_chip = n_wx // 2

    def at(step, other=0):
        return lax.rem(chip + step, n_chip) * 2 + (lax.rem(core + other, 2))

    return me, chip, core, at


def entry_barrier(peers):
    barrier = pltpu.get_barrier_semaphore()
    for peer in peers:
        pl.semaphore_signal(barrier, inc=1, device_id={'wx': peer}, device_id_type=MESH)
    pl.semaphore_wait(barrier, len(peers))


def gather_copies(n_wx, hall, send_sem, recv_sem):
    me, chip, core, at = ring_ids(n_wx)
    half = hall.shape[1] // 2
    right, left, partner = at(1), at(3), at(0, 1)
    top, bottom, whole = pl.ds(0, half), pl.ds(half, half), pl.ds(0, 2 * half)

    def copy(num, block, rows, target):
        ref = hall.at[block, rows]
        return pltpu.make_async_remote_copy(
            src_ref=ref, dst_ref=ref, send_sem=send_sem.at[num], recv_sem=recv_sem.at[num],
            device_id={'wx': target}, device_id_type=MESH)

    return [
        copy(0, me, whole, partner),
        copy(1, me, top, right), copy(2, me, bottom, left),
        copy(3, me, bottom, right), copy(4, me, top, left),
        copy(5, left, top, right), copy(6, right, bottom, left),
        copy(7, left, whole, partner), copy(8, right, whole, partner),
        copy(9, at(2), top, partner), copy(10, at(2), bottom, partner),
    ]


def arrivals(n_wx, hall, send_sem, recv_sem):
    me, chip, core, at = ring_ids(n_wx)
    half = hall.shape[1] // 2
    top, bottom, whole = pl.ds(0, half), pl.ds(half, half), pl.ds(0, 2 * half)

    def copy(num, block, rows):
        ref = hall.at[block, rows]
        return pltpu.make_async_remote_copy(
            src_ref=ref, dst_ref=ref, send_sem=send_sem.at[num], recv_sem=recv_sem.at[num],
            device_id={'wx': at(0, 1)}, device_id_type=MESH)

    return [
        copy(0, at(0, 1), whole),
        copy(1, at(3), top), copy(2, at(1), bottom), copy(3, at(3), bottom), copy(4, at(1), top),
        copy(5, at(2), top), copy(6, at(2), bottom),
        copy(7, at(3, 1), whole), copy(8, at(1, 1), whole),
        copy(9, at(2, 1), top), copy(10, at(2, 1), bottom),
    ]


PLANE = 4


class PlaneGather:
    def __init__(self, buf, send_sem, recv_sem):
        self.buf, self.send_sem, self.recv_sem = buf, send_sem, recv_sem
        pos = lax.axis_index('wy')
        self.pos = (lax.div(pos, PLANE), lax.rem(pos, PLANE))

    def at(self, half, first, second):
        step_z, step_y = (second, first) if half == 0 else (first, second)
        z, y = self.pos
        return lax.rem(z + step_z + PLANE, PLANE) * PLANE + lax.rem(y + step_y + PLANE, PLANE)

    def copy(self, num, block, half, quarter, target):
        rows = self.buf.shape[1]
        size = rows // 2 if quarter is None else rows // 4
        start = half * (rows // 2) + (quarter or 0) * size
        ref = self.buf.at[block, pl.ds(start, size)]
        return pltpu.make_async_remote_copy(
            src_ref=ref, dst_ref=ref, send_sem=self.send_sem.at[num], recv_sem=self.recv_sem.at[num],
            device_id={'wy': target}, device_id_type=MESH)

    def one(self, half, sign, landing=False):
        num = half * 2 + (sign < 0)
        block = self.at(half, -sign if landing else 0, 0)
        return self.copy(num, block, half, None, self.at(half, sign, 0))

    def two(self, half, sign, landing=False):
        num = 4 + half * 2 + (sign < 0)
        block = self.at(half, -2 * sign if landing else -sign, 0)
        return self.copy(num, block, half, int(sign < 0), self.at(half, sign, 0))

    def three(self, half, off, sign, landing=False):
        num = 8 + (half * 4 + off % 4) * 2 + (sign < 0)
        block = self.at(half, off, -sign if landing else 0)
        return self.copy(num, block, half, None, self.at(half, 0, sign))

    def four(self, half, off, sign, landing=False):
        num = 24 + (half * 4 + off % 4) * 2 + (sign < 0)
        block = self.at(half, off, -2 * sign if landing else -sign)
        return self.copy(num, block, half, int(sign < 0), self.at(half, 0, sign))

    ways = [(half, sign) for half in range(2) for sign in (1, -1)]

    def start(self):
        for half, sign in self.ways:
            self.one(half, sign).start()
        for half, sign in self.ways:
            self.three(half, 0, sign).start()

    def stage_1(self):
        for half, sign in self.ways:
            self.one(half, sign, True).wait_recv()
            self.two(half, sign).start()
        for half, sign in self.ways:
            for way in (1, -1):
                self.three(half, -sign, way).start()

    def stage_2(self):
        for half, sign in self.ways:
            self.three(half, 0, sign, True).wait_recv()
            self.four(half, 0, sign).start()

    def stage_3(self):
        for half, sign in self.ways:
            self.two(half, sign, True).wait_recv()
        for half, sign in self.ways:
            self.three(half, 2, sign).start()

    def stage_4(self):
        for half, sign in self.ways:
            for off in (1, -1):
                self.three(half, off, sign, True).wait_recv()
                self.four(half, off, sign).start()

    def stage_5(self):
        for half, sign in self.ways:
            self.three(half, 2, sign, True).wait_recv()
            self.four(half, 2, sign).start()

    def finish(self):
        for half, sign in self.ways:
            for off in (0, 1, -1, 2):
                self.four(half, off, sign, True).wait_recv()

    def drain(self):
        for half, sign in self.ways:
            self.one(half, sign).wait_send()
            self.two(half, sign).wait_send()
            for off in (0, 1, -1, 2):
                self.three(half, off, sign).wait_send()
                self.four(half, off, sign).wait_send()


def up_step(hall, wa, mo, kv_out, xt, cos, sin, f_loc, head_dim):
    seq, d_model = hall.shape[1], hall.shape[2]
    n_w = wa.shape[0] // 2
    first = pl.multiple_of(xt * 2 * seq, 2 * seq)
    h = hall[pl.ds(xt * 2, 2)].reshape(2 * seq, d_model)
    width = f_loc + head_dim

    def project(hh, lo, hi):
        weight = wa[hh * n_w:(hh + 1) * n_w, :, lo:hi].reshape(d_model, hi - lo)
        return jnp.dot(h, weight, preferred_element_type=jnp.float32).astype(jnp.bfloat16)

    narrow = [project(hh, 2 * f_loc, 2 * (f_loc + head_dim)) for hh in range(2)]
    for hh in range(2):
        g_f = project(hh, 0, f_loc).astype(jnp.float32)
        u_f = project(hh, f_loc, 2 * f_loc).astype(jnp.float32)
        hidden = g_f * (1.0 / (1.0 + jnp.exp(-g_f))) * u_f
        mo[pl.ds(first, 2 * seq), hh * width:hh * width + f_loc] = hidden.astype(jnp.bfloat16)

    def rot(val):
        val_f = val.astype(jnp.float32)
        return (val_f * cos + pltpu.roll(val_f, head_dim // 2, 1) * sin).astype(jnp.bfloat16)

    allowed = lax.broadcasted_iota(jnp.int32, (seq, seq), 0) >= lax.broadcasted_iota(jnp.int32, (seq, seq), 1)
    for b in range(2):
        part = slice(b * seq, (b + 1) * seq)
        k_rot = rot(narrow[0][part, head_dim:])
        v_val = narrow[1][part, head_dim:]
        kv_out[b, 0] = k_rot
        kv_out[b, 1] = v_val
        for hh in range(2):
            q_rot = rot(narrow[hh][part, :head_dim])
            scores = lax.dot_general(q_rot, k_rot, (((1,), (1,)), ((), ())), preferred_element_type=jnp.float32) * head_dim ** -0.5
            scores = jnp.where(allowed, scores, -jnp.inf)
            top = jnp.max(scores, axis=-1, keepdims=True)
            expd = jnp.exp(scores - top)
            probs = (expd / jnp.sum(expd, axis=-1, keepdims=True)).astype(jnp.bfloat16)
            att = jnp.dot(probs, v_val, preferred_element_type=jnp.float32)
            mo[pl.ds(first + b * seq, seq), hh * width + f_loc:(hh + 1) * width] = att.astype(jnp.bfloat16)


def up_kernel(n_wx, f_loc, head_dim, gathers, *refs):
    if gathers:
        (h_ref, wa_ref, wb_ref, cos_ref, sin_ref, mo_ref, k_ref, v_ref, wb_out, hall, wa, mo, kv, send_sem, recv_sem, own_sem, w_sem, out_sem, kv_sem,
         wb, a_send, a_recv, b_send, b_recv, wb_sem) = refs
    else:
        h_ref, wa_ref, cos_ref, sin_ref, mo_ref, k_ref, v_ref, hall, wa, mo, kv, send_sem, recv_sem, own_sem, w_sem, out_sem, kv_sem = refs
    me, chip, core, at = ring_ids(n_wx)
    n_chip = n_wx // 2
    seq = hall.shape[1]
    sends = gather_copies(n_wx, hall, send_sem, recv_sem)
    lands = arrivals(n_wx, hall, send_sem, recv_sem)
    own_load = pltpu.make_async_copy(h_ref, hall.at[me], own_sem)
    own_load.start()
    if gathers:
        here = lax.axis_index('wy')
        gather_a = PlaneGather(wa, a_send, a_recv)
        gather_b = PlaneGather(wb, b_send, b_recv)
        a_load = pltpu.make_async_copy(wa_ref, wa.at[here], w_sem.at[0])
        b_load = pltpu.make_async_copy(wb_ref, wb.at[here], w_sem.at[1])
        a_load.start()
        b_load.start()
    else:
        half_w = wa.shape[0] // 2
        w_loads = [pltpu.make_async_copy(wa_ref.at[pl.ds(hh * half_w, half_w)], wa.at[pl.ds(hh * half_w, half_w)], w_sem.at[hh]) for hh in range(2)]
        for load in w_loads:
            load.start()
    barrier = pltpu.get_barrier_semaphore()
    peers = [{'wx': at(1)}, {'wx': at(3)}, {'wx': at(0, 1)}]
    if gathers:
        peers += [{'wy': gather_a.at(0, 1, 0)}, {'wy': gather_a.at(0, -1, 0)}, {'wy': gather_a.at(1, 1, 0)}, {'wy': gather_a.at(1, -1, 0)}]
    for peer in peers:
        pl.semaphore_signal(barrier, inc=1, device_id=peer, device_id_type=MESH)
    pl.semaphore_wait(barrier, len(peers))
    own_load.wait()
    for num in range(5):
        sends[num].start()
    if gathers:
        a_load.wait()
        gather_a.start()
        gather_a.stage_1()
        lands[1].wait_recv()
        sends[5].start()
        lands[2].wait_recv()
        sends[6].start()
        gather_a.stage_2()
        gather_a.stage_3()
        lands[3].wait_recv()
        sends[7].start()
        lands[4].wait_recv()
        sends[8].start()
        lands[0].wait_recv()
        gather_a.stage_4()
        lands[5].wait_recv()
        sends[9].start()
        lands[6].wait_recv()
        sends[10].start()
        gather_a.stage_5()
        b_load.wait()
        gather_b.start()
        for num in range(7, 11):
            lands[num].wait_recv()
        gather_a.finish()
    else:
        for load in w_loads:
            load.wait()

    def out_copy(xt):
        rows = pl.ds(pl.multiple_of(xt * 2 * seq, 2 * seq), 2 * seq)
        return pltpu.make_async_copy(mo.at[rows], mo_ref.at[rows], out_sem.at[xt])

    def body(step, carry):
        off = jnp.where(step == 0, 0, jnp.where(step == 1, 3, jnp.where(step == 2, 1, 2)))
        xt = lax.rem(chip + off, n_chip)
        if gathers:
            @pl.when(step == 1)
            def _():
                gather_b.stage_1()

            @pl.when(step == 2)
            def _():
                gather_b.stage_2()
                gather_b.stage_3()

            @pl.when(step == 3)
            def _():
                gather_b.stage_4()
                gather_b.stage_5()
        else:
            @pl.when(step == 0)
            def _():
                lands[0].wait_recv()

            @pl.when(step == 1)
            def _():
                lands[1].wait_recv()
                sends[5].start()
                lands[2].wait_recv()
                sends[6].start()
                lands[3].wait_recv()
                sends[7].start()
                lands[4].wait_recv()
                sends[8].start()
                lands[7].wait_recv()

            @pl.when(step == 2)
            def _():
                lands[8].wait_recv()

            @pl.when(step == 3)
            def _():
                lands[5].wait_recv()
                sends[9].start()
                lands[6].wait_recv()
                sends[10].start()
                lands[9].wait_recv()
                lands[10].wait_recv()

        up_step(hall, wa, mo, kv.at[step], xt, cos_ref[...], sin_ref[...], f_loc, head_dim)
        out_copy(xt).start()
        return carry

    lax.fori_loop(0, n_chip, body, 0)
    caches = [pltpu.make_async_copy(kv.at[0, core, num], ref, kv_sem.at[num]) for num, ref in enumerate((k_ref, v_ref))]
    for cache in caches:
        cache.start()
    if gathers:
        gather_b.finish()
        wb_copy = pltpu.make_async_copy(wb, wb_out, wb_sem)
        wb_copy.start()
        wb_copy.wait()
        gather_a.drain()
        gather_b.drain()
    for num in range(11):
        sends[num].wait_send()
    for xt in range(n_chip):
        out_copy(xt).wait()
    for cache in caches:
        cache.wait()


def up_project(h, wa, wb, cos, sin, f_loc, head_dim, n_wx, gathers):
    seq, d_model = h.shape
    n_chip = n_wx // 2
    n_block = PLANE * PLANE
    width = 2 * (f_loc + head_dim)
    any_spec, vmem_spec = pl.BlockSpec(memory_space=pl.ANY), pl.BlockSpec(memory_space=pltpu.VMEM)
    out_shape = [
        jax.ShapeDtypeStruct((n_wx * seq, width), jnp.bfloat16),
        jax.ShapeDtypeStruct((seq, head_dim), jnp.bfloat16),
        jax.ShapeDtypeStruct((seq, head_dim), jnp.bfloat16),
    ]
    wa_shape = (n_block,) + wa.shape if gathers else wa.shape
    scratch = [
        pltpu.VMEM((n_wx, seq, d_model), jnp.bfloat16),
        pltpu.VMEM(wa_shape, jnp.bfloat16),
        pltpu.VMEM((n_wx * seq, width), jnp.bfloat16),
        pltpu.VMEM((n_chip, 2, 2, seq, head_dim), jnp.bfloat16),
        pltpu.SemaphoreType.DMA((11,)), pltpu.SemaphoreType.DMA((11,)),
        pltpu.SemaphoreType.DMA, pltpu.SemaphoreType.DMA((2,)),
        pltpu.SemaphoreType.DMA((n_chip,)), pltpu.SemaphoreType.DMA((2,)),
    ]
    args = [h, wa, cos, sin]
    in_specs = [any_spec, any_spec, vmem_spec, vmem_spec]
    if gathers:
        out_shape.append(jax.ShapeDtypeStruct((n_block,) + wb.shape, jnp.bfloat16))
        scratch += [
            pltpu.VMEM((n_block,) + wb.shape, jnp.bfloat16),
            pltpu.SemaphoreType.DMA((40,)), pltpu.SemaphoreType.DMA((40,)),
            pltpu.SemaphoreType.DMA((40,)), pltpu.SemaphoreType.DMA((40,)),
            pltpu.SemaphoreType.DMA,
        ]
        args.insert(2, wb)
        in_specs.insert(2, any_spec)
    return pl.pallas_call(
        functools.partial(up_kernel, n_wx, f_loc, head_dim, gathers),
        out_shape=tuple(out_shape),
        in_specs=in_specs,
        out_specs=[any_spec] * len(out_shape),
        scratch_shapes=scratch,
        compiler_params=pltpu.CompilerParams(collective_id=0 if gathers else 2, has_side_effects=True, vmem_limit_bytes=VMEM_LIMIT),
        cost_estimate=pl.CostEstimate(flops=40_000_000_000, bytes_accessed=24 * 2**20, transcendentals=0),
        name='up_gather' if gathers else 'up_project',
    )(*args)


N_COL = 4


def down_kernel(n_wx, normed, mo_ref, wb_ref, resid_ref, gamma_ref, *refs):
    if normed:
        out_ref, h_ref = refs[:2]
    else:
        out_ref = refs[0]
    (mo, wb, given, taken, acc, landed, mo_sem, wb_sem, pair_send, pair_recv, ring_send, ring_recv) = refs[1 + normed:]
    me, chip, core, at = ring_ids(n_wx)
    n_chip = n_wx // 2
    right, left, partner = at(1), at(3), at(0, 1)
    seq = resid_ref.shape[0]
    n_block, k_loc, col_w = wb_ref.shape
    n_w = n_wx
    n_hh = n_block // n_w
    col = wb.shape[1] // N_COL

    def step_of(i):
        phase, j = lax.div(i, 4), lax.rem(i, 4)
        odd, slot = lax.rem(j, 2), lax.div(j, 2)
        off = jnp.where(phase == 0, 2, jnp.where(phase == 3, 0, 1 + 2 * odd))
        q = jnp.where(phase == 3, j, jnp.where(phase == 1, (1 - odd) * 2 + slot, odd * 2 + slot))
        return lax.rem(chip + off, n_chip), q, odd

    def mo_load(off):
        rows = pl.ds(pl.multiple_of(lax.rem(chip + off, n_chip) * 2 * seq, 2 * seq), 2 * seq)
        return pltpu.make_async_copy(mo_ref.at[rows], mo.at[rows], mo_sem.at[off])

    def wb_load(hh, w):
        return pltpu.make_async_copy(
            wb_ref.at[hh * n_w + w], wb.at[pl.ds(hh * k_loc, k_loc), pl.ds(w * col_w, col_w)], wb_sem.at[hh * n_w + w])

    def pair_copy(i):
        return pltpu.make_async_remote_copy(
            src_ref=given.at[i], dst_ref=taken.at[i], send_sem=pair_send.at[i], recv_sem=pair_recv.at[i],
            device_id={'wx': partner}, device_id_type=MESH)

    def ring_copy(k, odd):
        return pltpu.make_async_remote_copy(
            src_ref=acc.at[k], dst_ref=landed.at[k], send_sem=ring_send.at[k], recv_sem=ring_recv.at[k],
            device_id={'wx': jnp.where(odd == 0, right, left)}, device_id_type=MESH)

    mo_load(2).start()
    for hh in range(n_hh):
        for w in range(n_w):
            wb_load(hh, w).start()
    for off in (1, 3, 0):
        mo_load(off).start()
    entry_barrier([right, left, partner])
    mo_load(2).wait()
    for hh in range(n_hh):
        for w in range(n_w):
            wb_load(hh, w).wait()
    for off in (1, 3, 0):
        mo_load(off).wait()

    def dot_of(i, which):
        xt, q, _ = step_of(i)
        rows = pl.ds(pl.multiple_of((xt * 2 + which) * seq, seq), seq)
        cols = pl.ds(pl.multiple_of(q * col, col), col)
        return jnp.dot(mo[rows, :], wb[:, cols], preferred_element_type=jnp.float32)

    def body(i, carry):
        given[i] = dot_of(i, 1 - core)

        @pl.when(i > 0)
        def _():
            pair_copy(i - 1).wait_recv()
            acc[i - 1] = acc[i - 1] + taken[i - 1]

        acc[i] = dot_of(i, core)
        pair_copy(i).start()

        @pl.when((i > 0) & (i <= 8))
        def _():
            ring_copy(i - 1, lax.rem(i - 1, 2)).start()

        return carry

    n_step = 4 * N_COL
    lax.fori_loop(0, n_step, body, 0)
    pair_copy(n_step - 1).wait_recv()
    acc[n_step - 1] = acc[n_step - 1] + taken[n_step - 1]
    for pair in range(2):
        for odd in range(2):
            k = 8 + pair * 2 + odd
            ring_copy(k - 8, odd).wait_recv()
            acc[k] = acc[k] + landed[k - 8]
        for q in (pair, pair + 2):
            cols = slice(q * col, (q + 1) * col)
            acc[12 + q] = acc[12 + q] + resid_ref[:, cols].astype(jnp.float32)
        for odd in range(2):
            ring_copy(8 + pair * 2 + odd, odd).start()
    for q, (raw, comb) in ((0, (5, 8)), (2, (4, 9)), (1, (7, 10)), (3, (6, 11))):
        ring_copy(raw, raw % 2).wait_recv()
        ring_copy(comb, comb % 2).wait_recv()
        cols = slice(q * col, (q + 1) * col)
        out_ref[:, cols] = (acc[12 + q] + (landed[raw] + landed[comb])).astype(jnp.bfloat16)
    if normed:
        resid_f = out_ref[...].astype(jnp.float32)
        centered = resid_f - jnp.mean(resid_f, axis=-1, keepdims=True)
        variance = jnp.mean(centered * centered, axis=-1, keepdims=True)
        h_ref[...] = (centered * lax.rsqrt(variance + LN_EPS) * gamma_ref[...]).astype(jnp.bfloat16)
    for i in range(n_step):
        pair_copy(i).wait_send()
    for k in range(12):
        ring_copy(k, k % 2).wait_send()


def down_project(mo, wb, resid, gamma, n_wx, normed):
    seq, d_model = resid.shape
    col = d_model // N_COL
    n_block, k_loc, col_w = wb.shape
    n_w = n_wx
    n_hh = n_block // n_w
    n_step = 4 * N_COL
    return pl.pallas_call(
        functools.partial(down_kernel, n_wx, normed),
        out_shape=(jax.ShapeDtypeStruct((seq, d_model), jnp.bfloat16),) * (1 + normed),
        in_specs=[pl.BlockSpec(memory_space=pl.ANY), pl.BlockSpec(memory_space=pl.ANY), pl.BlockSpec(memory_space=pltpu.VMEM),
                  pl.BlockSpec(memory_space=pltpu.VMEM)],
        out_specs=[pl.BlockSpec(memory_space=pltpu.VMEM)] * (1 + normed),
        scratch_shapes=[
            pltpu.VMEM(mo.shape, jnp.bfloat16),
            pltpu.VMEM((n_hh * k_loc, n_w * col_w), jnp.bfloat16),
            pltpu.VMEM((n_step, seq, col), jnp.float32),
            pltpu.VMEM((n_step, seq, col), jnp.float32),
            pltpu.VMEM((n_step, seq, col), jnp.float32),
            pltpu.VMEM((12, seq, col), jnp.float32),
            pltpu.SemaphoreType.DMA((4,)), pltpu.SemaphoreType.DMA((n_hh * n_w,)),
            pltpu.SemaphoreType.DMA((n_step,)), pltpu.SemaphoreType.DMA((n_step,)),
            pltpu.SemaphoreType.DMA((12,)), pltpu.SemaphoreType.DMA((12,)),
        ],
        compiler_params=pltpu.CompilerParams(collective_id=1 if normed else 3, has_side_effects=True, vmem_limit_bytes=VMEM_LIMIT),
        cost_estimate=pl.CostEstimate(flops=40_000_000_000, bytes_accessed=16 * 2**20, transcendentals=0),
        name='down_project',
    )(mo, wb, resid, gamma)


def solution(mesh):
    batch_axes = ('dp', 'wy', 'wx')
    in_specs = (P(batch_axes), P(), P(None, 'wx', 'wy'), P(None, 'wx'), P(None, 'wx', None, 'wy'), P(None, 'wy', 'wx'), P(None, 'wy', 'wx'))
    out_specs = (P(batch_axes), P(None, batch_axes), P(None, batch_axes))
    n_wy, n_wx = mesh.shape['wy'], mesh.shape['wx']
    per = n_wy // n_wx
    perm = []
    for iy in range(n_wy):
        for ix in range(n_wx):
            perm.append((iy * n_wx + ix, ((iy % per) * n_wx + ix) * n_wx + iy // per))

    def device_step(x_tokens, gamma_ln, w_q, w_kv, w_gu, w_o, w_d):
        seq_len, d_model = x_tokens.shape[1], x_tokens.shape[2]
        head_dim = w_kv.shape[-1]
        d_loc = w_q.shape[1]
        f_loc = w_gu.shape[-1]
        cos_tab, sin_tab = rope_tables(seq_len, head_dim)
        iy = lax.axis_index('wy')
        packs = []
        for layer_idx in range(2):
            kv_half = lax.dynamic_index_in_dim(w_kv[layer_idx], lax.rem(iy, per), axis=1, keepdims=False)
            pack_a = jnp.concatenate([w_gu[layer_idx].reshape(d_loc, 2 * f_loc), w_q[layer_idx], kv_half], axis=1)
            pack_b = jnp.concatenate([w_d[layer_idx], w_o[layer_idx]], axis=0)
            if layer_idx:
                pack_a, pack_b, packs[0][0], packs[0][1] = lax.optimization_barrier((pack_a, pack_b, packs[0][0], packs[0][1]))
            packs.append([lax.ppermute(pack, ('wy', 'wx'), perm) for pack in (pack_a, pack_b)])
        resid = x_tokens[0]
        normed = layer_norm(resid, gamma_ln[0])
        mo, k_0, v_0, wb_0 = up_project(normed, packs[0][0], packs[0][1], cos_tab, sin_tab, f_loc, head_dim, n_wx, True)
        pack_a, pack_b, mo, wb_0 = lax.optimization_barrier((packs[1][0], packs[1][1], mo, wb_0))
        wa_1 = lax.all_gather(pack_a, 'wy', axis=0, tiled=True).reshape((n_wy,) + pack_a.shape)
        wb_1 = lax.all_gather(pack_b, 'wy', axis=0, tiled=True).reshape((n_wy,) + pack_b.shape)
        resid, normed = down_project(mo, wb_0, resid, gamma_ln[1:], n_wx, True)
        mo, k_1, v_1 = up_project(normed, wa_1, None, cos_tab, sin_tab, f_loc, head_dim, n_wx, False)
        resid, = down_project(mo, wb_1, resid, gamma_ln[1:], n_wx, False)
        return resid[None], jnp.stack([k_0, k_1])[:, None], jnp.stack([v_0, v_1])[:, None]

    return jax.shard_map(device_step, mesh=mesh, in_specs=in_specs, out_specs=out_specs, check_vma=False)
```

```python
import functools

import jax
import jax.numpy as jnp
from jax import lax
from jax.experimental import pallas as pl
from jax.experimental.pallas import tpu as pltpu
from jax.sharding import PartitionSpec as P

LN_EPS = 1e-6
ROPE_BASE = 10000.0
MESH = pl.DeviceIdType.MESH
VMEM_LIMIT = 67043328
PLANE = 4
SUB = 128
N_COL = 4
N_RING = 12


def rope_tables(seq_len, head_dim):
    half_dim = head_dim // 2
    inv_freq = ROPE_BASE ** (-2.0 * jnp.arange(half_dim, dtype=jnp.float32) / head_dim)
    angles = jnp.arange(seq_len, dtype=jnp.float32)[:, None] * inv_freq[None, :]
    cos, sin = jnp.cos(angles), jnp.sin(angles)
    return jnp.concatenate([cos, cos], axis=1), jnp.concatenate([-sin, sin], axis=1)


def remote(src, dst, send, recv, target):
    return pltpu.make_async_remote_copy(src_ref=src, dst_ref=dst, send_sem=send, recv_sem=recv, device_id=target, device_id_type=MESH)


class Ring:
    def __init__(self, n_wx):
        self.me = lax.axis_index('wx')
        self.chip, self.core = lax.div(self.me, 2), lax.rem(self.me, 2)
        self.n_chip = n_wx // 2
        self.right, self.left, self.far = self.at(1), self.at(self.n_chip - 1), self.at(2)
        self.pair = self.at(0, 1)

    def at(self, step, other=0):
        return lax.rem(self.chip + step, self.n_chip) * 2 + lax.rem(self.core + other, 2)


class ChipGather:
    def __init__(self, ring, hall, send_sem, recv_sem):
        half = hall.shape[1] // 2
        top, bottom, whole = pl.ds(0, half), pl.ds(half, half), pl.ds(0, 2 * half)
        me, left, right, far, pair = ring.me, ring.left, ring.right, ring.far, ring.pair
        moves = [
            (me, whole, pair, pair),
            (me, top, right, left), (me, bottom, left, right),
            (me, bottom, right, left), (me, top, left, right),
            (left, top, right, far), (right, bottom, left, far),
            (left, whole, pair, ring.at(ring.n_chip - 1, 1)), (right, whole, pair, ring.at(1, 1)),
            (far, top, pair, ring.at(2, 1)), (far, bottom, pair, ring.at(2, 1)),
        ]
        self.sends, self.lands = [], []
        for num, (block, rows, target, landed) in enumerate(moves):
            for kept, there in ((self.sends, block), (self.lands, landed)):
                ref = hall.at[there, rows]
                kept.append(remote(ref, ref, send_sem.at[num], recv_sem.at[num], {'wx': target}))
        self.first = 5

    def start(self):
        for copy in self.sends[:self.first]:
            copy.start()

    def relay(self, landed, sent):
        self.lands[landed].wait_recv()
        self.sends[sent].start()

    def near_halves(self):
        self.relay(1, 5)
        self.relay(2, 6)

    def near_rest(self):
        self.relay(3, 7)
        self.relay(4, 8)

    def far_halves(self):
        self.relay(5, 9)
        self.relay(6, 10)

    def wait(self, *nums):
        for num in nums:
            self.lands[num].wait_recv()

    def drain(self):
        for copy in self.sends:
            copy.wait_send()


class PlaneGather:
    ways = [(half, sign) for half in range(2) for sign in (1, -1)]

    def __init__(self, buf, send_sem, recv_sem):
        self.buf, self.send_sem, self.recv_sem = buf, send_sem, recv_sem
        self.here = lax.axis_index('wy')
        self.pos = (lax.div(self.here, PLANE), lax.rem(self.here, PLANE))

    def at(self, half, first, second=0):
        step_z, step_y = (second, first) if half == 0 else (first, second)
        z, y = self.pos
        return lax.rem(z + step_z + PLANE, PLANE) * PLANE + lax.rem(y + step_y + PLANE, PLANE)

    def neighbours(self):
        return [{'wy': self.at(half, sign)} for half, sign in self.ways]

    def place(self, block, start, size):
        return self.buf.at[lax.div(block, 2), lax.rem(block, 2), pl.ds(start, size)]

    def copy(self, kind, num, block, half, quarter, target):
        rows = self.buf.shape[2]
        size = rows // 2 if quarter is None else rows // PLANE
        ref = self.place(block, half * (rows // 2) + (quarter or 0) * size, size)
        slot = kind * PLANE + num
        return remote(ref, ref, self.send_sem.at[slot], self.recv_sem.at[slot], {'wy': target})

    def one(self, half, sign, landing=False):
        block = self.at(half, -sign if landing else 0)
        return self.copy(0, half * 2 + (sign < 0), block, half, None, self.at(half, sign))

    def two(self, half, sign, landing=False):
        block = self.at(half, -2 * sign if landing else -sign)
        return self.copy(1, half * 2 + (sign < 0), block, half, int(sign < 0), self.at(half, sign))

    def three(self, half, off, sign, landing=False):
        block = self.at(half, off, -sign if landing else 0)
        return self.copy(2, (half * PLANE + off % PLANE) * 2 + (sign < 0), block, half, None, self.at(half, 0, sign))

    def four(self, half, off, sign, landing=False):
        block = self.at(half, off, -2 * sign if landing else -sign)
        return self.copy(6, (half * PLANE + off % PLANE) * 2 + (sign < 0), block, half, int(sign < 0), self.at(half, 0, sign))

    def start(self):
        for half, sign in self.ways:
            self.one(half, sign).start()
        for half, sign in self.ways:
            self.three(half, 0, sign).start()

    def stage_1(self):
        for half, sign in self.ways:
            self.one(half, sign, True).wait_recv()
            self.two(half, sign).start()
        for half, sign in self.ways:
            for way in (1, -1):
                self.three(half, -sign, way).start()

    def fourth(self, off):
        for half, sign in self.ways:
            self.three(half, off, sign, True).wait_recv()
            self.four(half, off, sign).start()

    def stage_2(self):
        self.fourth(0)

    def stage_3(self):
        for half, sign in self.ways:
            self.two(half, sign, True).wait_recv()
        for half, sign in self.ways:
            self.three(half, 2, sign).start()

    def stage_4(self):
        self.fourth(1)
        self.fourth(-1)

    def stage_5(self):
        self.fourth(2)

    def each(self, call):
        for half, sign in self.ways:
            for off in (0, 1, -1, 2):
                call(half, off, sign)

    def finish(self):
        self.each(lambda half, off, sign: self.four(half, off, sign, True).wait_recv())

    def drain(self):
        for half, sign in self.ways:
            self.one(half, sign).wait_send()
            self.two(half, sign).wait_send()
        self.each(lambda half, off, sign: self.three(half, off, sign).wait_send())
        self.each(lambda half, off, sign: self.four(half, off, sign).wait_send())


class Exchange:
    def __init__(self, ring, layer, shards, at_a, at_b, send_sem, recv_sem):
        pos = lax.axis_index('wy')
        odd = lax.rem(pos, 2)
        other = pos + 1 - 2 * odd
        same = odd == ring.core
        half = ring.n_chip * 2
        self.ring, self.pos = ring, pos
        self.send_to = (jnp.where(same, other, pos), jnp.where(same, ring.core, 1 - ring.core))
        self.recv_from = (jnp.where(same, pos, other), jnp.where(same, 1 - ring.core, ring.core))
        self.head_to = {'wy': odd * half + (1 - ring.core) * ring.n_chip + ring.chip, 'wx': lax.div(pos, 2)}
        self.head_from = {
            'wy': 2 * ring.me + lax.div(pos, half),
            'wx': lax.rem(pos, ring.n_chip) * 2 + 1 - lax.div(lax.rem(pos, half), ring.n_chip)}
        self.layer, self.shards = layer, shards
        self.at_a, self.at_b = at_a, at_b
        self.send_sem, self.recv_sem = send_sem, recv_sem

    def peers(self):
        wy, core = self.recv_from
        return [{'wy': wy, 'wx': self.chip(k) * 2 + core} for k in range(self.ring.n_chip)] + [self.head_from]

    def chip(self, step):
        return lax.rem(self.ring.chip + step, self.ring.n_chip)

    def block(self, which, step, landing):
        chip = self.chip(step)
        wy, core = self.send_to
        origin = chip if landing else self.ring.chip
        gu, d = self.shards[:2]
        rows = SUB if which else gu.shape[2]
        src = d.at[self.layer, pl.ds(pl.multiple_of(chip * SUB, SUB), SUB)] if which else gu.at[self.layer, chip]
        place = self.at_b if which else self.at_a
        dst = place(self.pos if landing else wy, pl.multiple_of(origin * rows, rows), rows)
        base = which * self.ring.n_chip
        return remote(src, dst, self.send_sem.at[base + chip], self.recv_sem.at[base + origin], {'wy': wy, 'wx': chip * 2 + core})

    def heads(self, which, landing):
        gu, d, q, kv, o = self.shards
        unit = self.pos if landing else self.head_to['wy']
        if which:
            parts = [(o, self.at_b(unit, self.ring.n_chip * SUB, o.shape[1]))]
        else:
            ref = self.at_a(unit, self.ring.n_chip * gu.shape[2], q.shape[1])
            parts = [(src, ref.at[:, pl.ds(num * SUB, SUB)]) for num, src in enumerate((q, kv))]
        base = self.ring.n_chip * 2 + which * 2
        return [remote(src.at[self.layer], dst, self.send_sem.at[base + num], self.recv_sem.at[base + num], self.head_to) for num, (src, dst) in enumerate(parts)]

    def copies(self, which, landing=False):
        return [self.block(which, step, landing) for step in (1, 3, 2, 0)] + self.heads(which, landing)

    def start(self, which):
        for copy in self.copies(which):
            copy.start()

    def land(self, which):
        for copy in self.copies(which, True):
            copy.wait_recv()

    def drain(self, which):
        for copy in self.copies(which):
            copy.wait_send()


def up_step(hall, wa, mo, kv_out, xt, cos, sin, between):
    seq, d_model = hall.shape[1], hall.shape[2]
    n_jj, tile, head_dim = wa.shape[0], wa.shape[3], cos.shape[1]
    half_d = d_model // 2
    first = pl.multiple_of(xt * 2 * seq, 2 * seq)
    h = hall[pl.ds(xt * 2, 2)].reshape(2 * seq, d_model)

    def project(weight):
        return jnp.dot(h, weight, preferred_element_type=jnp.float32).astype(jnp.bfloat16)

    narrow = [project(wa[hh * n_jj // 2:(hh + 1) * n_jj // 2, :, half_d:, :].reshape(d_model, tile)) for hh in range(2)]
    for jj in range(0, n_jj, 2):
        if jj == n_jj // 2:
            between()
        weight = jnp.concatenate([wa[jj + k, :, :half_d, :].reshape(d_model, tile) for k in range(2)], axis=1)
        both = project(weight)
        for k in range(2):
            g_f, u_f = (both[:, k * tile + part * SUB:k * tile + (part + 1) * SUB].astype(jnp.float32) for part in range(2))
            hidden = g_f * (1.0 / (1.0 + jnp.exp(-g_f))) * u_f
            mo[pl.ds(first, 2 * seq), (jj + k) * SUB:(jj + k + 1) * SUB] = hidden.astype(jnp.bfloat16)

    def rot(val):
        val_f = val.astype(jnp.float32)
        return (val_f * cos + pltpu.roll(val_f, head_dim // 2, 1) * sin).astype(jnp.bfloat16)

    allowed = lax.broadcasted_iota(jnp.int32, (seq, seq), 0) >= lax.broadcasted_iota(jnp.int32, (seq, seq), 1)
    for b in range(2):
        part = slice(b * seq, (b + 1) * seq)
        k_rot = rot(narrow[0][part, head_dim:])
        v_val = narrow[1][part, head_dim:]
        kv_out[b, 0] = k_rot
        kv_out[b, 1] = v_val
        for hh in range(2):
            q_rot = rot(narrow[hh][part, :head_dim])
            scores = lax.dot_general(q_rot, k_rot, (((1,), (1,)), ((), ())), preferred_element_type=jnp.float32) * head_dim ** -0.5
            scores = jnp.where(allowed, scores, -jnp.inf)
            expd = jnp.exp(scores - jnp.max(scores, axis=-1, keepdims=True))
            probs = (expd / jnp.sum(expd, axis=-1, keepdims=True)).astype(jnp.bfloat16)
            att = jnp.dot(probs, v_val, preferred_element_type=jnp.float32)
            lo = n_jj * SUB + hh * head_dim
            mo[pl.ds(first + b * seq, seq), lo:lo + head_dim] = att.astype(jnp.bfloat16)


class Scatter:
    def __init__(self, ring, first, mo, wb, given, taken, acc, landed, pair_send, pair_recv, ring_send, ring_recv):
        self.ring, self.first = ring, first
        self.mo, self.wb, self.given, self.taken, self.acc, self.landed = mo, wb, given, taken, acc, landed
        self.pair_send, self.pair_recv, self.ring_send, self.ring_recv = pair_send, pair_recv, ring_send, ring_recv

    def piece(self, n):
        if self.first:
            return n
        return jnp.where(n < N_COL, n + N_COL, jnp.where(n < 2 * N_COL, n - N_COL, n))

    def pair_copy(self, n):
        k, slot = self.piece(n), lax.rem(n, N_COL)
        return remote(self.given.at[slot], self.taken.at[k], self.pair_send.at[k], self.pair_recv.at[k], {'wx': self.ring.pair})

    def ring_copy(self, k):
        target = jnp.where(lax.rem(k, 2) == 0, self.ring.right, self.ring.left)
        return remote(self.acc.at[k], self.landed.at[k], self.ring_send.at[k], self.ring_recv.at[k], {'wx': target})

    def products(self, k):
        seq, col = self.acc.shape[1:]
        n_jj, _, rows, tile = self.wb.shape
        phase, j = lax.div(k, N_COL), lax.rem(k, N_COL)
        odd, slot = lax.rem(j, 2), lax.div(j, 2)
        own = phase == 3
        off = jnp.where(phase == 0, 2, jnp.where(own, 0, 1 + 2 * odd))
        q = jnp.where(own, j, jnp.where(phase == 1, 1 - odd, odd) * 2 + slot)
        xt = lax.rem(self.ring.chip + off, self.ring.n_chip)

        def columns(side):
            parts = [self.wb[:, side, pl.ds(pl.multiple_of(q * SUB, SUB), SUB), :].reshape(n_jj * SUB, tile)]
            for hh in range(2):
                unit = hh * n_jj + side * N_COL + q
                parts.append(self.wb[lax.div(unit, 2), lax.rem(unit, 2), N_COL * SUB:, :])
            return jnp.concatenate(parts, axis=0)

        weight = jnp.concatenate([columns(1), columns(0)], axis=1)

        def product(core):
            return jnp.dot(self.mo[pl.ds(pl.multiple_of((xt * 2 + core) * seq, seq), seq), :], weight, preferred_element_type=jnp.float32)

        return product

    def combine(self, n):
        k = self.piece(n)
        self.pair_copy(n).wait_recv()
        self.acc[k] = self.acc[k] + self.taken[k]

    def send(self, n):
        k = self.piece(n)

        @pl.when(k < 2 * N_COL)
        def _():
            self.ring_copy(k).start()

    def run(self, lo, hi):
        def body(n, carry):
            product = self.products(self.piece(n))

            @pl.when(n >= N_COL)
            def _():
                self.pair_copy(n - N_COL).wait_send()

            self.given[lax.rem(n, N_COL)] = product(1 - self.ring.core)

            @pl.when(n > lo)
            def _():
                self.combine(n - 1)

            self.acc[self.piece(n)] = product(self.ring.core)
            self.pair_copy(n).start()

            @pl.when(n > lo)
            def _():
                self.send(n - 1)

            return carry

        lax.fori_loop(lo, hi, body, 0)

        @pl.when(hi > lo)
        def _():
            self.combine(hi - 1)
            self.send(hi - 1)

    def finish(self, resid_ref, out_ref, beside):
        col = self.acc.shape[2]
        own = 3 * N_COL
        for pair in range(2):
            for odd in range(2):
                k = 2 * (N_COL + pair) + odd
                self.ring_copy(k - 2 * N_COL).wait_recv()
                self.acc[k] = self.acc[k] + self.landed[k - 2 * N_COL]
            for q in (pair, pair + 2):
                self.acc[own + q] = self.acc[own + q] + resid_ref[:, q * col:(q + 1) * col].astype(jnp.float32)
            for odd in range(2):
                self.ring_copy(2 * (N_COL + pair) + odd).start()
            beside[pair]()
        for pair in range(2):
            for q, raw, comb in ((pair, 5, 8), (pair + 2, 4, 9)):
                raw, comb = raw + 2 * pair, comb + 2 * pair
                self.ring_copy(raw).wait_recv()
                self.ring_copy(comb).wait_recv()
                out_ref[:, q * col:(q + 1) * col] = (self.acc[own + q] + (self.landed[raw] + self.landed[comb])).astype(jnp.bfloat16)
            beside[2 + pair]()
        for n in range(own, own + N_COL):
            self.pair_copy(n).wait_send()
        for k in range(N_RING):
            self.ring_copy(k).wait_send()


def layer_kernel(n_wx, first, *refs):
    if first:
        (resid_ref, gamma_ref, cos_ref, sin_ref, gu_ref, d_ref, q_ref, kv_ref, o_ref, out_ref, k_ref, v_ref, next_a, next_b,
         next_send, next_recv, x0_send, x0_recv, x1_send, x1_recv, a_send, a_recv, *rest) = refs
    else:
        resid_ref, gamma_ref, cos_ref, sin_ref, wa_ref, b_ref, out_ref, k_ref, v_ref, w_sem, *rest = refs
    hall, wa, wb, mo, kv, h_send, h_recv, b_send, b_recv, kv_sem, *parts = rest
    ring = Ring(n_wx)
    gather_h = ChipGather(ring, hall, h_send, h_recv)
    gather_b = PlaneGather(wb, b_send, b_recv)
    scatter = Scatter(ring, first, mo, wb, *parts)
    peers = [{'wx': ring.right}, {'wx': ring.left}, {'wx': ring.pair}] + gather_b.neighbours()
    if first:
        shards = gu_ref, d_ref, q_ref, kv_ref, o_ref
        gather_a = PlaneGather(wa, a_send, a_recv)
        gather_n = PlaneGather(next_a, next_send, next_recv)
        swap_0 = Exchange(ring, 0, shards, gather_a.place, gather_b.place, x0_send, x0_recv)
        swap_1 = Exchange(ring, 1, shards, gather_n.place, lambda unit, start, size: next_b.at[pl.ds(start, size)], x1_send, x1_recv)
        peers += swap_0.peers()
    else:
        here = gather_b.here
        b_load = pltpu.make_async_copy(b_ref, wb.at[lax.div(here, 2), lax.rem(here, 2)], w_sem.at[0])
        a_load = pltpu.make_async_copy(wa_ref, wa, w_sem.at[1])
        b_load.start()
        a_load.start()
    barrier = pltpu.get_barrier_semaphore()
    for peer in peers:
        pl.semaphore_signal(barrier, inc=1, device_id=peer, device_id_type=MESH)

    resid_f = resid_ref[...].astype(jnp.float32)
    centered = resid_f - jnp.mean(resid_f, axis=-1, keepdims=True)
    variance = jnp.mean(centered * centered, axis=-1, keepdims=True)
    normed = (centered * lax.rsqrt(variance + LN_EPS) * gamma_ref[...]).astype(jnp.bfloat16)
    tile = normed.shape[1] // n_wx
    for w in range(n_wx):
        lo = ((1 - w % 2) * ring.n_chip + w // 2) * tile
        hall[ring.me, :, lo:lo + tile] = normed[:, w * tile:(w + 1) * tile]

    pl.semaphore_wait(barrier, len(peers))
    if first:
        swap_0.start(0)
        gather_h.start()
        swap_0.land(0)
        gather_a.start()
        swap_0.start(1)
        gather_a.stage_1()
        gather_h.near_halves()
        gather_a.stage_2()
        gather_a.stage_3()
        gather_h.near_rest()
        swap_1.start(0)
        swap_1.start(1)
        gather_a.stage_4()
        gather_h.far_halves()
        gather_a.stage_5()
        swap_0.land(1)
        gather_b.start()
        gather_h.wait(0, 7, 8, 9, 10)
        gather_a.finish()
    else:
        b_load.wait()
        gather_h.start()
        gather_b.start()
        a_load.wait()

    def body(step, carry):
        turn = lax.rem(step + 1, PLANE) if first else step
        off = jnp.where(turn == 0, 0, jnp.where(turn == 1, 3, jnp.where(turn == 2, 1, 2)))

        def when(num, *calls):
            @pl.when(step == num)
            def _():
                for call in calls:
                    call()

        if first:
            when(1, gather_b.stage_1)
            when(2, gather_b.stage_3)
            when(3, gather_n.stage_1)
        else:
            when(0, lambda: gather_h.wait(0))
            when(1, gather_b.stage_1, gather_h.near_halves, gather_b.stage_2, gather_b.stage_3, gather_h.near_rest, lambda: gather_h.wait(7))
            when(2, gather_b.stage_4, gather_b.stage_5, lambda: gather_h.wait(8))
            when(3, gather_h.far_halves, lambda: gather_h.wait(9, 10))

        def between():
            if first:
                when(1, gather_b.stage_2)
                when(2, gather_b.stage_4)

        mine = jnp.where(turn == 0, 0, 1)
        up_step(hall, wa, mo, kv.at[mine], lax.rem(ring.chip + off, ring.n_chip), cos_ref[...], sin_ref[...], between)
        if first:
            when(2, gather_b.stage_5, gather_b.finish, lambda: swap_1.land(0), gather_n.start)
        else:
            when(2, gather_b.finish)
        split = 2 * N_COL if first else N_COL
        last = step == 3
        scatter.run(jnp.where(last, split, 0), jnp.where(last, 4 * N_COL, jnp.where(step == 2, split, 0)))
        return carry

    lax.fori_loop(0, ring.n_chip, body, 0)
    caches = [pltpu.make_async_copy(kv.at[0, ring.core, num], ref, kv_sem.at[num]) for num, ref in enumerate((k_ref, v_ref))]
    for cache in caches:
        cache.start()
    if first:
        scatter.finish(resid_ref, out_ref, (gather_n.stage_2, gather_n.stage_3, gather_n.stage_4, gather_n.stage_5))
        gather_n.finish()
        swap_1.land(1)
        for swap in (swap_0, swap_1):
            swap.drain(0)
            swap.drain(1)
        gather_a.drain()
        gather_n.drain()
    else:
        scatter.finish(resid_ref, out_ref, [lambda: None] * 4)
    gather_b.drain()
    gather_h.drain()
    for cache in caches:
        cache.wait()


def layer(resid, gamma, cos, sin, weights, n_wx, first):
    seq, d_model = resid.shape
    head_dim = cos.shape[1]
    n_unit = PLANE * PLANE
    col = d_model // N_COL
    any_spec, vmem_spec = pl.BlockSpec(memory_space=pl.ANY), pl.BlockSpec(memory_space=pltpu.VMEM)
    tile = d_model // n_wx
    unit_b = (PLANE * SUB + head_dim, tile)
    wa_shape = (n_unit // 2, 2, (PLANE + 1) * tile, tile)
    wb_shape = (n_unit // 2, 2) + unit_b
    piece = (seq, col)
    n_piece = 4 * N_COL
    dma = pltpu.SemaphoreType.DMA
    out_shape = [jax.ShapeDtypeStruct(shape, jnp.bfloat16) for shape in (resid.shape, (seq, head_dim), (seq, head_dim))]
    n_plane, n_swap, n_hop = dma((40,)), dma((11,)), dma((11,))
    if first:
        out_shape += [jax.ShapeDtypeStruct(shape, jnp.bfloat16) for shape in (wa_shape, unit_b)]
        scratch = [n_plane, n_plane, n_swap, n_swap, n_swap, n_swap, n_plane, n_plane]
    else:
        scratch = [dma((2,))]
    scratch += [
        pltpu.VMEM((n_wx, seq, d_model), jnp.bfloat16),
        pltpu.VMEM(wa_shape, jnp.bfloat16),
        pltpu.VMEM(wb_shape, jnp.bfloat16),
        pltpu.VMEM((n_wx * seq, n_unit // 2 * SUB + 2 * head_dim), jnp.bfloat16),
        pltpu.VMEM((2, 2, 2, seq, head_dim), jnp.bfloat16),
        n_hop, n_hop, n_plane, n_plane, dma((2,)),
        pltpu.VMEM((N_COL,) + piece, jnp.float32),
        pltpu.VMEM((n_piece,) + piece, jnp.float32),
        pltpu.VMEM((n_piece,) + piece, jnp.float32),
        pltpu.VMEM((N_RING,) + piece, jnp.float32),
        dma((n_piece,)), dma((n_piece,)), dma((N_RING,)), dma((N_RING,)),
    ]
    return pl.pallas_call(
        functools.partial(layer_kernel, n_wx, first),
        out_shape=tuple(out_shape),
        in_specs=[vmem_spec] * 4 + [any_spec] * len(weights),
        out_specs=[vmem_spec] + [any_spec] * (len(out_shape) - 1),
        scratch_shapes=scratch,
        compiler_params=pltpu.CompilerParams(collective_id=int(first), has_side_effects=True, vmem_limit_bytes=VMEM_LIMIT),
        name='layer_0' if first else 'layer_1',
    )(resid, gamma, cos, sin, *weights)


def solution(mesh):
    batch_axes = ('dp', 'wy', 'wx')
    in_specs = (P(batch_axes), P(), P(None, 'wx', 'wy'), P(None, 'wx'), P(None, 'wx', None, 'wy'), P(None, 'wy', 'wx'), P(None, 'wy', 'wx'))
    out_specs = (P(batch_axes), P(None, batch_axes), P(None, batch_axes))
    n_wx = mesh.shape['wx']

    def device_step(x_tokens, gamma_ln, w_q, w_kv, w_gu, w_o, w_d):
        n_layers, d_loc = w_q.shape[:2]
        cos_tab, sin_tab = rope_tables(x_tokens.shape[1], w_kv.shape[-1])
        kv_half = lax.dynamic_index_in_dim(w_kv, lax.rem(lax.axis_index('wy'), 2), axis=2, keepdims=False)
        gu = jnp.transpose(w_gu.reshape(n_layers, d_loc, 2, n_wx // 2, SUB), (0, 3, 1, 2, 4)).reshape(n_layers, n_wx // 2, d_loc, 2 * SUB)
        resid, k_0, v_0, wa, unit_b = layer(x_tokens[0], gamma_ln[:1], cos_tab, sin_tab, (gu, w_d, w_q, kv_half, w_o), n_wx, True)
        resid, k_1, v_1 = layer(resid, gamma_ln[1:], cos_tab, sin_tab, (wa, unit_b), n_wx, False)
        return resid[None], jnp.stack([k_0, k_1])[:, None], jnp.stack([v_0, v_1])[:, None]

    return jax.shard_map(device_step, mesh=mesh, in_specs=in_specs, out_specs=out_specs, check_vma=False)
```

```python
import functools

import jax
import jax.numpy as jnp
from jax import lax
from jax.experimental import pallas as pl
from jax.experimental.pallas import tpu as pltpu
from jax.sharding import PartitionSpec as P

LN_EPS = 1e-6
ROPE_BASE = 10000.0
MESH = pl.DeviceIdType.MESH
VMEM_LIMIT = 67043328
PLANE = 4
SUB = 128
N_COL = 4
N_RING = 12


def rope_tables(seq_len, head_dim):
    half_dim = head_dim // 2
    inv_freq = ROPE_BASE ** (-2.0 * jnp.arange(half_dim, dtype=jnp.float32) / head_dim)
    angles = jnp.arange(seq_len, dtype=jnp.float32)[:, None] * inv_freq[None, :]
    cos, sin = jnp.cos(angles), jnp.sin(angles)
    return jnp.concatenate([cos, cos], axis=1), jnp.concatenate([-sin, sin], axis=1)


def remote(src, dst, send, recv, target):
    return pltpu.make_async_remote_copy(src_ref=src, dst_ref=dst, send_sem=send, recv_sem=recv, device_id=target, device_id_type=MESH)


class Ring:
    def __init__(self, n_wx):
        self.me = lax.axis_index('wx')
        self.chip, self.core = lax.div(self.me, 2), lax.rem(self.me, 2)
        self.n_chip = n_wx // 2
        self.right, self.left, self.far = self.at(1), self.at(self.n_chip - 1), self.at(2)
        self.pair = self.at(0, 1)

    def at(self, step, other=0):
        return lax.rem(self.chip + step, self.n_chip) * 2 + lax.rem(self.core + other, 2)


class ChipGather:
    def __init__(self, ring, hall, send_sem, recv_sem):
        half = hall.shape[1] // 2
        top, bottom, whole = pl.ds(0, half), pl.ds(half, half), pl.ds(0, 2 * half)
        me, left, right, far, pair = ring.me, ring.left, ring.right, ring.far, ring.pair
        moves = [
            (me, whole, pair, pair),
            (me, top, right, left), (me, bottom, left, right),
            (me, bottom, right, left), (me, top, left, right),
            (left, top, right, far), (right, bottom, left, far),
            (left, top, pair, ring.at(ring.n_chip - 1, 1)), (right, bottom, pair, ring.at(1, 1)),
            (left, bottom, pair, ring.at(ring.n_chip - 1, 1)), (right, top, pair, ring.at(1, 1)),
            (far, top, pair, ring.at(2, 1)), (far, bottom, pair, ring.at(2, 1)),
        ]
        self.sends, self.lands = [], []
        for num, (block, rows, target, landed) in enumerate(moves):
            for kept, there in ((self.sends, block), (self.lands, landed)):
                ref = hall.at[there, rows]
                kept.append(remote(ref, ref, send_sem.at[num], recv_sem.at[num], {'wx': target}))
        self.first = 5

    def start(self):
        for copy in self.sends[:self.first]:
            copy.start()

    def relay(self, landed, *sent):
        self.lands[landed].wait_recv()
        for num in sent:
            self.sends[num].start()

    def near_halves(self):
        self.relay(1, 5, 7)
        self.relay(2, 6, 8)

    def near_rest(self):
        self.relay(3, 9)
        self.relay(4, 10)

    def far_halves(self):
        self.relay(5, 11)
        self.relay(6, 12)

    def wait(self, *nums):
        for num in nums:
            self.lands[num].wait_recv()

    def drain(self):
        for copy in self.sends:
            copy.wait_send()


class PlaneGather:
    ways = [(half, sign) for half in range(2) for sign in (1, -1)]

    def __init__(self, buf, send_sem, recv_sem):
        self.buf, self.send_sem, self.recv_sem = buf, send_sem, recv_sem
        self.here = lax.axis_index('wy')
        self.pos = (lax.div(self.here, PLANE), lax.rem(self.here, PLANE))

    def at(self, half, first, second=0):
        step_z, step_y = (second, first) if half == 0 else (first, second)
        z, y = self.pos
        return lax.rem(z + step_z + PLANE, PLANE) * PLANE + lax.rem(y + step_y + PLANE, PLANE)

    def neighbours(self):
        return [{'wy': self.at(half, sign)} for half, sign in self.ways]

    def place(self, block, start, size):
        return self.buf.at[lax.div(block, 2), lax.rem(block, 2), pl.ds(start, size)]

    def copy(self, kind, num, block, half, quarter, target):
        rows = self.buf.shape[2]
        size = rows // 2 if quarter is None else rows // PLANE
        ref = self.place(block, half * (rows // 2) + (quarter or 0) * size, size)
        slot = kind * PLANE + num
        return remote(ref, ref, self.send_sem.at[slot], self.recv_sem.at[slot], {'wy': target})

    def one(self, half, sign, landing=False):
        block = self.at(half, -sign if landing else 0)
        return self.copy(0, half * 2 + (sign < 0), block, half, None, self.at(half, sign))

    def two(self, half, sign, landing=False):
        block = self.at(half, -2 * sign if landing else -sign)
        return self.copy(1, half * 2 + (sign < 0), block, half, int(sign < 0), self.at(half, sign))

    def three(self, half, off, sign, landing=False):
        block = self.at(half, off, -sign if landing else 0)
        return self.copy(2, (half * PLANE + off % PLANE) * 2 + (sign < 0), block, half, None, self.at(half, 0, sign))

    def four(self, half, off, sign, landing=False):
        block = self.at(half, off, -2 * sign if landing else -sign)
        return self.copy(6, (half * PLANE + off % PLANE) * 2 + (sign < 0), block, half, int(sign < 0), self.at(half, 0, sign))

    def start(self):
        for half, sign in self.ways:
            self.one(half, sign).start()
        for half, sign in self.ways:
            self.three(half, 0, sign).start()

    def stage_1(self):
        for half, sign in self.ways:
            self.one(half, sign, True).wait_recv()
            self.two(half, sign).start()
        for half, sign in self.ways:
            for way in (1, -1):
                self.three(half, -sign, way).start()

    def fourth(self, off):
        for half, sign in self.ways:
            self.three(half, off, sign, True).wait_recv()
            self.four(half, off, sign).start()

    def stage_2(self):
        self.fourth(0)

    def stage_3(self):
        for half, sign in self.ways:
            self.two(half, sign, True).wait_recv()
        for half, sign in self.ways:
            self.three(half, 2, sign).start()

    def stage_4(self):
        self.fourth(1)
        self.fourth(-1)

    def stage_5(self):
        self.fourth(2)

    def each(self, call):
        for half, sign in self.ways:
            for off in (0, 1, -1, 2):
                call(half, off, sign)

    def finish(self):
        self.each(lambda half, off, sign: self.four(half, off, sign, True).wait_recv())

    def drain(self):
        for half, sign in self.ways:
            self.one(half, sign).wait_send()
            self.two(half, sign).wait_send()
        self.each(lambda half, off, sign: self.three(half, off, sign).wait_send())
        self.each(lambda half, off, sign: self.four(half, off, sign).wait_send())


class Exchange:
    def __init__(self, ring, layer, shards, at_a, at_b, send_sem, recv_sem):
        pos = lax.axis_index('wy')
        odd = lax.rem(pos, 2)
        other = pos + 1 - 2 * odd
        same = odd == ring.core
        half = ring.n_chip * 2
        self.ring, self.pos = ring, pos
        self.send_to = (jnp.where(same, other, pos), jnp.where(same, ring.core, 1 - ring.core))
        self.recv_from = (jnp.where(same, pos, other), jnp.where(same, 1 - ring.core, ring.core))
        self.head_to = {'wy': odd * half + (1 - ring.core) * ring.n_chip + ring.chip, 'wx': lax.div(pos, 2)}
        self.head_from = {
            'wy': 2 * ring.me + lax.div(pos, half),
            'wx': lax.rem(pos, ring.n_chip) * 2 + 1 - lax.div(lax.rem(pos, half), ring.n_chip)}
        self.layer, self.shards = layer, shards
        self.at_a, self.at_b = at_a, at_b
        self.send_sem, self.recv_sem = send_sem, recv_sem

    def peers(self):
        wy, core = self.recv_from
        return [{'wy': wy, 'wx': self.chip(k) * 2 + core} for k in range(self.ring.n_chip)] + [self.head_from]

    def chip(self, step):
        return lax.rem(self.ring.chip + step, self.ring.n_chip)

    def block(self, which, step, landing):
        chip = self.chip(step)
        wy, core = self.send_to
        origin = chip if landing else self.ring.chip
        gu, d = self.shards[:2]
        rows = SUB if which else gu.shape[2]
        src = d.at[self.layer, pl.ds(pl.multiple_of(chip * SUB, SUB), SUB)] if which else gu.at[self.layer, chip]
        place = self.at_b if which else self.at_a
        dst = place(self.pos if landing else wy, pl.multiple_of(origin * rows, rows), rows)
        base = which * self.ring.n_chip
        return remote(src, dst, self.send_sem.at[base + chip], self.recv_sem.at[base + origin], {'wy': wy, 'wx': chip * 2 + core})

    def heads(self, which, landing):
        gu, d, q, kv, o = self.shards
        unit = self.pos if landing else self.head_to['wy']
        if which:
            parts = [(o, self.at_b(unit, self.ring.n_chip * SUB, o.shape[1]))]
        else:
            ref = self.at_a(unit, self.ring.n_chip * gu.shape[2], q.shape[1])
            parts = [(src, ref.at[:, pl.ds(num * SUB, SUB)]) for num, src in enumerate((q, kv))]
        base = self.ring.n_chip * 2 + which * 2
        return [remote(src.at[self.layer], dst, self.send_sem.at[base + num], self.recv_sem.at[base + num], self.head_to) for num, (src, dst) in enumerate(parts)]

    def copies(self, which, landing=False):
        return [self.block(which, step, landing) for step in (1, 3, 2, 0)] + self.heads(which, landing)

    def start(self, which):
        for copy in self.copies(which):
            copy.start()

    def land(self, which):
        for copy in self.copies(which, True):
            copy.wait_recv()

    def drain(self, which):
        for copy in self.copies(which):
            copy.wait_send()


def up_step(hall, wa, mo, narrow, chunks, between):
    d_model = hall.shape[2]
    half = hall.shape[1] // 2
    n_jj, tile = wa.shape[0], wa.shape[3]
    half_d = d_model // 2
    rows = [(prompt, pl.ds(pl.multiple_of(start, half), half)) for prompt, start in chunks]
    h = jnp.concatenate([hall[prompt, part] for prompt, part in rows], axis=0)

    def project(weight):
        return jnp.dot(h, weight, preferred_element_type=jnp.float32).astype(jnp.bfloat16)

    def keep(value, ref, lo):
        for num, (prompt, part) in enumerate(rows):
            ref[prompt, part, lo:lo + value.shape[1]] = value[num * half:(num + 1) * half]

    for hh in range(2):
        keep(project(wa[hh * n_jj // 2:(hh + 1) * n_jj // 2, :, half_d:, :].reshape(d_model, tile)), narrow, hh * tile)
    for jj in range(0, n_jj, 2):
        if jj == n_jj // 2:
            between()
        weight = jnp.concatenate([wa[jj + k, :, :half_d, :].reshape(d_model, tile) for k in range(2)], axis=1)
        both = project(weight)
        for k in range(2):
            g_f, u_f = (both[:, k * tile + part * SUB:k * tile + (part + 1) * SUB].astype(jnp.float32) for part in range(2))
            hidden = g_f * (1.0 / (1.0 + jnp.exp(-g_f))) * u_f
            keep(hidden.astype(jnp.bfloat16), mo, (jj + k) * SUB)


def attend(narrow, mo, kv_out, xt, cos, sin):
    seq, head_dim = cos.shape
    tile = 2 * head_dim

    def rot(val):
        val_f = val.astype(jnp.float32)
        return (val_f * cos + pltpu.roll(val_f, head_dim // 2, 1) * sin).astype(jnp.bfloat16)

    allowed = lax.broadcasted_iota(jnp.int32, (seq, seq), 0) >= lax.broadcasted_iota(jnp.int32, (seq, seq), 1)
    for b in range(2):
        prompt = xt * 2 + b
        k_rot = rot(narrow[prompt, :, head_dim:tile])
        v_val = narrow[prompt, :, tile + head_dim:]
        kv_out[b, 0] = k_rot
        kv_out[b, 1] = v_val
        for hh in range(2):
            q_rot = rot(narrow[prompt, :, hh * tile:hh * tile + head_dim])
            scores = lax.dot_general(q_rot, k_rot, (((1,), (1,)), ((), ())), preferred_element_type=jnp.float32) * head_dim ** -0.5
            scores = jnp.where(allowed, scores, -jnp.inf)
            expd = jnp.exp(scores - jnp.max(scores, axis=-1, keepdims=True))
            probs = (expd / jnp.sum(expd, axis=-1, keepdims=True)).astype(jnp.bfloat16)
            att = jnp.dot(probs, v_val, preferred_element_type=jnp.float32)
            lo = mo.shape[2] - (2 - hh) * head_dim
            mo[prompt, :, lo:lo + head_dim] = att.astype(jnp.bfloat16)


class Scatter:
    def __init__(self, ring, first, mo, wb, given, taken, acc, landed, pair_send, pair_recv, ring_send, ring_recv):
        self.ring, self.first = ring, first
        self.mo, self.wb, self.given, self.taken, self.acc, self.landed = mo, wb, given, taken, acc, landed
        self.pair_send, self.pair_recv, self.ring_send, self.ring_recv = pair_send, pair_recv, ring_send, ring_recv

    def piece(self, n):
        if self.first:
            return n
        return jnp.where(n < N_COL, n + N_COL, jnp.where(n < 2 * N_COL, n - N_COL, n))

    def pair_copy(self, n):
        k, slot = self.piece(n), lax.rem(n, N_COL)
        return remote(self.given.at[slot], self.taken.at[k], self.pair_send.at[k], self.pair_recv.at[k], {'wx': self.ring.pair})

    def ring_copy(self, k):
        target = jnp.where(lax.rem(k, 2) == 0, self.ring.right, self.ring.left)
        return remote(self.acc.at[k], self.landed.at[k], self.ring_send.at[k], self.ring_recv.at[k], {'wx': target})

    def products(self, k):
        n_jj, tile = self.wb.shape[0], self.wb.shape[3]
        phase, j = lax.div(k, N_COL), lax.rem(k, N_COL)
        odd, slot = lax.rem(j, 2), lax.div(j, 2)
        own = phase == 3
        off = jnp.where(phase == 0, 2, jnp.where(own, 0, 1 + 2 * odd))
        q = jnp.where(own, j, jnp.where(phase == 1, 1 - odd, odd) * 2 + slot)
        xt = lax.rem(self.ring.chip + off, self.ring.n_chip)

        def columns(side):
            parts = [self.wb[:, side, pl.ds(pl.multiple_of(q * SUB, SUB), SUB), :].reshape(n_jj * SUB, tile)]
            for hh in range(2):
                unit = hh * n_jj + side * N_COL + q
                parts.append(self.wb[lax.div(unit, 2), lax.rem(unit, 2), N_COL * SUB:, :])
            return jnp.concatenate(parts, axis=0)

        weight = jnp.concatenate([columns(1), columns(0)], axis=1)

        def product(core):
            return jnp.dot(self.mo[xt * 2 + core], weight, preferred_element_type=jnp.float32)

        return product

    def combine(self, n):
        k = self.piece(n)
        self.pair_copy(n).wait_recv()
        self.acc[k] = self.acc[k] + self.taken[k]

    def send(self, n):
        k = self.piece(n)

        @pl.when(k < 2 * N_COL)
        def _():
            self.ring_copy(k).start()

    def run(self, lo, hi):
        def body(n, carry):
            product = self.products(self.piece(n))

            @pl.when(n >= N_COL)
            def _():
                self.pair_copy(n - N_COL).wait_send()

            self.given[lax.rem(n, N_COL)] = product(1 - self.ring.core)

            @pl.when(n > lo)
            def _():
                self.combine(n - 1)

            self.acc[self.piece(n)] = product(self.ring.core)
            self.pair_copy(n).start()

            @pl.when(n > lo)
            def _():
                self.send(n - 1)

            return carry

        lax.fori_loop(lo, hi, body, 0)

        @pl.when(hi > lo)
        def _():
            self.combine(hi - 1)
            self.send(hi - 1)

    def finish(self, resid_ref, out_ref, beside):
        col = self.acc.shape[2]
        own = 3 * N_COL
        for pair in range(2):
            for odd in range(2):
                k = 2 * (N_COL + pair) + odd
                self.ring_copy(k - 2 * N_COL).wait_recv()
                self.acc[k] = self.acc[k] + self.landed[k - 2 * N_COL]
            for q in (pair, pair + 2):
                self.acc[own + q] = self.acc[own + q] + resid_ref[:, q * col:(q + 1) * col].astype(jnp.float32)
            for odd in range(2):
                self.ring_copy(2 * (N_COL + pair) + odd).start()
            beside[pair]()
        for pair in range(2):
            for k in (N_COL + 2 * pair, N_COL + 2 * pair + 1):
                self.ring_copy(k).wait_recv()
            beside[2 + pair]()
        for pair in range(2):
            for q, raw, comb in ((pair, 5, 8), (pair + 2, 4, 9)):
                raw, comb = raw + 2 * pair, comb + 2 * pair
                self.ring_copy(comb).wait_recv()
                out_ref[:, q * col:(q + 1) * col] = (self.acc[own + q] + (self.landed[raw] + self.landed[comb])).astype(jnp.bfloat16)
        for n in range(own, own + N_COL):
            self.pair_copy(n).wait_send()
        for k in range(N_RING):
            self.ring_copy(k).wait_send()


def layer_kernel(n_wx, first, *refs):
    if first:
        (resid_ref, gamma_ref, cos_ref, sin_ref, gu_ref, d_ref, q_ref, kv_ref, o_ref, out_ref, k_out, v_out, next_a, next_b,
         next_send, next_recv, x0_send, x0_recv, x1_send, x1_recv, a_send, a_recv, *rest) = refs
    else:
        resid_ref, gamma_ref, cos_ref, sin_ref, wa_ref, b_ref, k_ref, v_ref, out_ref, k_out, v_out, w_sem, old_sem, *rest = refs
    hall, wa, wb, mo, narrow, kv, h_send, h_recv, b_send, b_recv, kv_sem, *parts = rest
    ring = Ring(n_wx)
    gather_h = ChipGather(ring, hall, h_send, h_recv)
    gather_b = PlaneGather(wb, b_send, b_recv)
    scatter = Scatter(ring, first, mo, wb, *parts)
    peers = [{'wx': ring.right}, {'wx': ring.left}, {'wx': ring.pair}] + gather_b.neighbours()
    if first:
        shards = gu_ref, d_ref, q_ref, kv_ref, o_ref
        gather_a = PlaneGather(wa, a_send, a_recv)
        gather_n = PlaneGather(next_a, next_send, next_recv)
        swap_0 = Exchange(ring, 0, shards, gather_a.place, gather_b.place, x0_send, x0_recv)
        swap_1 = Exchange(ring, 1, shards, gather_n.place, lambda unit, start, size: next_b.at[pl.ds(start, size)], x1_send, x1_recv)
        peers += swap_0.peers()
    else:
        here = gather_b.here
        b_load = pltpu.make_async_copy(b_ref, wb.at[lax.div(here, 2), lax.rem(here, 2)], w_sem.at[0])
        a_load = pltpu.make_async_copy(wa_ref, wa, w_sem.at[1])
        old_loads = [pltpu.make_async_copy(ref, kv.at[2, 0, num], old_sem.at[num]) for num, ref in enumerate((k_ref, v_ref))]
        for load in (b_load, a_load, *old_loads):
            load.start()
    barrier = pltpu.get_barrier_semaphore()
    for peer in peers:
        pl.semaphore_signal(barrier, inc=1, device_id=peer, device_id_type=MESH)

    resid_f = resid_ref[...].astype(jnp.float32)
    centered = resid_f - jnp.mean(resid_f, axis=-1, keepdims=True)
    variance = jnp.mean(centered * centered, axis=-1, keepdims=True)
    normed = (centered * lax.rsqrt(variance + LN_EPS) * gamma_ref[1 - first:2 - first, :]).astype(jnp.bfloat16)
    tile = normed.shape[1] // n_wx
    for w in range(n_wx):
        lo = ((1 - w % 2) * ring.n_chip + w // 2) * tile
        hall[ring.me, :, lo:lo + tile] = normed[:, w * tile:(w + 1) * tile]

    pl.semaphore_wait(barrier, len(peers))
    if first:
        swap_0.start(0)
        gather_h.start()
        swap_0.land(0)
        gather_a.start()
        swap_0.start(1)
        gather_a.stage_1()
        gather_h.near_halves()
        gather_a.stage_2()
        gather_a.stage_3()
        gather_h.near_rest()
        swap_1.start(0)
        swap_1.start(1)
        gather_a.stage_4()
        gather_h.far_halves()
        gather_a.stage_5()
        swap_0.land(1)
        gather_b.start()
        gather_h.wait(0, 7, 8, 9, 10, 11, 12)
        gather_a.finish()
    else:
        gather_h.start()
        b_load.wait()
        gather_b.start()
        a_load.wait()

    seq = hall.shape[1]
    half = seq // 2

    def body(step, carry):
        turn = lax.rem(step + 1, PLANE) if first else step

        def when(num, *calls):
            @pl.when(step == num)
            def _():
                for call in calls:
                    call()

        if first:
            when(1, gather_b.stage_1)
            when(2, gather_b.stage_3)
        else:
            when(0, lambda: gather_h.wait(0))
            when(1, gather_b.stage_1, gather_h.near_halves, gather_b.stage_2, lambda: gather_h.wait(7, 8))
            when(2, gather_b.stage_3, gather_h.near_rest, gather_b.stage_4, lambda: gather_h.wait(9, 10))
            when(3, gather_h.far_halves, lambda: gather_h.wait(11, 12))

        def between():
            if first:
                when(1, gather_b.stage_2)
                when(2, gather_b.stage_4)
                when(3, gather_n.stage_1)
            else:
                when(2, gather_b.stage_5)

        near = (turn == 1) | (turn == 2)
        lone = jnp.where(turn == 0, ring.chip, lax.rem(ring.chip + 2, ring.n_chip))
        one = jnp.where(near, lax.div(ring.left, 2), lone)
        two = jnp.where(near, lax.div(ring.right, 2), lone)
        start = jnp.where(turn == 2, half, 0)
        up_step(hall, wa, mo, narrow, [(one * 2 + b, start) for b in range(2)] + [(two * 2 + b, half - start) for b in range(2)], between)

        def attention(num, carry):
            place = lax.rem(num + 1, PLANE) if first else num
            off = jnp.where(place == 0, 0, jnp.where(place == 1, 3, jnp.where(place == 2, 1, 2)))
            attend(narrow, mo, kv.at[jnp.where(place == 0, 0, 1)], lax.rem(ring.chip + off, ring.n_chip), cos_ref[...], sin_ref[...])
            return carry

        early = 0 if first else 1
        lo = jnp.where(step == 3, 3, jnp.where(step == 2, 2 - early, 0))
        if first:
            hi = jnp.where(step == 0, 0, step + 1)
            lo = jnp.where(step == 2, 2, lo)
        else:
            lo, hi = jnp.where(step == 1, 1, lo), jnp.where(step < 2, 1, step + 1)
        lax.fori_loop(lo, hi, attention, 0)
        if first:
            when(2, gather_b.stage_5, gather_b.finish, lambda: swap_1.land(0), gather_n.start)
        else:
            when(2, gather_b.finish)
        split = 2 * N_COL if first else N_COL
        last = step == 3
        scatter.run(jnp.where(last, split, 0), jnp.where(last, 4 * N_COL, jnp.where(step == 2, split, 0)))
        return carry

    lax.fori_loop(0, ring.n_chip, body, 0)
    if first:
        caches = [(kv.at[0, ring.core, num], ref) for num, ref in enumerate((k_out, v_out))]
    else:
        for load in old_loads:
            load.wait()
        caches = [(kv.at[0, ring.core, num], ref.at[1]) for num, ref in enumerate((k_out, v_out))]
        caches += [(kv.at[2, 0, num], ref.at[0]) for num, ref in enumerate((k_out, v_out))]
    caches = [pltpu.make_async_copy(src, dst, kv_sem.at[num]) for num, (src, dst) in enumerate(caches)]
    for cache in caches:
        cache.start()
    if first:
        scatter.finish(resid_ref, out_ref, (gather_n.stage_2, gather_n.stage_3, gather_n.stage_4, gather_n.stage_5))
        gather_n.finish()
        swap_1.land(1)
        for swap in (swap_0, swap_1):
            swap.drain(0)
            swap.drain(1)
        gather_a.drain()
        gather_n.drain()
    else:
        scatter.finish(resid_ref, out_ref, [lambda: None] * 4)
    gather_b.drain()
    gather_h.drain()
    for cache in caches:
        cache.wait()


def layer(resid, gamma, cos, sin, weights, n_wx, first):
    seq, d_model = resid.shape
    head_dim = cos.shape[1]
    n_unit = PLANE * PLANE
    col = d_model // N_COL
    any_spec, vmem_spec = pl.BlockSpec(memory_space=pl.ANY), pl.BlockSpec(memory_space=pltpu.VMEM)
    tile = d_model // n_wx
    unit_b = (PLANE * SUB + head_dim, tile)
    wa_shape = (n_unit // 2, 2, (PLANE + 1) * tile, tile)
    wb_shape = (n_unit // 2, 2) + unit_b
    piece = (seq, col)
    n_piece = 4 * N_COL
    dma = pltpu.SemaphoreType.DMA
    cache = (seq, head_dim) if first else (2, seq, head_dim)
    out_shape = [jax.ShapeDtypeStruct(shape, jnp.bfloat16) for shape in (resid.shape, cache, cache)]
    n_plane, n_swap, n_hop = dma((40,)), dma((11,)), dma((13,))
    if first:
        out_shape += [jax.ShapeDtypeStruct(shape, jnp.bfloat16) for shape in (wa_shape, unit_b)]
        scratch = [n_plane, n_plane, n_swap, n_swap, n_swap, n_swap, n_plane, n_plane]
    else:
        scratch = [dma((2,)), dma((2,))]
    scratch += [
        pltpu.VMEM((n_wx, seq, d_model), jnp.bfloat16),
        pltpu.VMEM(wa_shape, jnp.bfloat16),
        pltpu.VMEM(wb_shape, jnp.bfloat16),
        pltpu.VMEM((n_wx, seq, n_unit // 2 * SUB + 2 * head_dim), jnp.bfloat16),
        pltpu.VMEM((n_wx, seq, 4 * head_dim), jnp.bfloat16),
        pltpu.VMEM((3, 2, 2, seq, head_dim), jnp.bfloat16),
        n_hop, n_hop, n_plane, n_plane, dma((4,)),
        pltpu.VMEM((N_COL,) + piece, jnp.float32),
        pltpu.VMEM((n_piece,) + piece, jnp.float32),
        pltpu.VMEM((n_piece,) + piece, jnp.float32),
        pltpu.VMEM((N_RING,) + piece, jnp.float32),
        dma((n_piece,)), dma((n_piece,)), dma((N_RING,)), dma((N_RING,)),
    ]
    return pl.pallas_call(
        functools.partial(layer_kernel, n_wx, first),
        out_shape=tuple(out_shape),
        in_specs=[vmem_spec] * 4 + [any_spec] * len(weights),
        out_specs=[vmem_spec] + [any_spec] * (len(out_shape) - 1),
        scratch_shapes=scratch,
        compiler_params=pltpu.CompilerParams(collective_id=int(first), has_side_effects=True, vmem_limit_bytes=VMEM_LIMIT),
        name='layer_0' if first else 'layer_1',
    )(resid, gamma, cos, sin, *weights)


def solution(mesh):
    batch_axes = ('dp', 'wy', 'wx')
    in_specs = (P(batch_axes), P(), P(None, 'wx', 'wy'), P(None, 'wx'), P(None, 'wx', None, 'wy'), P(None, 'wy', 'wx'), P(None, 'wy', 'wx'))
    out_specs = (P(batch_axes), P(None, batch_axes), P(None, batch_axes))
    n_wx = mesh.shape['wx']

    def device_step(x_tokens, gamma_ln, w_q, w_kv, w_gu, w_o, w_d):
        n_layers, d_loc = w_q.shape[:2]
        cos_tab, sin_tab = rope_tables(x_tokens.shape[1], w_kv.shape[-1])
        kv_half = lax.dynamic_index_in_dim(w_kv, lax.rem(lax.axis_index('wy'), 2), axis=2, keepdims=False)
        gu = jnp.transpose(w_gu.reshape(n_layers, d_loc, 2, n_wx // 2, SUB), (0, 3, 1, 2, 4)).reshape(n_layers, n_wx // 2, d_loc, 2 * SUB)
        resid, k_0, v_0, wa, unit_b = layer(x_tokens[0], gamma_ln, cos_tab, sin_tab, (gu, w_d, w_q, kv_half, w_o), n_wx, True)
        resid, k_all, v_all = layer(resid, gamma_ln, cos_tab, sin_tab, (wa, unit_b, k_0, v_0), n_wx, False)
        return resid[None], k_all[:, None], v_all[:, None]

    return jax.shard_map(device_step, mesh=mesh, in_specs=in_specs, out_specs=out_specs, check_vma=False)
```

```python
import functools

import jax
import jax.numpy as jnp
from jax import lax
from jax.experimental import pallas as pl
from jax.experimental.pallas import tpu as pltpu
from jax.sharding import PartitionSpec as P

LN_EPS = 1e-6
ROPE_BASE = 10000.0
MESH = pl.DeviceIdType.MESH
VMEM_LIMIT = 67043328
PLANE = 4
SUB = 64
N_COL = 4
N_RING = 12


def rope_tables(seq_len, head_dim):
    half_dim = head_dim // 2
    inv_freq = ROPE_BASE ** (-2.0 * jnp.arange(half_dim, dtype=jnp.float32) / head_dim)
    angles = jnp.arange(seq_len, dtype=jnp.float32)[:, None] * inv_freq[None, :]
    cos, sin = jnp.cos(angles), jnp.sin(angles)
    return jnp.concatenate([cos, cos], axis=1), jnp.concatenate([-sin, sin], axis=1)


def remote(src, dst, send, recv, target):
    return pltpu.make_async_remote_copy(src_ref=src, dst_ref=dst, send_sem=send, recv_sem=recv, device_id=target, device_id_type=MESH)


class Ring:
    def __init__(self, n_wx):
        self.me = lax.axis_index('wx')
        self.chip, self.core = lax.div(self.me, 2), lax.rem(self.me, 2)
        self.n_chip = n_wx // 2
        self.right, self.left, self.far = self.at(1), self.at(self.n_chip - 1), self.at(2)
        self.pair = self.at(0, 1)

    def at(self, step, other=0):
        return lax.rem(self.chip + step, self.n_chip) * 2 + lax.rem(self.core + other, 2)


class ChipGather:
    def __init__(self, ring, hall, send_sem, recv_sem):
        half = hall.shape[1] // 2
        top, bottom, whole = pl.ds(0, half), pl.ds(half, half), pl.ds(0, 2 * half)
        me, left, right, far, pair = ring.me, ring.left, ring.right, ring.far, ring.pair
        moves = [
            (me, whole, pair, pair),
            (me, top, right, left), (me, bottom, left, right),
            (me, bottom, right, left), (me, top, left, right),
            (left, top, right, far), (right, bottom, left, far),
            (left, top, pair, ring.at(ring.n_chip - 1, 1)), (right, bottom, pair, ring.at(1, 1)),
            (left, bottom, pair, ring.at(ring.n_chip - 1, 1)), (right, top, pair, ring.at(1, 1)),
            (far, top, pair, ring.at(2, 1)), (far, bottom, pair, ring.at(2, 1)),
        ]
        self.sends, self.lands = [], []
        for num, (block, rows, target, landed) in enumerate(moves):
            for kept, there in ((self.sends, block), (self.lands, landed)):
                ref = hall.at[there, rows]
                kept.append(remote(ref, ref, send_sem.at[num], recv_sem.at[num], {'wx': target}))
        self.first = 5

    def start(self):
        for copy in self.sends[:self.first]:
            copy.start()

    def relay(self, landed, *sent):
        self.lands[landed].wait_recv()
        for num in sent:
            self.sends[num].start()

    def near_halves(self):
        self.relay(1, 5, 7)
        self.relay(2, 6, 8)

    def near_rest(self):
        self.relay(3, 9)
        self.relay(4, 10)

    def far_halves(self):
        self.relay(5, 11)
        self.relay(6, 12)

    def wait(self, *nums):
        for num in nums:
            self.lands[num].wait_recv()

    def drain(self):
        for copy in self.sends:
            copy.wait_send()


class PlaneGather:
    ways = [(half, sign) for half in range(2) for sign in (1, -1)]

    def __init__(self, buf, send_sem, recv_sem):
        self.buf, self.send_sem, self.recv_sem = buf, send_sem, recv_sem
        self.here = lax.axis_index('wy')
        self.pos = (lax.div(self.here, PLANE), lax.rem(self.here, PLANE))

    def at(self, half, first, second=0):
        step_z, step_y = (second, first) if half == 0 else (first, second)
        z, y = self.pos
        return lax.rem(z + step_z + PLANE, PLANE) * PLANE + lax.rem(y + step_y + PLANE, PLANE)

    def neighbours(self):
        return [{'wy': self.at(half, sign)} for half, sign in self.ways]

    def place(self, block, start, size):
        return self.buf.at[block, pl.ds(start, size)]

    def copy(self, kind, num, block, half, quarter, target):
        rows = self.buf.shape[1]
        size = rows // 2 if quarter is None else rows // PLANE
        ref = self.place(block, half * (rows // 2) + (quarter or 0) * size, size)
        slot = kind * PLANE + num
        return remote(ref, ref, self.send_sem.at[slot], self.recv_sem.at[slot], {'wy': target})

    def one(self, half, sign, landing=False):
        block = self.at(half, -sign if landing else 0)
        return self.copy(0, half * 2 + (sign < 0), block, half, None, self.at(half, sign))

    def two(self, half, sign, landing=False):
        block = self.at(half, -2 * sign if landing else -sign)
        return self.copy(1, half * 2 + (sign < 0), block, half, int(sign < 0), self.at(half, sign))

    def three(self, half, off, sign, landing=False):
        block = self.at(half, off, -sign if landing else 0)
        return self.copy(2, (half * PLANE + off % PLANE) * 2 + (sign < 0), block, half, None, self.at(half, 0, sign))

    def four(self, half, off, sign, landing=False):
        block = self.at(half, off, -2 * sign if landing else -sign)
        return self.copy(6, (half * PLANE + off % PLANE) * 2 + (sign < 0), block, half, int(sign < 0), self.at(half, 0, sign))

    def start(self):
        for half, sign in self.ways:
            self.one(half, sign).start()
        for half, sign in self.ways:
            self.three(half, 0, sign).start()

    def stage_1(self):
        for half, sign in self.ways:
            self.one(half, sign, True).wait_recv()
            self.two(half, sign).start()
        for half, sign in self.ways:
            for way in (1, -1):
                self.three(half, -sign, way).start()

    def fourth(self, off):
        for half, sign in self.ways:
            self.three(half, off, sign, True).wait_recv()
            self.four(half, off, sign).start()

    def stage_2(self):
        self.fourth(0)

    def stage_3(self):
        for half, sign in self.ways:
            self.two(half, sign, True).wait_recv()
        for half, sign in self.ways:
            self.three(half, 2, sign).start()

    def stage_4(self):
        self.fourth(1)
        self.fourth(-1)

    def stage_5(self):
        self.fourth(2)

    def each(self, call):
        for half, sign in self.ways:
            for off in (0, 1, -1, 2):
                call(half, off, sign)

    def finish(self):
        self.each(lambda half, off, sign: self.four(half, off, sign, True).wait_recv())

    def drain(self):
        for half, sign in self.ways:
            self.one(half, sign).wait_send()
            self.two(half, sign).wait_send()
        self.each(lambda half, off, sign: self.three(half, off, sign).wait_send())
        self.each(lambda half, off, sign: self.four(half, off, sign).wait_send())


class Exchange:
    def __init__(self, ring, layer, shards, at_a, at_b, send_sem, recv_sem):
        self.me, self.n_wx = ring.me, ring.n_chip * 2
        self.pos = pos = lax.axis_index('wy')
        self.head_to = {'wy': lax.rem(pos, 2) * self.n_wx + self.turn(self.me), 'wx': lax.div(pos, 2)}
        self.head_from = {'wy': 2 * self.me + lax.div(pos, self.n_wx), 'wx': self.turn(lax.rem(pos, self.n_wx))}
        self.layer, self.shards = layer, shards
        self.at_a, self.at_b = at_a, at_b
        self.send_sem, self.recv_sem = send_sem, recv_sem

    def turn(self, w):
        return lax.rem(w + self.n_wx // 2, self.n_wx)

    def others(self):
        return [lax.rem(self.me + step, self.n_wx) for step in (4, 5, 3, 2, 6, 7, 1)]

    def peers(self):
        return [{'wx': other} for other in self.others()] + [self.head_from]

    def block(self, which, to, origin):
        gu, d = self.shards[:2]
        if which:
            src, place, rows = d.at[self.layer, pl.ds(pl.multiple_of(to * SUB, SUB), SUB)], self.at_b, SUB
        else:
            src, place, rows = gu.at[self.layer, to], self.at_a, gu.shape[2]
        return src, place(self.pos, pl.multiple_of(origin * rows, rows), rows)

    def kept(self, which):
        return pltpu.make_async_copy(*self.block(which, self.me, self.me), self.send_sem.at[which * self.n_wx + self.me])

    def copies(self, which, landing=False):
        base = which * self.n_wx
        found = []
        for other in self.others():
            origin = other if landing else self.me
            src, dst = self.block(which, other, origin)
            found.append(remote(src, dst, self.send_sem.at[base + other], self.recv_sem.at[base + origin], {'wx': other}))
        gu, d, q, kv, o = self.shards
        unit = self.pos if landing else self.head_to['wy']
        base = self.n_wx * 2 + which * 2
        if which:
            parts = [(o, self.at_b(unit, self.n_wx * SUB, o.shape[1]))]
        else:
            parts = [(src, self.at_a(unit, (self.n_wx + num) * q.shape[1], q.shape[1])) for num, src in enumerate((q, kv))]
        for num, (src, dst) in enumerate(parts):
            found.append(remote(src.at[self.layer], dst, self.send_sem.at[base + num], self.recv_sem.at[base + num], self.head_to))
        return found

    def start(self, which):
        self.kept(which).start()
        for copy in self.copies(which):
            copy.start()

    def land(self, which):
        for copy in self.copies(which, True):
            copy.wait_recv()
        self.kept(which).wait()

    def drain(self, which):
        for copy in self.copies(which):
            copy.wait_send()


def up_step(hall, wa, mo, narrow, chunks, between):
    d_model = hall.shape[2]
    half = hall.shape[1] // 2
    n_unit, tile = wa.shape[0], wa.shape[2]
    n_w = n_unit // 2
    rows = [(prompt, pl.ds(pl.multiple_of(start, half), half)) for prompt, start in chunks]
    h = jnp.concatenate([hall[prompt, part] for prompt, part in rows], axis=0)
    low = lax.broadcasted_iota(jnp.int32, (h.shape[0], tile), 1) < SUB

    def project(weight):
        return jnp.dot(h, weight, preferred_element_type=jnp.float32).astype(jnp.bfloat16)

    def keep(value, ref, lo):
        for num, (prompt, part) in enumerate(rows):
            ref[prompt, part, lo:lo + value.shape[1]] = value[num * half:(num + 1) * half]

    for hh in range(2):
        sides = []
        for num in range(2):
            lo = d_model + num * d_model // n_w
            parts = [wa[hh * n_w + k:hh * n_w + k + n_w // 2, lo:lo + d_model // n_w, :].reshape(d_model // 2, tile) for k in (n_w // 2, 0)]
            sides.append(jnp.concatenate(parts, axis=0))
        keep(project(jnp.concatenate(sides, axis=1)), narrow, hh * 2 * tile)
    for first in range(0, n_unit, PLANE):
        if first == n_w:
            between()
        both = project(jnp.concatenate([wa[first + k, :d_model, :] for k in range(PLANE)], axis=1))
        for k in range(0, PLANE, 2):
            one, two = (both[:, part * tile:(part + 1) * tile].astype(jnp.float32) for part in (k, k + 1))
            g_f = jnp.where(low, one, pltpu.roll(two, SUB, 1))
            u_f = jnp.where(low, pltpu.roll(one, SUB, 1), two)
            hidden = g_f * (1.0 / (1.0 + jnp.exp(-g_f))) * u_f
            keep(hidden.astype(jnp.bfloat16), mo, (first + k) * SUB)


def attend(narrow, mo, kv_out, xt, cos, sin):
    seq, head_dim = cos.shape
    tile = 2 * head_dim

    def rot(val):
        val_f = val.astype(jnp.float32)
        return (val_f * cos + pltpu.roll(val_f, head_dim // 2, 1) * sin).astype(jnp.bfloat16)

    allowed = lax.broadcasted_iota(jnp.int32, (seq, seq), 0) >= lax.broadcasted_iota(jnp.int32, (seq, seq), 1)
    for b in range(2):
        prompt = xt * 2 + b
        k_rot = rot(narrow[prompt, :, head_dim:tile])
        v_val = narrow[prompt, :, tile + head_dim:]
        kv_out[b, 0] = k_rot
        kv_out[b, 1] = v_val
        for hh in range(2):
            q_rot = rot(narrow[prompt, :, hh * tile:hh * tile + head_dim])
            scores = lax.dot_general(q_rot, k_rot, (((1,), (1,)), ((), ())), preferred_element_type=jnp.float32) * head_dim ** -0.5
            scores = jnp.where(allowed, scores, -jnp.inf)
            expd = jnp.exp(scores - jnp.max(scores, axis=-1, keepdims=True))
            probs = (expd / jnp.sum(expd, axis=-1, keepdims=True)).astype(jnp.bfloat16)
            att = jnp.dot(probs, v_val, preferred_element_type=jnp.float32)
            lo = mo.shape[2] - (2 - hh) * head_dim
            mo[prompt, :, lo:lo + head_dim] = att.astype(jnp.bfloat16)


class Scatter:
    def __init__(self, ring, first, mo, wb, given, taken, acc, landed, pair_send, pair_recv, ring_send, ring_recv):
        self.ring, self.first = ring, first
        self.mo, self.wb, self.given, self.taken, self.acc, self.landed = mo, wb, given, taken, acc, landed
        self.pair_send, self.pair_recv, self.ring_send, self.ring_recv = pair_send, pair_recv, ring_send, ring_recv

    def piece(self, n):
        if self.first:
            return n
        return jnp.where(n < N_COL, n + N_COL, jnp.where(n < 2 * N_COL, n - N_COL, n))

    def pair_copy(self, n):
        k, slot = self.piece(n), lax.rem(n, N_COL)
        return remote(self.given.at[slot], self.taken.at[k], self.pair_send.at[k], self.pair_recv.at[k], {'wx': self.ring.pair})

    def ring_copy(self, k):
        target = jnp.where(lax.rem(k, 2) == 0, self.ring.right, self.ring.left)
        return remote(self.acc.at[k], self.landed.at[k], self.ring_send.at[k], self.ring_recv.at[k], {'wx': target})

    def products(self, k):
        n_unit, rows, tile = self.wb.shape
        n_w = n_unit // 2
        phase, j = lax.div(k, N_COL), lax.rem(k, N_COL)
        odd, slot = lax.rem(j, 2), lax.div(j, 2)
        own = phase == 3
        off = jnp.where(phase == 0, 2, jnp.where(own, 0, 1 + 2 * odd))
        q = jnp.where(own, j, jnp.where(phase == 1, 1 - odd, odd) * 2 + slot)
        xt = lax.rem(self.ring.chip + off, self.ring.n_chip)

        def columns(w):
            parts = [self.wb[:, pl.ds(pl.multiple_of(w * SUB, SUB), SUB), :].reshape(n_unit * SUB, tile)]
            for hh in range(2):
                parts.append(self.wb[hh * n_w + lax.rem(w + n_w // 2, n_w), n_w * SUB:, :])
            return jnp.concatenate(parts, axis=0)

        weight = jnp.concatenate([columns(2 * q), columns(2 * q + 1)], axis=1)

        def product(core):
            return jnp.dot(self.mo[xt * 2 + core], weight, preferred_element_type=jnp.float32)

        return product

    def combine(self, n):
        k = self.piece(n)
        self.pair_copy(n).wait_recv()
        self.acc[k] = self.acc[k] + self.taken[k]

    def send(self, n):
        k = self.piece(n)

        @pl.when(k < 2 * N_COL)
        def _():
            self.ring_copy(k).start()

    def run(self, lo, hi):
        def body(n, carry):
            product = self.products(self.piece(n))

            @pl.when(n >= N_COL)
            def _():
                self.pair_copy(n - N_COL).wait_send()

            self.given[lax.rem(n, N_COL)] = product(1 - self.ring.core)

            @pl.when(n > lo)
            def _():
                self.combine(n - 1)

            self.acc[self.piece(n)] = product(self.ring.core)
            self.pair_copy(n).start()

            @pl.when(n > lo)
            def _():
                self.send(n - 1)

            return carry

        lax.fori_loop(lo, hi, body, 0)

        @pl.when(hi > lo)
        def _():
            self.combine(hi - 1)
            self.send(hi - 1)

    def finish(self, resid_ref, out_ref, beside):
        col = self.acc.shape[2]
        own = 3 * N_COL
        for pair in range(2):
            for odd in range(2):
                k = 2 * (N_COL + pair) + odd
                self.ring_copy(k - 2 * N_COL).wait_recv()
                self.acc[k] = self.acc[k] + self.landed[k - 2 * N_COL]
            for q in (pair, pair + 2):
                self.acc[own + q] = self.acc[own + q] + resid_ref[:, q * col:(q + 1) * col].astype(jnp.float32)
            for odd in range(2):
                self.ring_copy(2 * (N_COL + pair) + odd).start()
            beside[pair]()
        for pair in range(2):
            for k in (N_COL + 2 * pair, N_COL + 2 * pair + 1):
                self.ring_copy(k).wait_recv()
            beside[2 + pair]()
        for pair in range(2):
            for q, raw, comb in ((pair, 5, 8), (pair + 2, 4, 9)):
                raw, comb = raw + 2 * pair, comb + 2 * pair
                self.ring_copy(comb).wait_recv()
                out_ref[:, q * col:(q + 1) * col] = (self.acc[own + q] + (self.landed[raw] + self.landed[comb])).astype(jnp.bfloat16)
        for n in range(own, own + N_COL):
            self.pair_copy(n).wait_send()
        for k in range(N_RING):
            self.ring_copy(k).wait_send()


def layer_kernel(n_wx, first, *refs):
    if first:
        (resid_ref, gamma_ref, cos_ref, sin_ref, gu_ref, d_ref, q_ref, kv_ref, o_ref, out_ref, k_out, v_out, next_a, next_b,
         next_send, next_recv, x0_send, x0_recv, x1_send, x1_recv, a_send, a_recv, *rest) = refs
    else:
        resid_ref, gamma_ref, cos_ref, sin_ref, wa_ref, b_ref, k_ref, v_ref, out_ref, k_out, v_out, w_sem, old_sem, *rest = refs
    hall, wa, wb, mo, narrow, kv, h_send, h_recv, b_send, b_recv, kv_sem, *parts = rest
    ring = Ring(n_wx)
    gather_h = ChipGather(ring, hall, h_send, h_recv)
    gather_b = PlaneGather(wb, b_send, b_recv)
    scatter = Scatter(ring, first, mo, wb, *parts)
    peers = [{'wx': ring.right}, {'wx': ring.left}, {'wx': ring.pair}] + gather_b.neighbours()
    if first:
        shards = gu_ref, d_ref, q_ref, kv_ref, o_ref
        gather_a = PlaneGather(wa, a_send, a_recv)
        gather_n = PlaneGather(next_a, next_send, next_recv)
        swap_0 = Exchange(ring, 0, shards, gather_a.place, gather_b.place, x0_send, x0_recv)
        swap_1 = Exchange(ring, 1, shards, gather_n.place, lambda unit, start, size: next_b.at[pl.ds(start, size)], x1_send, x1_recv)
        peers += swap_0.peers()
    else:
        here = gather_b.here
        b_load = pltpu.make_async_copy(b_ref, wb.at[here], w_sem.at[0])
        a_load = pltpu.make_async_copy(wa_ref, wa, w_sem.at[1])
        old_loads = [pltpu.make_async_copy(ref, kv.at[2, 0, num], old_sem.at[num]) for num, ref in enumerate((k_ref, v_ref))]
        for load in (b_load, a_load, *old_loads):
            load.start()
    barrier = pltpu.get_barrier_semaphore()
    for peer in peers:
        pl.semaphore_signal(barrier, inc=1, device_id=peer, device_id_type=MESH)

    resid_f = resid_ref[...].astype(jnp.float32)
    centered = resid_f - jnp.mean(resid_f, axis=-1, keepdims=True)
    variance = jnp.mean(centered * centered, axis=-1, keepdims=True)
    normed = (centered * lax.rsqrt(variance + LN_EPS) * gamma_ref[1 - first:2 - first, :]).astype(jnp.bfloat16)
    hall[ring.me] = normed
    pl.semaphore_wait(barrier, len(peers))
    if first:
        swap_0.start(0)
        gather_h.start()
        swap_0.land(0)
        gather_a.start()
        swap_0.start(1)
        gather_a.stage_1()
        gather_h.near_halves()
        gather_a.stage_2()
        gather_a.stage_3()
        gather_h.near_rest()
        swap_1.start(0)
        swap_1.start(1)
        gather_a.stage_4()
        gather_h.far_halves()
        gather_a.stage_5()
        swap_0.land(1)
        gather_b.start()
        gather_h.wait(0, 7, 8, 9, 10, 11, 12)
        gather_a.finish()
    else:
        gather_h.start()
        b_load.wait()
        gather_b.start()
        a_load.wait()

    seq = hall.shape[1]
    half = seq // 2

    def body(step, carry):
        turn = lax.rem(step + 1, PLANE) if first else step

        def when(num, *calls):
            @pl.when(step == num)
            def _():
                for call in calls:
                    call()

        if first:
            when(1, gather_b.stage_1)
            when(2, gather_b.stage_3)
        else:
            when(0, lambda: gather_h.wait(0))
            when(1, gather_b.stage_1, gather_h.near_halves, gather_b.stage_2, lambda: gather_h.wait(7, 8))
            when(2, gather_b.stage_3, gather_h.near_rest, gather_b.stage_4, lambda: gather_h.wait(9, 10))
            when(3, gather_h.far_halves, lambda: gather_h.wait(11, 12))

        def between():
            if first:
                when(1, gather_b.stage_2)
                when(2, gather_b.stage_4)
                when(3, gather_n.stage_1)
            else:
                when(2, gather_b.stage_5)

        near = (turn == 1) | (turn == 2)
        lone = jnp.where(turn == 0, ring.chip, lax.rem(ring.chip + 2, ring.n_chip))
        one = jnp.where(near, lax.div(ring.left, 2), lone)
        two = jnp.where(near, lax.div(ring.right, 2), lone)
        start = jnp.where(turn == 2, half, 0)
        up_step(hall, wa, mo, narrow, [(one * 2 + b, start) for b in range(2)] + [(two * 2 + b, half - start) for b in range(2)], between)

        def attention(num, carry):
            place = lax.rem(num + 1, PLANE) if first else num
            off = jnp.where(place == 0, 0, jnp.where(place == 1, 3, jnp.where(place == 2, 1, 2)))
            attend(narrow, mo, kv.at[jnp.where(place == 0, 0, 1)], lax.rem(ring.chip + off, ring.n_chip), cos_ref[...], sin_ref[...])
            return carry

        early = 0 if first else 1
        lo = jnp.where(step == 3, 3, jnp.where(step == 2, 2 - early, 0))
        if first:
            hi = jnp.where(step == 0, 0, step + 1)
            lo = jnp.where(step == 2, 2, lo)
        else:
            lo, hi = jnp.where(step == 1, 1, lo), jnp.where(step < 2, 1, step + 1)
        lax.fori_loop(lo, hi, attention, 0)
        if first:
            when(2, gather_b.stage_5, gather_b.finish, lambda: swap_1.land(0), gather_n.start)
        else:
            when(2, gather_b.finish)
        split = 2 * N_COL if first else N_COL
        last = step == 3
        scatter.run(jnp.where(last, split, 0), jnp.where(last, 4 * N_COL, jnp.where(step == 2, split, 0)))
        return carry

    lax.fori_loop(0, ring.n_chip, body, 0)
    if first:
        caches = [(kv.at[0, ring.core, num], ref) for num, ref in enumerate((k_out, v_out))]
    else:
        for load in old_loads:
            load.wait()
        caches = [(kv.at[0, ring.core, num], ref.at[1]) for num, ref in enumerate((k_out, v_out))]
        caches += [(kv.at[2, 0, num], ref.at[0]) for num, ref in enumerate((k_out, v_out))]
    caches = [pltpu.make_async_copy(src, dst, kv_sem.at[num]) for num, (src, dst) in enumerate(caches)]
    for cache in caches:
        cache.start()
    if first:
        scatter.finish(resid_ref, out_ref, (gather_n.stage_2, gather_n.stage_3, gather_n.stage_4, gather_n.stage_5))
        gather_n.finish()
        swap_1.land(1)
        for swap in (swap_0, swap_1):
            swap.drain(0)
            swap.drain(1)
        gather_a.drain()
        gather_n.drain()
    else:
        scatter.finish(resid_ref, out_ref, [lambda: None] * 4)
    gather_b.drain()
    gather_h.drain()
    for cache in caches:
        cache.wait()


def layer(resid, gamma, cos, sin, weights, n_wx, first):
    seq, d_model = resid.shape
    head_dim = cos.shape[1]
    n_unit = PLANE * PLANE
    col = d_model // N_COL
    any_spec, vmem_spec = pl.BlockSpec(memory_space=pl.ANY), pl.BlockSpec(memory_space=pltpu.VMEM)
    tile = d_model // n_wx
    unit_b = (n_wx * SUB + head_dim, tile)
    wa_shape = (n_unit, d_model + 2 * tile, 2 * SUB)
    wb_shape = (n_unit,) + unit_b
    piece = (seq, col)
    n_piece = 4 * N_COL
    dma = pltpu.SemaphoreType.DMA
    cache = (seq, head_dim) if first else (2, seq, head_dim)
    out_shape = [jax.ShapeDtypeStruct(shape, jnp.bfloat16) for shape in (resid.shape, cache, cache)]
    n_plane, n_swap, n_hop = dma((40,)), dma((19,)), dma((13,))
    if first:
        out_shape += [jax.ShapeDtypeStruct(shape, jnp.bfloat16) for shape in (wa_shape, unit_b)]
        scratch = [n_plane, n_plane, n_swap, n_swap, n_swap, n_swap, n_plane, n_plane]
    else:
        scratch = [dma((2,)), dma((2,))]
    scratch += [
        pltpu.VMEM((n_wx, seq, d_model), jnp.bfloat16),
        pltpu.VMEM(wa_shape, jnp.bfloat16),
        pltpu.VMEM(wb_shape, jnp.bfloat16),
        pltpu.VMEM((n_wx, seq, n_unit * SUB + 2 * head_dim), jnp.bfloat16),
        pltpu.VMEM((n_wx, seq, 4 * head_dim), jnp.bfloat16),
        pltpu.VMEM((3, 2, 2, seq, head_dim), jnp.bfloat16),
        n_hop, n_hop, n_plane, n_plane, dma((4,)),
        pltpu.VMEM((N_COL,) + piece, jnp.float32),
        pltpu.VMEM((n_piece,) + piece, jnp.float32),
        pltpu.VMEM((n_piece,) + piece, jnp.float32),
        pltpu.VMEM((N_RING,) + piece, jnp.float32),
        dma((n_piece,)), dma((n_piece,)), dma((N_RING,)), dma((N_RING,)),
    ]
    return pl.pallas_call(
        functools.partial(layer_kernel, n_wx, first),
        out_shape=tuple(out_shape),
        in_specs=[vmem_spec] * 4 + [any_spec] * len(weights),
        out_specs=[vmem_spec] + [any_spec] * (len(out_shape) - 1),
        scratch_shapes=scratch,
        compiler_params=pltpu.CompilerParams(collective_id=int(first), has_side_effects=True, vmem_limit_bytes=VMEM_LIMIT),
        name='layer_0' if first else 'layer_1',
    )(resid, gamma, cos, sin, *weights)


def settle_kernel(*refs):
    n = len(refs) // 3
    srcs, dsts, held, sem = refs[:n], refs[n:2 * n], refs[2 * n:3 * n], refs[-1]
    loads = [pltpu.make_async_copy(src, mid, sem.at[num]) for num, (src, mid) in enumerate(zip(srcs, held))]
    stores = [pltpu.make_async_copy(mid, dst, sem.at[n + num]) for num, (mid, dst) in enumerate(zip(held, dsts))]
    for load in loads:
        load.start()
    for load, store in zip(loads, stores):
        load.wait()
        store.start()
    for store in stores:
        store.wait()


def settle(arrays):
    n = len(arrays)
    return pl.pallas_call(
        settle_kernel,
        out_shape=tuple(jax.ShapeDtypeStruct(a.shape, a.dtype) for a in arrays),
        in_specs=[pl.BlockSpec(memory_space=pl.ANY)] * n,
        out_specs=[pl.BlockSpec(memory_space=pl.ANY)] * n,
        scratch_shapes=[pltpu.VMEM(a.shape, a.dtype) for a in arrays] + [pltpu.SemaphoreType.DMA((2 * n,))],
        name='settle',
    )(*arrays)


def solution(mesh):
    batch_axes = ('dp', 'wy', 'wx')
    in_specs = (P(batch_axes), P(), P(None, 'wx', 'wy'), P(None, 'wx'), P(None, 'wx', None, 'wy'), P(None, 'wy', 'wx'), P(None, 'wy', 'wx'))
    out_specs = (P(batch_axes), P(None, batch_axes), P(None, batch_axes))
    n_wx = mesh.shape['wx']

    def device_step(x_tokens, gamma_ln, w_q, w_kv, w_gu, w_o, w_d):
        n_layers, d_loc = w_q.shape[:2]
        cos_tab, sin_tab = rope_tables(x_tokens.shape[1], w_kv.shape[-1])
        kv_half = lax.dynamic_index_in_dim(w_kv, lax.rem(lax.axis_index('wy'), 2), axis=2, keepdims=False)
        gu = jnp.transpose(w_gu.reshape(n_layers, d_loc, 2, n_wx, SUB), (0, 3, 1, 2, 4)).reshape(n_layers, n_wx, d_loc, 2 * SUB)
        resid, k_0, v_0, wa, unit_b = layer(x_tokens[0], gamma_ln, cos_tab, sin_tab, (gu, w_d, w_q, kv_half, w_o), n_wx, True)
        resid, k_all, v_all = settle(layer(resid, gamma_ln, cos_tab, sin_tab, (wa, unit_b, k_0, v_0), n_wx, False))
        return resid[None], k_all[:, None], v_all[:, None]

    return jax.shard_map(device_step, mesh=mesh, in_specs=in_specs, out_specs=out_specs, check_vma=False)
```

```python
import functools

import jax
import jax.numpy as jnp
from jax import lax
from jax.experimental import pallas as pl
from jax.experimental.pallas import tpu as pltpu
from jax.sharding import PartitionSpec as P

LN_EPS = 1e-6
ROPE_BASE = 10000.0
MESH = pl.DeviceIdType.MESH
VMEM_LIMIT = 67043328
PLANE = 4
SUB = 64
N_COL = 4
N_RING = 12


def rope_tables(seq_len, head_dim):
    half_dim = head_dim // 2
    inv_freq = ROPE_BASE ** (-2.0 * jnp.arange(half_dim, dtype=jnp.float32) / head_dim)
    angles = jnp.arange(seq_len, dtype=jnp.float32)[:, None] * inv_freq[None, :]
    cos, sin = jnp.cos(angles), jnp.sin(angles)
    return jnp.concatenate([cos, cos], axis=1), jnp.concatenate([-sin, sin], axis=1)


def remote(src, dst, send, recv, target):
    return pltpu.make_async_remote_copy(src_ref=src, dst_ref=dst, send_sem=send, recv_sem=recv, device_id=target, device_id_type=MESH)


class Ring:
    def __init__(self, n_wx):
        self.me = lax.axis_index('wx')
        self.chip, self.core = lax.div(self.me, 2), lax.rem(self.me, 2)
        self.n_chip = n_wx // 2
        self.right, self.left, self.far = self.at(1), self.at(self.n_chip - 1), self.at(2)
        self.pair = self.at(0, 1)

    def at(self, step, other=0):
        return lax.rem(self.chip + step, self.n_chip) * 2 + lax.rem(self.core + other, 2)


class ChipGather:
    def __init__(self, ring, hall, send_sem, recv_sem):
        half = hall.shape[1] // 2
        top, bottom, whole = pl.ds(0, half), pl.ds(half, half), pl.ds(0, 2 * half)
        me, left, right, far, pair = ring.me, ring.left, ring.right, ring.far, ring.pair
        moves = [
            (me, whole, pair, pair),
            (me, top, right, left), (me, bottom, left, right),
            (me, bottom, right, left), (me, top, left, right),
            (left, top, right, far), (right, bottom, left, far),
            (left, top, pair, ring.at(ring.n_chip - 1, 1)), (right, bottom, pair, ring.at(1, 1)),
            (left, bottom, pair, ring.at(ring.n_chip - 1, 1)), (right, top, pair, ring.at(1, 1)),
            (far, top, pair, ring.at(2, 1)), (far, bottom, pair, ring.at(2, 1)),
        ]
        self.sends, self.lands = [], []
        for num, (block, rows, target, landed) in enumerate(moves):
            for kept, there in ((self.sends, block), (self.lands, landed)):
                ref = hall.at[there, rows]
                kept.append(remote(ref, ref, send_sem.at[num], recv_sem.at[num], {'wx': target}))
        self.first = 5

    def start(self):
        for copy in self.sends[:self.first]:
            copy.start()

    def relay(self, landed, *sent):
        self.lands[landed].wait_recv()
        for num in sent:
            self.sends[num].start()

    def near_halves(self):
        self.relay(1, 5, 7)
        self.relay(2, 6, 8)

    def near_rest(self):
        self.relay(3, 9)
        self.relay(4, 10)

    def far_halves(self):
        self.relay(5, 11)
        self.relay(6, 12)

    def wait(self, *nums):
        for num in nums:
            self.lands[num].wait_recv()

    def drain(self):
        for copy in self.sends:
            copy.wait_send()


class PlaneGather:
    ways = [(half, sign) for half in range(2) for sign in (1, -1)]

    def __init__(self, buf, send_sem, recv_sem):
        self.buf, self.send_sem, self.recv_sem = buf, send_sem, recv_sem
        self.here = lax.axis_index('wy')
        self.pos = (lax.div(self.here, PLANE), lax.rem(self.here, PLANE))

    def at(self, half, first, second=0):
        step_z, step_y = (second, first) if half == 0 else (first, second)
        z, y = self.pos
        return lax.rem(z + step_z + PLANE, PLANE) * PLANE + lax.rem(y + step_y + PLANE, PLANE)

    def neighbours(self):
        return [{'wy': self.at(half, sign)} for half, sign in self.ways]

    def place(self, block, start, size):
        return self.buf.at[block, pl.ds(start, size)]

    def copy(self, kind, num, block, half, quarter, target):
        rows = self.buf.shape[1]
        size = rows // 2 if quarter is None else rows // PLANE
        ref = self.place(block, half * (rows // 2) + (quarter or 0) * size, size)
        slot = kind * PLANE + num
        return remote(ref, ref, self.send_sem.at[slot], self.recv_sem.at[slot], {'wy': target})

    def one(self, half, sign, landing=False):
        block = self.at(half, -sign if landing else 0)
        return self.copy(0, half * 2 + (sign < 0), block, half, None, self.at(half, sign))

    def two(self, half, sign, landing=False):
        block = self.at(half, -2 * sign if landing else -sign)
        return self.copy(1, half * 2 + (sign < 0), block, half, int(sign < 0), self.at(half, sign))

    def three(self, half, off, sign, landing=False):
        block = self.at(half, off, -sign if landing else 0)
        return self.copy(2, (half * PLANE + off % PLANE) * 2 + (sign < 0), block, half, None, self.at(half, 0, sign))

    def four(self, half, off, sign, landing=False):
        block = self.at(half, off, -2 * sign if landing else -sign)
        return self.copy(6, (half * PLANE + off % PLANE) * 2 + (sign < 0), block, half, int(sign < 0), self.at(half, 0, sign))

    def start(self):
        for half, sign in self.ways:
            self.one(half, sign).start()
        for half, sign in self.ways:
            self.three(half, 0, sign).start()

    def stage_1(self):
        for half, sign in self.ways:
            self.one(half, sign, True).wait_recv()
            self.two(half, sign).start()
        for half, sign in self.ways:
            for way in (1, -1):
                self.three(half, -sign, way).start()

    def fourth(self, off):
        for half, sign in self.ways:
            self.three(half, off, sign, True).wait_recv()
            self.four(half, off, sign).start()

    def stage_2(self):
        self.fourth(0)

    def stage_3(self):
        for half, sign in self.ways:
            self.two(half, sign, True).wait_recv()
        for half, sign in self.ways:
            self.three(half, 2, sign).start()

    def stage_4(self):
        self.fourth(1)
        self.fourth(-1)

    def stage_5(self):
        self.fourth(2)

    def each(self, call):
        for half, sign in self.ways:
            for off in (0, 1, -1, 2):
                call(half, off, sign)

    def finish(self):
        self.each(lambda half, off, sign: self.four(half, off, sign, True).wait_recv())

    def drain(self):
        for half, sign in self.ways:
            self.one(half, sign).wait_send()
            self.two(half, sign).wait_send()
        self.each(lambda half, off, sign: self.three(half, off, sign).wait_send())
        self.each(lambda half, off, sign: self.four(half, off, sign).wait_send())


class Exchange:
    def __init__(self, ring, layer, shards, at_a, at_b, send_sem, recv_sem):
        self.me, self.n_wx = ring.me, ring.n_chip * 2
        self.pos = pos = lax.axis_index('wy')
        self.head_to = {'wy': lax.rem(pos, 2) * self.n_wx + self.turn(self.me), 'wx': lax.div(pos, 2)}
        self.head_from = {'wy': 2 * self.me + lax.div(pos, self.n_wx), 'wx': self.turn(lax.rem(pos, self.n_wx))}
        self.layer, self.shards = layer, shards
        self.at_a, self.at_b = at_a, at_b
        self.send_sem, self.recv_sem = send_sem, recv_sem

    def turn(self, w):
        return lax.rem(w + self.n_wx // 2, self.n_wx)

    def others(self):
        return [lax.rem(self.me + step, self.n_wx) for step in (4, 5, 3, 2, 6, 7, 1)]

    def peers(self):
        return [{'wx': other} for other in self.others()] + [self.head_from]

    def block(self, which, to, origin):
        gu, d = self.shards[:2]
        if which:
            src, place, rows = d.at[self.layer, pl.ds(pl.multiple_of(to * SUB, SUB), SUB)], self.at_b, SUB
        else:
            src, place, rows = gu.at[self.layer, to], self.at_a, gu.shape[2]
        return src, place(self.pos, pl.multiple_of(origin * rows, rows), rows)

    def kept(self, which):
        return pltpu.make_async_copy(*self.block(which, self.me, self.me), self.send_sem.at[which * self.n_wx + self.me])

    def copies(self, which, landing=False):
        base = which * self.n_wx
        found = []
        for other in self.others():
            origin = other if landing else self.me
            src, dst = self.block(which, other, origin)
            found.append(remote(src, dst, self.send_sem.at[base + other], self.recv_sem.at[base + origin], {'wx': other}))
        gu, d, q, kv, o = self.shards
        unit = self.pos if landing else self.head_to['wy']
        base = self.n_wx * 2 + which * 2
        if which:
            parts = [(o, self.at_b(unit, self.n_wx * SUB, o.shape[1]))]
            if self.layer == 0:
                both = self.at_b(unit, self.n_wx * SUB + o.shape[1], q.shape[1])
                parts += [(src, both.at[:, pl.ds(num * q.shape[2], q.shape[2])]) for num, src in enumerate((q, kv))]
        elif self.layer:
            parts = [(src, self.at_a(unit, (self.n_wx + num) * q.shape[1], q.shape[1])) for num, src in enumerate((q, kv))]
        else:
            parts = []
        for num, (src, dst) in enumerate(parts):
            found.append(remote(src.at[self.layer], dst, self.send_sem.at[base + num], self.recv_sem.at[base + num], self.head_to))
        return found

    def start(self, which):
        self.kept(which).start()
        for copy in self.copies(which):
            copy.start()

    def land(self, which):
        for copy in self.copies(which, True):
            copy.wait_recv()
        self.kept(which).wait()

    def drain(self, which):
        for copy in self.copies(which):
            copy.wait_send()


def up_step(hall, wa, mo, chunks, between):
    d_model = hall.shape[2]
    half = hall.shape[1] // 2
    n_unit, tile = wa.shape[0], wa.shape[2]
    n_w = n_unit // 2
    rows = [(prompt, pl.ds(pl.multiple_of(start, half), half)) for prompt, start in chunks]
    h = jnp.concatenate([hall[prompt, part] for prompt, part in rows], axis=0)
    low = lax.broadcasted_iota(jnp.int32, (h.shape[0], tile), 1) < SUB

    def project(weight):
        return jnp.dot(h, weight, preferred_element_type=jnp.float32).astype(jnp.bfloat16)

    def keep(value, ref, lo):
        for num, (prompt, part) in enumerate(rows):
            ref[prompt, part, lo:lo + value.shape[1]] = value[num * half:(num + 1) * half]

    for first in range(0, n_unit, PLANE):
        if first == n_w:
            between()
        both = project(jnp.concatenate([wa[first + k, :d_model, :] for k in range(PLANE)], axis=1))
        for k in range(0, PLANE, 2):
            one, two = (both[:, part * tile:(part + 1) * tile].astype(jnp.float32) for part in (k, k + 1))
            g_f = jnp.where(low, one, pltpu.roll(two, SUB, 1))
            u_f = jnp.where(low, pltpu.roll(one, SUB, 1), two)
            hidden = g_f * (1.0 / (1.0 + jnp.exp(-g_f))) * u_f
            keep(hidden.astype(jnp.bfloat16), mo, (first + k) * SUB)


def head_weight(first, wa, wb, hh, d_model):
    n_w = wa.shape[0] // 2
    rows = d_model // n_w
    turned = [hh * n_w + k for k in (n_w // 2, 0)]

    def piece(ref, lo):
        return jnp.concatenate([ref[unit:unit + n_w // 2, lo:lo + rows, :].reshape(d_model // 2, ref.shape[2]) for unit in turned], axis=0)

    if first:
        return piece(wb, wb.shape[1] - rows)
    return jnp.concatenate([piece(wa, d_model + num * rows) for num in range(2)], axis=1)


def head_step(first, hall, wa, wb, narrow, chunks):
    half, d_model = hall.shape[1] // 2, hall.shape[2]
    rows = [(prompt, pl.ds(pl.multiple_of(start, half), half)) for prompt, start in chunks]
    h = jnp.concatenate([hall[prompt, part] for prompt, part in rows], axis=0)
    for hh in range(2):
        value = jnp.dot(h, head_weight(first, wa, wb, hh, d_model), preferred_element_type=jnp.float32).astype(jnp.bfloat16)
        for num, (prompt, part) in enumerate(rows):
            narrow[prompt, part, hh * value.shape[1]:(hh + 1) * value.shape[1]] = value[num * half:(num + 1) * half]


def attend(narrow, mo, kv_out, xt, cos, sin):
    seq, head_dim = cos.shape
    tile = 2 * head_dim

    def rot(val):
        val_f = val.astype(jnp.float32)
        return (val_f * cos + pltpu.roll(val_f, head_dim // 2, 1) * sin).astype(jnp.bfloat16)

    allowed = lax.broadcasted_iota(jnp.int32, (seq, seq), 0) >= lax.broadcasted_iota(jnp.int32, (seq, seq), 1)
    for b in range(2):
        prompt = xt * 2 + b
        k_rot = rot(narrow[prompt, :, head_dim:tile])
        v_val = narrow[prompt, :, tile + head_dim:]
        kv_out[b, 0] = k_rot
        kv_out[b, 1] = v_val
        for hh in range(2):
            q_rot = rot(narrow[prompt, :, hh * tile:hh * tile + head_dim])
            scores = lax.dot_general(q_rot, k_rot, (((1,), (1,)), ((), ())), preferred_element_type=jnp.float32) * head_dim ** -0.5
            scores = jnp.where(allowed, scores, -jnp.inf)
            expd = jnp.exp(scores - jnp.max(scores, axis=-1, keepdims=True))
            probs = (expd / jnp.sum(expd, axis=-1, keepdims=True)).astype(jnp.bfloat16)
            att = jnp.dot(probs, v_val, preferred_element_type=jnp.float32)
            lo = mo.shape[2] - (2 - hh) * head_dim
            mo[prompt, :, lo:lo + head_dim] = att.astype(jnp.bfloat16)


class Scatter:
    def __init__(self, ring, first, mo, wb, given, taken, acc, landed, pair_send, pair_recv, ring_send, ring_recv):
        self.ring, self.first = ring, first
        self.mo, self.wb, self.given, self.taken, self.acc, self.landed = mo, wb, given, taken, acc, landed
        self.pair_send, self.pair_recv, self.ring_send, self.ring_recv = pair_send, pair_recv, ring_send, ring_recv

    def piece(self, n):
        if self.first:
            return n
        return jnp.where(n < N_COL, n + N_COL, jnp.where(n < 2 * N_COL, n - N_COL, n))

    def pair_copy(self, n):
        k, slot = self.piece(n), lax.rem(n, N_COL)
        return remote(self.given.at[slot], self.taken.at[k], self.pair_send.at[k], self.pair_recv.at[k], {'wx': self.ring.pair})

    def ring_copy(self, k):
        target = jnp.where(lax.rem(k, 2) == 0, self.ring.right, self.ring.left)
        return remote(self.acc.at[k], self.landed.at[k], self.ring_send.at[k], self.ring_recv.at[k], {'wx': target})

    def products(self, k):
        n_unit, rows, tile = self.wb.shape
        n_w = n_unit // 2
        phase, j = lax.div(k, N_COL), lax.rem(k, N_COL)
        odd, slot = lax.rem(j, 2), lax.div(j, 2)
        own = phase == 3
        off = jnp.where(phase == 0, 2, jnp.where(own, 0, 1 + 2 * odd))
        q = jnp.where(own, j, jnp.where(phase == 1, 1 - odd, odd) * 2 + slot)
        xt = lax.rem(self.ring.chip + off, self.ring.n_chip)

        def columns(w):
            parts = [self.wb[:, pl.ds(pl.multiple_of(w * SUB, SUB), SUB), :].reshape(n_unit * SUB, tile)]
            for hh in range(2):
                parts.append(self.wb[hh * n_w + lax.rem(w + n_w // 2, n_w), n_w * SUB:n_w * SUB + 2 * SUB, :])
            return jnp.concatenate(parts, axis=0)

        weight = jnp.concatenate([columns(2 * q), columns(2 * q + 1)], axis=1)

        def product(core):
            return jnp.dot(self.mo[xt * 2 + core], weight, preferred_element_type=jnp.float32)

        return product

    def combine(self, n):
        k = self.piece(n)
        self.pair_copy(n).wait_recv()
        self.acc[k] = self.acc[k] + self.taken[k]

    def send(self, n):
        k = self.piece(n)

        @pl.when(k < 2 * N_COL)
        def _():
            self.ring_copy(k).start()

    def run(self, lo, hi):
        def body(n, carry):
            product = self.products(self.piece(n))

            @pl.when(n >= N_COL)
            def _():
                self.pair_copy(n - N_COL).wait_send()

            self.given[lax.rem(n, N_COL)] = product(1 - self.ring.core)

            @pl.when(n > lo)
            def _():
                self.combine(n - 1)

            self.acc[self.piece(n)] = product(self.ring.core)
            self.pair_copy(n).start()

            @pl.when(n > lo)
            def _():
                self.send(n - 1)

            return carry

        lax.fori_loop(lo, hi, body, 0)

        @pl.when(hi > lo)
        def _():
            self.combine(hi - 1)
            self.send(hi - 1)

    def finish(self, resid_ref, out_ref, beside):
        col = self.acc.shape[2]
        own = 3 * N_COL
        for pair in range(2):
            for odd in range(2):
                k = 2 * (N_COL + pair) + odd
                self.ring_copy(k - 2 * N_COL).wait_recv()
                self.acc[k] = self.acc[k] + self.landed[k - 2 * N_COL]
            for q in (pair, pair + 2):
                self.acc[own + q] = self.acc[own + q] + resid_ref[:, q * col:(q + 1) * col].astype(jnp.float32)
            for odd in range(2):
                self.ring_copy(2 * (N_COL + pair) + odd).start()
            beside[pair]()
        for pair in range(2):
            for k in (N_COL + 2 * pair, N_COL + 2 * pair + 1):
                self.ring_copy(k).wait_recv()
            beside[2 + pair]()
        for pair in range(2):
            for q, raw, comb in ((pair, 5, 8), (pair + 2, 4, 9)):
                raw, comb = raw + 2 * pair, comb + 2 * pair
                self.ring_copy(comb).wait_recv()
                out_ref[:, q * col:(q + 1) * col] = (self.acc[own + q] + (self.landed[raw] + self.landed[comb])).astype(jnp.bfloat16)
        for n in range(own, own + N_COL):
            self.pair_copy(n).wait_send()
        for k in range(N_RING):
            self.ring_copy(k).wait_send()


def layer_kernel(n_wx, first, *refs):
    if first:
        (resid_ref, gamma_ref, cos_ref, sin_ref, gu_ref, d_ref, q_ref, kv_ref, o_ref, out_ref, k_out, v_out, next_a, next_b,
         next_send, next_recv, x0_send, x0_recv, x1_send, x1_recv, a_send, a_recv, *rest) = refs
    else:
        resid_ref, gamma_ref, cos_ref, sin_ref, wa_ref, b_ref, k_ref, v_ref, out_ref, k_out, v_out, w_sem, old_sem, *rest = refs
    hall, wa, wb, mo, narrow, kv, h_send, h_recv, b_send, b_recv, kv_sem, *parts = rest
    ring = Ring(n_wx)
    gather_h = ChipGather(ring, hall, h_send, h_recv)
    gather_b = PlaneGather(wb, b_send, b_recv)
    scatter = Scatter(ring, first, mo, wb, *parts)
    peers = [{'wx': ring.right}, {'wx': ring.left}, {'wx': ring.pair}] + gather_b.neighbours()
    if first:
        shards = gu_ref, d_ref, q_ref, kv_ref, o_ref
        gather_a = PlaneGather(wa, a_send, a_recv)
        gather_n = PlaneGather(next_a, next_send, next_recv)
        swap_0 = Exchange(ring, 0, shards, gather_a.place, gather_b.place, x0_send, x0_recv)
        swap_1 = Exchange(ring, 1, shards, gather_n.place, lambda unit, start, size: next_b.at[pl.ds(start, size)], x1_send, x1_recv)
        peers += swap_0.peers()
    else:
        here = gather_b.here
        b_load = pltpu.make_async_copy(b_ref, wb.at[here], w_sem.at[0])
        a_load = pltpu.make_async_copy(wa_ref, wa, w_sem.at[1])
        old_loads = [pltpu.make_async_copy(ref, kv.at[2, 0, num], old_sem.at[num]) for num, ref in enumerate((k_ref, v_ref))]
        for load in (b_load, a_load, *old_loads):
            load.start()
    barrier = pltpu.get_barrier_semaphore()
    for peer in peers:
        pl.semaphore_signal(barrier, inc=1, device_id=peer, device_id_type=MESH)

    resid_f = resid_ref[...].astype(jnp.float32)
    centered = resid_f - jnp.mean(resid_f, axis=-1, keepdims=True)
    variance = jnp.mean(centered * centered, axis=-1, keepdims=True)
    normed = (centered * lax.rsqrt(variance + LN_EPS) * gamma_ref[1 - first:2 - first, :]).astype(jnp.bfloat16)
    hall[ring.me] = normed
    pl.semaphore_wait(barrier, len(peers))
    if first:
        swap_0.start(0)
        gather_h.start()
        swap_0.land(0)
        gather_a.start()
        swap_0.start(1)
        gather_a.stage_1()
        gather_h.near_halves()
        gather_a.stage_2()
        gather_a.stage_3()
        gather_h.near_rest()
        swap_1.start(0)
        swap_1.start(1)
        gather_a.stage_4()
        gather_h.far_halves()
        gather_a.stage_5()
        swap_0.land(1)
        gather_b.start()
        gather_h.wait(0, 7, 8, 9, 10, 11, 12)
        gather_a.finish()
    else:
        gather_h.start()
        b_load.wait()
        gather_b.start()
        a_load.wait()

    seq = hall.shape[1]
    half = seq // 2

    def whole(xt):
        return [(xt * 2 + b, start) for start in (0, half) for b in range(2)]

    def attend_to(off):
        xt = lax.rem(ring.chip + off, ring.n_chip)
        attend(narrow, mo, kv.at[jnp.where(off == 0, 0, 1)], xt, cos_ref[...], sin_ref[...])

    def at_step(step):
        def when(num, *calls):
            @pl.when(step == num)
            def _():
                for call in calls:
                    call()

        return when

    def wide(step, carry):
        when = at_step(step)
        when(1, gather_b.stage_1)
        when(2, gather_b.stage_3)
        when(3, gather_b.stage_4)
        up_step(hall, wa, mo, whole(step), lambda: when(1, gather_b.stage_2))
        return carry

    def heads(num, carry):
        when = at_step(num)
        when(1, gather_n.stage_1)
        when(3, gather_n.stage_2)
        off = jnp.where(num == 0, 2, jnp.where(num == 1, 3, jnp.where(num == 2, 1, 0)))
        head_step(first, hall, wa, wb, narrow, whole(lax.rem(ring.chip + off, ring.n_chip)))
        attend_to(off)
        lo = jnp.where(num == 3, 2 * N_COL, jnp.where(num == 2, N_COL, 0))
        scatter.run(lo, jnp.where(num == 3, 4 * N_COL, jnp.where(num == 1, 0, lo + N_COL)))
        return carry

    def body(step, carry):
        when = at_step(step)
        when(0, lambda: gather_h.wait(0))
        when(1, gather_b.stage_1, gather_h.near_halves, gather_b.stage_2, lambda: gather_h.wait(7, 8))
        when(2, gather_b.stage_3, gather_h.near_rest, gather_b.stage_4, lambda: gather_h.wait(9, 10))
        when(3, gather_h.far_halves, lambda: gather_h.wait(11, 12))
        near = (step == 1) | (step == 2)
        lone = jnp.where(step == 0, ring.chip, lax.rem(ring.chip + 2, ring.n_chip))
        one = jnp.where(near, lax.div(ring.left, 2), lone)
        two = jnp.where(near, lax.div(ring.right, 2), lone)
        start = jnp.where(step == 2, half, 0)
        chunks = [(one * 2 + b, start) for b in range(2)] + [(two * 2 + b, half - start) for b in range(2)]
        head_step(first, hall, wa, wb, narrow, chunks)
        up_step(hall, wa, mo, chunks, lambda: when(2, gather_b.stage_5))

        def attention(num, carry):
            attend_to(jnp.where(num == 0, 0, jnp.where(num == 1, 3, jnp.where(num == 2, 1, 2))))
            return carry

        lo = jnp.where(step == 3, 3, jnp.where(step == 0, 0, 1))
        lax.fori_loop(lo, jnp.where(step < 2, 1, step + 1), attention, 0)
        when(2, gather_b.finish)
        last = step == 3
        scatter.run(jnp.where(last, N_COL, 0), jnp.where(last, 4 * N_COL, jnp.where(step == 2, N_COL, 0)))
        return carry

    if first:
        lax.fori_loop(0, ring.n_chip, wide, 0)
        gather_b.stage_5()
        gather_b.finish()
        swap_1.land(0)
        gather_n.start()
        lax.fori_loop(0, ring.n_chip, heads, 0)
    else:
        lax.fori_loop(0, ring.n_chip, body, 0)
    if first:
        caches = [(kv.at[0, ring.core, num], ref) for num, ref in enumerate((k_out, v_out))]
    else:
        for load in old_loads:
            load.wait()
        caches = [(kv.at[0, ring.core, num], ref.at[1]) for num, ref in enumerate((k_out, v_out))]
        caches += [(kv.at[2, 0, num], ref.at[0]) for num, ref in enumerate((k_out, v_out))]
    caches = [pltpu.make_async_copy(src, dst, kv_sem.at[num]) for num, (src, dst) in enumerate(caches)]
    for cache in caches:
        cache.start()
    if first:
        scatter.finish(resid_ref, out_ref, (lambda: None, gather_n.stage_3, gather_n.stage_4, gather_n.stage_5))
        gather_n.finish()
        swap_1.land(1)
        for swap in (swap_0, swap_1):
            swap.drain(0)
            swap.drain(1)
        gather_a.drain()
        gather_n.drain()
    else:
        scatter.finish(resid_ref, out_ref, [lambda: None] * 4)
    gather_b.drain()
    gather_h.drain()
    for cache in caches:
        cache.wait()


def layer(resid, gamma, cos, sin, weights, n_wx, first):
    seq, d_model = resid.shape
    head_dim = cos.shape[1]
    n_unit = PLANE * PLANE
    col = d_model // N_COL
    any_spec, vmem_spec = pl.BlockSpec(memory_space=pl.ANY), pl.BlockSpec(memory_space=pltpu.VMEM)
    tile = d_model // n_wx
    unit_b = (n_wx * SUB + head_dim, tile)
    next_shape = (n_unit, d_model + 2 * tile, 2 * SUB)
    wa_shape = (n_unit, d_model, 2 * SUB) if first else next_shape
    wb_shape = (n_unit, unit_b[0] + (tile if first else 0), tile)
    piece = (seq, col)
    n_piece = 4 * N_COL
    dma = pltpu.SemaphoreType.DMA
    cache = (seq, head_dim) if first else (2, seq, head_dim)
    out_shape = [jax.ShapeDtypeStruct(shape, jnp.bfloat16) for shape in (resid.shape, cache, cache)]
    n_plane, n_swap, n_hop = dma((40,)), dma((21,)), dma((13,))
    if first:
        out_shape += [jax.ShapeDtypeStruct(shape, jnp.bfloat16) for shape in (next_shape, unit_b)]
        scratch = [n_plane, n_plane, n_swap, n_swap, n_swap, n_swap, n_plane, n_plane]
    else:
        scratch = [dma((2,)), dma((2,))]
    scratch += [
        pltpu.VMEM((n_wx, seq, d_model), jnp.bfloat16),
        pltpu.VMEM(wa_shape, jnp.bfloat16),
        pltpu.VMEM(wb_shape, jnp.bfloat16),
        pltpu.VMEM((n_wx, seq, n_unit * SUB + 2 * head_dim), jnp.bfloat16),
        pltpu.VMEM((n_wx, seq, 4 * head_dim), jnp.bfloat16),
        pltpu.VMEM((3, 2, 2, seq, head_dim), jnp.bfloat16),
        n_hop, n_hop, n_plane, n_plane, dma((4,)),
        pltpu.VMEM((N_COL,) + piece, jnp.float32),
        pltpu.VMEM((n_piece,) + piece, jnp.float32),
        pltpu.VMEM((n_piece,) + piece, jnp.float32),
        pltpu.VMEM((N_RING,) + piece, jnp.float32),
        dma((n_piece,)), dma((n_piece,)), dma((N_RING,)), dma((N_RING,)),
    ]
    return pl.pallas_call(
        functools.partial(layer_kernel, n_wx, first),
        out_shape=tuple(out_shape),
        in_specs=[vmem_spec] * 4 + [any_spec] * len(weights),
        out_specs=[vmem_spec] + [any_spec] * (len(out_shape) - 1),
        scratch_shapes=scratch,
        compiler_params=pltpu.CompilerParams(collective_id=int(first), has_side_effects=True, vmem_limit_bytes=VMEM_LIMIT),
        name='layer_0' if first else 'layer_1',
    )(resid, gamma, cos, sin, *weights)


def settle_kernel(*refs):
    n = len(refs) // 3
    srcs, dsts, held, sem = refs[:n], refs[n:2 * n], refs[2 * n:3 * n], refs[-1]
    loads = [pltpu.make_async_copy(src, mid, sem.at[num]) for num, (src, mid) in enumerate(zip(srcs, held))]
    stores = [pltpu.make_async_copy(mid, dst, sem.at[n + num]) for num, (mid, dst) in enumerate(zip(held, dsts))]
    for load in loads:
        load.start()
    for load, store in zip(loads, stores):
        load.wait()
        store.start()
    for store in stores:
        store.wait()


def settle(arrays):
    n = len(arrays)
    return pl.pallas_call(
        settle_kernel,
        out_shape=tuple(jax.ShapeDtypeStruct(a.shape, a.dtype) for a in arrays),
        in_specs=[pl.BlockSpec(memory_space=pl.ANY)] * n,
        out_specs=[pl.BlockSpec(memory_space=pl.ANY)] * n,
        scratch_shapes=[pltpu.VMEM(a.shape, a.dtype) for a in arrays] + [pltpu.SemaphoreType.DMA((2 * n,))],
        name='settle',
    )(*arrays)


def solution(mesh):
    batch_axes = ('dp', 'wy', 'wx')
    in_specs = (P(batch_axes), P(), P(None, 'wx', 'wy'), P(None, 'wx'), P(None, 'wx', None, 'wy'), P(None, 'wy', 'wx'), P(None, 'wy', 'wx'))
    out_specs = (P(batch_axes), P(None, batch_axes), P(None, batch_axes))
    n_wx = mesh.shape['wx']

    def device_step(x_tokens, gamma_ln, w_q, w_kv, w_gu, w_o, w_d):
        n_layers, d_loc = w_q.shape[:2]
        cos_tab, sin_tab = rope_tables(x_tokens.shape[1], w_kv.shape[-1])
        kv_half = lax.dynamic_index_in_dim(w_kv, lax.rem(lax.axis_index('wy'), 2), axis=2, keepdims=False)
        gu = jnp.transpose(w_gu.reshape(n_layers, d_loc, 2, n_wx, SUB), (0, 3, 1, 2, 4)).reshape(n_layers, n_wx, d_loc, 2 * SUB)
        resid, k_0, v_0, wa, unit_b = layer(x_tokens[0], gamma_ln, cos_tab, sin_tab, (gu, w_d, w_q, kv_half, w_o), n_wx, True)
        resid, k_all, v_all = settle(layer(resid, gamma_ln, cos_tab, sin_tab, (wa, unit_b, k_0, v_0), n_wx, False))
        return resid[None], k_all[:, None], v_all[:, None]

    return jax.shard_map(device_step, mesh=mesh, in_specs=in_specs, out_specs=out_specs, check_vma=False)
```

```python
import functools

import jax
import jax.numpy as jnp
from jax import lax
from jax.experimental import pallas as pl
from jax.experimental.pallas import tpu as pltpu
from jax.sharding import PartitionSpec as P

LN_EPS = 1e-6
ROPE_BASE = 10000.0
MESH = pl.DeviceIdType.MESH
VMEM_LIMIT = 67043328
PLANE = 4
SUB = 64
N_COL = 4
N_RING = 12


def rope_tables(seq_len, head_dim):
    half_dim = head_dim // 2
    inv_freq = ROPE_BASE ** (-2.0 * jnp.arange(half_dim, dtype=jnp.float32) / head_dim)
    angles = jnp.arange(seq_len, dtype=jnp.float32)[:, None] * inv_freq[None, :]
    cos, sin = jnp.cos(angles), jnp.sin(angles)
    return jnp.concatenate([cos, cos], axis=1), jnp.concatenate([-sin, sin], axis=1)


def remote(src, dst, send, recv, target):
    return pltpu.make_async_remote_copy(src_ref=src, dst_ref=dst, send_sem=send, recv_sem=recv, device_id=target, device_id_type=MESH)


class Ring:
    def __init__(self, n_wx):
        self.me = lax.axis_index('wx')
        self.chip, self.core = lax.div(self.me, 2), lax.rem(self.me, 2)
        self.n_chip = n_wx // 2
        self.right, self.left, self.far = self.at(1), self.at(self.n_chip - 1), self.at(2)
        self.pair = self.at(0, 1)

    def at(self, step, other=0):
        return lax.rem(self.chip + step, self.n_chip) * 2 + lax.rem(self.core + other, 2)


class ChipGather:
    def __init__(self, ring, hall, send_sem, recv_sem):
        half = hall.shape[1] // 2
        top, bottom, whole = pl.ds(0, half), pl.ds(half, half), pl.ds(0, 2 * half)
        me, left, right, far, pair = ring.me, ring.left, ring.right, ring.far, ring.pair
        moves = [
            (me, whole, pair, pair),
            (me, top, right, left), (me, bottom, left, right),
            (me, bottom, right, left), (me, top, left, right),
            (left, top, right, far), (right, bottom, left, far),
            (left, top, pair, ring.at(ring.n_chip - 1, 1)), (right, bottom, pair, ring.at(1, 1)),
            (left, bottom, pair, ring.at(ring.n_chip - 1, 1)), (right, top, pair, ring.at(1, 1)),
            (far, top, pair, ring.at(2, 1)), (far, bottom, pair, ring.at(2, 1)),
        ]
        self.sends, self.lands = [], []
        for num, (block, rows, target, landed) in enumerate(moves):
            for kept, there in ((self.sends, block), (self.lands, landed)):
                ref = hall.at[there, rows]
                kept.append(remote(ref, ref, send_sem.at[num], recv_sem.at[num], {'wx': target}))
        self.first = 5

    def start(self):
        for copy in self.sends[:self.first]:
            copy.start()

    def relay(self, landed, *sent):
        self.lands[landed].wait_recv()
        for num in sent:
            self.sends[num].start()

    def near_halves(self):
        self.relay(1, 5, 7)
        self.relay(2, 6, 8)

    def near_rest(self):
        self.relay(3, 9)
        self.relay(4, 10)

    def far_halves(self):
        self.relay(5, 11)
        self.relay(6, 12)

    def wait(self, *nums):
        for num in nums:
            self.lands[num].wait_recv()

    def drain(self):
        for copy in self.sends:
            copy.wait_send()


class PlaneGather:
    ways = [(half, sign) for half in range(2) for sign in (1, -1)]

    def __init__(self, buf, send_sem, recv_sem):
        self.buf, self.send_sem, self.recv_sem = buf, send_sem, recv_sem
        self.here = lax.axis_index('wy')
        self.pos = (lax.div(self.here, PLANE), lax.rem(self.here, PLANE))

    def at(self, half, first, second=0):
        step_z, step_y = (second, first) if half == 0 else (first, second)
        z, y = self.pos
        return lax.rem(z + step_z + PLANE, PLANE) * PLANE + lax.rem(y + step_y + PLANE, PLANE)

    def neighbours(self):
        return [{'wy': self.at(half, sign)} for half, sign in self.ways]

    def place(self, block, start, size):
        return self.buf.at[block, pl.ds(start, size)]

    def copy(self, kind, num, block, half, quarter, target):
        rows = self.buf.shape[1]
        size = rows // 2 if quarter is None else rows // PLANE
        ref = self.place(block, half * (rows // 2) + (quarter or 0) * size, size)
        slot = kind * PLANE + num
        return remote(ref, ref, self.send_sem.at[slot], self.recv_sem.at[slot], {'wy': target})

    def one(self, half, sign, landing=False):
        block = self.at(half, -sign if landing else 0)
        return self.copy(0, half * 2 + (sign < 0), block, half, None, self.at(half, sign))

    def two(self, half, sign, landing=False):
        block = self.at(half, -2 * sign if landing else -sign)
        return self.copy(1, half * 2 + (sign < 0), block, half, int(sign < 0), self.at(half, sign))

    def three(self, half, off, sign, landing=False):
        block = self.at(half, off, -sign if landing else 0)
        return self.copy(2, (half * PLANE + off % PLANE) * 2 + (sign < 0), block, half, None, self.at(half, 0, sign))

    def four(self, half, off, sign, landing=False):
        block = self.at(half, off, -2 * sign if landing else -sign)
        return self.copy(6, (half * PLANE + off % PLANE) * 2 + (sign < 0), block, half, int(sign < 0), self.at(half, 0, sign))

    def start(self):
        for half, sign in self.ways:
            self.one(half, sign).start()
        for half, sign in self.ways:
            self.three(half, 0, sign).start()

    def stage_1(self):
        for half, sign in self.ways:
            self.one(half, sign, True).wait_recv()
            self.two(half, sign).start()
        for half, sign in self.ways:
            for way in (1, -1):
                self.three(half, -sign, way).start()

    def fourth(self, off):
        for half, sign in self.ways:
            self.three(half, off, sign, True).wait_recv()
            self.four(half, off, sign).start()

    def stage_2(self):
        self.fourth(0)

    def stage_3(self):
        for half, sign in self.ways:
            self.two(half, sign, True).wait_recv()
        for half, sign in self.ways:
            self.three(half, 2, sign).start()

    def stage_4(self):
        self.fourth(1)
        self.fourth(-1)

    def stage_5(self):
        self.fourth(2)

    def each(self, call):
        for half, sign in self.ways:
            for off in (0, 1, -1, 2):
                call(half, off, sign)

    def finish(self):
        self.each(lambda half, off, sign: self.four(half, off, sign, True).wait_recv())

    def drain(self):
        for half, sign in self.ways:
            self.one(half, sign).wait_send()
            self.two(half, sign).wait_send()
        self.each(lambda half, off, sign: self.three(half, off, sign).wait_send())
        self.each(lambda half, off, sign: self.four(half, off, sign).wait_send())


class Exchange:
    def __init__(self, ring, layer, shards, at_a, at_b, send_sem, recv_sem):
        self.me, self.n_wx = ring.me, ring.n_chip * 2
        self.pos = pos = lax.axis_index('wy')
        self.head_to = {'wy': lax.rem(pos, 2) * self.n_wx + self.turn(self.me), 'wx': lax.div(pos, 2)}
        self.head_from = {'wy': 2 * self.me + lax.div(pos, self.n_wx), 'wx': self.turn(lax.rem(pos, self.n_wx))}
        self.layer, self.shards = layer, shards
        self.at_a, self.at_b = at_a, at_b
        self.send_sem, self.recv_sem = send_sem, recv_sem

    def turn(self, w):
        return lax.rem(w + self.n_wx // 2, self.n_wx)

    def others(self):
        return [lax.rem(self.me + step, self.n_wx) for step in (4, 5, 3, 2, 6, 7, 1)]

    def peers(self):
        return [{'wx': other} for other in self.others()] + [self.head_from]

    def block(self, which, to, origin):
        gu, d = self.shards[:2]
        if which:
            src, place, rows = d.at[self.layer, pl.ds(pl.multiple_of(to * SUB, SUB), SUB)], self.at_b, SUB
        else:
            src, place, rows = gu.at[self.layer, to], self.at_a, gu.shape[2]
        return src, place(self.pos, pl.multiple_of(origin * rows, rows), rows)

    def kept(self, which):
        return pltpu.make_async_copy(*self.block(which, self.me, self.me), self.send_sem.at[which * self.n_wx + self.me])

    def copies(self, which, landing=False):
        base = which * self.n_wx
        found = []
        for other in self.others():
            origin = other if landing else self.me
            src, dst = self.block(which, other, origin)
            found.append(remote(src, dst, self.send_sem.at[base + other], self.recv_sem.at[base + origin], {'wx': other}))
        gu, d, q, kv, o = self.shards
        unit = self.pos if landing else self.head_to['wy']
        base = self.n_wx * 2 + which * 2
        if which:
            parts = [(o, self.at_b(unit, self.n_wx * SUB, o.shape[1]))]
            if self.layer == 0:
                both = self.at_b(unit, self.n_wx * SUB + o.shape[1], q.shape[1])
                parts += [(src, both.at[:, pl.ds(num * q.shape[2], q.shape[2])]) for num, src in enumerate((q, kv))]
        elif self.layer:
            parts = [(src, self.at_a(unit, (self.n_wx + num) * q.shape[1], q.shape[1])) for num, src in enumerate((q, kv))]
        else:
            parts = []
        for num, (src, dst) in enumerate(parts):
            found.append(remote(src.at[self.layer], dst, self.send_sem.at[base + num], self.recv_sem.at[base + num], self.head_to))
        return found

    def start(self, which):
        self.kept(which).start()
        for copy in self.copies(which):
            copy.start()

    def land(self, which):
        for copy in self.copies(which, True):
            copy.wait_recv()
        self.kept(which).wait()

    def drain(self, which):
        for copy in self.copies(which):
            copy.wait_send()


def up_step(hall, wa, mo, chunks, between):
    d_model = hall.shape[2]
    half = hall.shape[1] // 2
    n_unit, tile = wa.shape[0], wa.shape[2]
    n_w = n_unit // 2
    rows = [(prompt, pl.ds(pl.multiple_of(start, half), half)) for prompt, start in chunks]
    h = jnp.concatenate([hall[prompt, part] for prompt, part in rows], axis=0)
    low = lax.broadcasted_iota(jnp.int32, (h.shape[0], tile), 1) < SUB

    def project(weight):
        return jnp.dot(h, weight, preferred_element_type=jnp.float32).astype(jnp.bfloat16)

    def keep(value, ref, lo):
        for num, (prompt, part) in enumerate(rows):
            ref[prompt, part, lo:lo + value.shape[1]] = value[num * half:(num + 1) * half]

    for first in range(0, n_unit, PLANE):
        if first == n_w:
            between()
        both = project(jnp.concatenate([wa[first + k, :d_model, :] for k in range(PLANE)], axis=1))
        for k in range(0, PLANE, 2):
            one, two = (both[:, part * tile:(part + 1) * tile].astype(jnp.float32) for part in (k, k + 1))
            g_f = jnp.where(low, one, pltpu.roll(two, SUB, 1))
            u_f = jnp.where(low, pltpu.roll(one, SUB, 1), two)
            hidden = g_f * (1.0 / (1.0 + jnp.exp(-g_f))) * u_f
            keep(hidden.astype(jnp.bfloat16), mo, (first + k) * SUB)


def head_weight(first, wa, wb, hh, d_model):
    n_w = wa.shape[0] // 2
    rows = d_model // n_w
    turned = [hh * n_w + k for k in (n_w // 2, 0)]

    def piece(ref, lo):
        return jnp.concatenate([ref[unit:unit + n_w // 2, lo:lo + rows, :].reshape(d_model // 2, ref.shape[2]) for unit in turned], axis=0)

    if first:
        return piece(wb, wb.shape[1] - rows)
    return jnp.concatenate([piece(wa, d_model + num * rows) for num in range(2)], axis=1)


def head_step(first, hall, wa, wb, narrow, chunks):
    half, d_model = hall.shape[1] // 2, hall.shape[2]
    rows = [(prompt, pl.ds(pl.multiple_of(start, half), half)) for prompt, start in chunks]
    h = jnp.concatenate([hall[prompt, part] for prompt, part in rows], axis=0)
    for hh in range(2):
        value = jnp.dot(h, head_weight(first, wa, wb, hh, d_model), preferred_element_type=jnp.float32).astype(jnp.bfloat16)
        for num, (prompt, part) in enumerate(rows):
            narrow[prompt, part, hh * value.shape[1]:(hh + 1) * value.shape[1]] = value[num * half:(num + 1) * half]


def attend(narrow, mo, kv_out, xt, cos, sin):
    seq, head_dim = cos.shape
    tile = 2 * head_dim

    def rot(val):
        val_f = val.astype(jnp.float32)
        return (val_f * cos + pltpu.roll(val_f, head_dim // 2, 1) * sin).astype(jnp.bfloat16)

    allowed = lax.broadcasted_iota(jnp.int32, (seq, seq), 0) >= lax.broadcasted_iota(jnp.int32, (seq, seq), 1)
    for b in range(2):
        prompt = xt * 2 + b
        k_rot = rot(narrow[prompt, :, head_dim:tile])
        v_val = narrow[prompt, :, tile + head_dim:]
        kv_out[b, 0] = k_rot
        kv_out[b, 1] = v_val
        for hh in range(2):
            q_rot = rot(narrow[prompt, :, hh * tile:hh * tile + head_dim])
            scores = lax.dot_general(q_rot, k_rot, (((1,), (1,)), ((), ())), preferred_element_type=jnp.float32) * head_dim ** -0.5
            scores = jnp.where(allowed, scores, -jnp.inf)
            expd = jnp.exp(scores - jnp.max(scores, axis=-1, keepdims=True))
            probs = (expd / jnp.sum(expd, axis=-1, keepdims=True)).astype(jnp.bfloat16)
            att = jnp.dot(probs, v_val, preferred_element_type=jnp.float32)
            lo = mo.shape[2] - (2 - hh) * head_dim
            mo[prompt, :, lo:lo + head_dim] = att.astype(jnp.bfloat16)


class Scatter:
    def __init__(self, ring, first, mo, wb, given, taken, acc, landed, pair_send, pair_recv, ring_send, ring_recv):
        self.ring, self.first = ring, first
        self.mo, self.wb, self.given, self.taken, self.acc, self.landed = mo, wb, given, taken, acc, landed
        self.pair_send, self.pair_recv, self.ring_send, self.ring_recv = pair_send, pair_recv, ring_send, ring_recv

    def piece(self, n):
        if self.first:
            return n
        return jnp.where(n < N_COL, n + N_COL, jnp.where(n < 2 * N_COL, n - N_COL, n))

    def pair_copy(self, n):
        k, slot = self.piece(n), lax.rem(n, N_COL)
        return remote(self.given.at[slot], self.taken.at[k], self.pair_send.at[k], self.pair_recv.at[k], {'wx': self.ring.pair})

    def ring_copy(self, k):
        target = jnp.where(lax.rem(k, 2) == 0, self.ring.right, self.ring.left)
        return remote(self.acc.at[k], self.landed.at[k], self.ring_send.at[k], self.ring_recv.at[k], {'wx': target})

    def products(self, k):
        n_unit, rows, tile = self.wb.shape
        n_w = n_unit // 2
        phase, j = lax.div(k, N_COL), lax.rem(k, N_COL)
        odd, slot = lax.rem(j, 2), lax.div(j, 2)
        own = phase == 3
        off = jnp.where(phase == 0, 2, jnp.where(own, 0, 1 + 2 * odd))
        q = jnp.where(own, j, jnp.where(phase == 1, 1 - odd, odd) * 2 + slot)
        xt = lax.rem(self.ring.chip + off, self.ring.n_chip)

        def columns(w):
            parts = [self.wb[:, pl.ds(pl.multiple_of(w * SUB, SUB), SUB), :].reshape(n_unit * SUB, tile)]
            for hh in range(2):
                parts.append(self.wb[hh * n_w + lax.rem(w + n_w // 2, n_w), n_w * SUB:n_w * SUB + 2 * SUB, :])
            return jnp.concatenate(parts, axis=0)

        weight = jnp.concatenate([columns(2 * q), columns(2 * q + 1)], axis=1)

        def product(core):
            return jnp.dot(self.mo[xt * 2 + core], weight, preferred_element_type=jnp.float32)

        return product

    def combine(self, n):
        k = self.piece(n)
        self.pair_copy(n).wait_recv()
        self.acc[k] = self.acc[k] + self.taken[k]

    def send(self, n):
        k = self.piece(n)

        @pl.when(k < 2 * N_COL)
        def _():
            self.ring_copy(k).start()

    def run(self, lo, hi):
        def body(n, carry):
            product = self.products(self.piece(n))

            @pl.when(n >= N_COL)
            def _():
                self.pair_copy(n - N_COL).wait_send()

            self.given[lax.rem(n, N_COL)] = product(1 - self.ring.core)

            @pl.when(n > lo)
            def _():
                self.combine(n - 1)

            self.acc[self.piece(n)] = product(self.ring.core)
            self.pair_copy(n).start()

            @pl.when(n > lo)
            def _():
                self.send(n - 1)

            return carry

        lax.fori_loop(lo, hi, body, 0)

        @pl.when(hi > lo)
        def _():
            self.combine(hi - 1)
            self.send(hi - 1)

    def finish(self, resid_ref, out_ref, beside):
        col = self.acc.shape[2]
        own = 3 * N_COL
        for pair in range(2):
            for odd in range(2):
                k = 2 * (N_COL + pair) + odd
                self.ring_copy(k - 2 * N_COL).wait_recv()
                self.acc[k] = self.acc[k] + self.landed[k - 2 * N_COL]
            for q in (pair, pair + 2):
                self.acc[own + q] = self.acc[own + q] + resid_ref[:, q * col:(q + 1) * col].astype(jnp.float32)
            for odd in range(2):
                self.ring_copy(2 * (N_COL + pair) + odd).start()
            beside[pair]()
        for pair in range(2):
            for k in (N_COL + 2 * pair, N_COL + 2 * pair + 1):
                self.ring_copy(k).wait_recv()
            beside[2 + pair]()
        for pair in range(2):
            for q, raw, comb in ((pair, 5, 8), (pair + 2, 4, 9)):
                raw, comb = raw + 2 * pair, comb + 2 * pair
                self.ring_copy(comb).wait_recv()
                out_ref[:, q * col:(q + 1) * col] = (self.acc[own + q] + (self.landed[raw] + self.landed[comb])).astype(jnp.bfloat16)
        for n in range(own, own + N_COL):
            self.pair_copy(n).wait_send()
        for k in range(N_RING):
            self.ring_copy(k).wait_send()


def layer_kernel(n_wx, first, *refs):
    if first:
        (resid_ref, gamma_ref, cos_ref, sin_ref, gu_ref, d_ref, q_ref, kv_ref, o_ref, out_ref, k_out, v_out, next_a, next_b,
         next_send, next_recv, x0_send, x0_recv, x1_send, x1_recv, a_send, a_recv, *rest) = refs
    else:
        resid_ref, gamma_ref, cos_ref, sin_ref, wa_ref, b_ref, k_ref, v_ref, out_ref, k_out, v_out, w_sem, old_sem, *rest = refs
    hall, wa, wb, mo, narrow, kv, h_send, h_recv, b_send, b_recv, kv_sem, *parts = rest
    ring = Ring(n_wx)
    gather_h = ChipGather(ring, hall, h_send, h_recv)
    gather_b = PlaneGather(wb, b_send, b_recv)
    scatter = Scatter(ring, first, mo, wb, *parts)
    peers = [{'wx': ring.right}, {'wx': ring.left}, {'wx': ring.pair}] + gather_b.neighbours()
    if first:
        shards = gu_ref, d_ref, q_ref, kv_ref, o_ref
        gather_a = PlaneGather(wa, a_send, a_recv)
        gather_n = PlaneGather(next_a, next_send, next_recv)
        swap_0 = Exchange(ring, 0, shards, gather_a.place, gather_b.place, x0_send, x0_recv)
        swap_1 = Exchange(ring, 1, shards, gather_n.place, lambda unit, start, size: next_b.at[pl.ds(start, size)], x1_send, x1_recv)
        peers += swap_0.peers()
    else:
        here = gather_b.here
        b_load = pltpu.make_async_copy(b_ref, wb.at[here], w_sem.at[0])
        a_load = pltpu.make_async_copy(wa_ref, wa, w_sem.at[1])
        old_loads = [pltpu.make_async_copy(ref, kv.at[2, 0, num], old_sem.at[num]) for num, ref in enumerate((k_ref, v_ref))]
        for load in (b_load, a_load, *old_loads):
            load.start()
    barrier = pltpu.get_barrier_semaphore()
    for peer in peers:
        pl.semaphore_signal(barrier, inc=1, device_id=peer, device_id_type=MESH)

    resid_f = resid_ref[...].astype(jnp.float32)
    centered = resid_f - jnp.mean(resid_f, axis=-1, keepdims=True)
    variance = jnp.mean(centered * centered, axis=-1, keepdims=True)
    normed = (centered * lax.rsqrt(variance + LN_EPS) * gamma_ref[1 - first:2 - first, :]).astype(jnp.bfloat16)
    hall[ring.me] = normed
    pl.semaphore_wait(barrier, len(peers))
    if first:
        swap_0.start(0)
        gather_h.start()
        swap_0.land(0)
        gather_a.start()
        swap_0.start(1)
        gather_a.stage_1()
        gather_h.near_halves()
        gather_a.stage_2()
        gather_a.stage_3()
        gather_h.near_rest()
        gather_a.stage_4()
        gather_h.far_halves()
        gather_a.stage_5()
        swap_0.land(1)
        gather_b.start()
        gather_h.wait(0, 7, 8, 9, 10, 11, 12)
        gather_a.finish()
    else:
        gather_h.start()
        b_load.wait()
        gather_b.start()
        a_load.wait()

    seq = hall.shape[1]
    half = seq // 2

    def whole(xt):
        return [(xt * 2 + b, start) for start in (0, half) for b in range(2)]

    def attend_to(off):
        xt = lax.rem(ring.chip + off, ring.n_chip)
        attend(narrow, mo, kv.at[jnp.where(off == 0, 0, 1)], xt, cos_ref[...], sin_ref[...])

    def at_step(step):
        def when(num, *calls):
            @pl.when(step == num)
            def _():
                for call in calls:
                    call()

        return when

    def wide(step, carry):
        when = at_step(step)
        when(1, gather_b.stage_1)
        when(2, gather_b.stage_3, lambda: swap_1.start(0), lambda: swap_1.start(1))
        when(3, gather_b.stage_4)
        up_step(hall, wa, mo, whole(step), lambda: when(1, gather_b.stage_2))
        return carry

    def heads(num, carry):
        when = at_step(num)
        when(1, gather_n.stage_1)
        when(3, gather_n.stage_2)
        off = jnp.where(num == 0, 2, jnp.where(num == 1, 3, jnp.where(num == 2, 1, 0)))
        head_step(first, hall, wa, wb, narrow, whole(lax.rem(ring.chip + off, ring.n_chip)))
        attend_to(off)
        lo = jnp.where(num == 3, 2 * N_COL, jnp.where(num == 2, N_COL, 0))
        scatter.run(lo, jnp.where(num == 3, 4 * N_COL, jnp.where(num == 1, 0, lo + N_COL)))
        return carry

    def body(step, carry):
        when = at_step(step)
        when(0, lambda: gather_h.wait(0))
        when(1, gather_b.stage_1, gather_h.near_halves, gather_b.stage_2, lambda: gather_h.wait(7, 8))
        when(2, gather_b.stage_3, gather_h.near_rest, gather_b.stage_4, lambda: gather_h.wait(9, 10))
        when(3, gather_h.far_halves, lambda: gather_h.wait(11, 12))
        near = (step == 1) | (step == 2)
        lone = jnp.where(step == 0, ring.chip, lax.rem(ring.chip + 2, ring.n_chip))
        one = jnp.where(near, lax.div(ring.left, 2), lone)
        two = jnp.where(near, lax.div(ring.right, 2), lone)
        start = jnp.where(step == 2, half, 0)
        chunks = [(one * 2 + b, start) for b in range(2)] + [(two * 2 + b, half - start) for b in range(2)]
        head_step(first, hall, wa, wb, narrow, chunks)
        up_step(hall, wa, mo, chunks, lambda: when(2, gather_b.stage_5))

        def attention(num, carry):
            attend_to(jnp.where(num == 0, 0, jnp.where(num == 1, 3, jnp.where(num == 2, 1, 2))))
            return carry

        lo = jnp.where(step == 3, 3, jnp.where(step == 0, 0, 1))
        lax.fori_loop(lo, jnp.where(step < 2, 1, step + 1), attention, 0)
        when(2, gather_b.finish)
        last = step == 3
        scatter.run(jnp.where(last, N_COL, 0), jnp.where(last, 4 * N_COL, jnp.where(step == 2, N_COL, 0)))
        return carry

    if first:
        lax.fori_loop(0, ring.n_chip, wide, 0)
        gather_b.stage_5()
        gather_b.finish()
        swap_1.land(0)
        gather_n.start()
        lax.fori_loop(0, ring.n_chip, heads, 0)
    else:
        lax.fori_loop(0, ring.n_chip, body, 0)
    if first:
        caches = [(kv.at[0, ring.core, num], ref) for num, ref in enumerate((k_out, v_out))]
    else:
        for load in old_loads:
            load.wait()
        caches = [(kv.at[0, ring.core, num], ref.at[1]) for num, ref in enumerate((k_out, v_out))]
        caches += [(kv.at[2, 0, num], ref.at[0]) for num, ref in enumerate((k_out, v_out))]
    caches = [pltpu.make_async_copy(src, dst, kv_sem.at[num]) for num, (src, dst) in enumerate(caches)]
    for cache in caches:
        cache.start()
    if first:
        scatter.finish(resid_ref, out_ref, (lambda: None, gather_n.stage_3, gather_n.stage_4, gather_n.stage_5))
        gather_n.finish()
        swap_1.land(1)
        for swap in (swap_0, swap_1):
            swap.drain(0)
            swap.drain(1)
        gather_a.drain()
        gather_n.drain()
    else:
        scatter.finish(resid_ref, out_ref, [lambda: None] * 4)
    gather_b.drain()
    gather_h.drain()
    for cache in caches:
        cache.wait()


def layer(resid, gamma, cos, sin, weights, n_wx, first):
    seq, d_model = resid.shape
    head_dim = cos.shape[1]
    n_unit = PLANE * PLANE
    col = d_model // N_COL
    any_spec, vmem_spec = pl.BlockSpec(memory_space=pl.ANY), pl.BlockSpec(memory_space=pltpu.VMEM)
    tile = d_model // n_wx
    unit_b = (n_wx * SUB + head_dim, tile)
    next_shape = (n_unit, d_model + 2 * tile, 2 * SUB)
    wa_shape = (n_unit, d_model, 2 * SUB) if first else next_shape
    wb_shape = (n_unit, unit_b[0] + (tile if first else 0), tile)
    piece = (seq, col)
    n_piece = 4 * N_COL
    dma = pltpu.SemaphoreType.DMA
    cache = (seq, head_dim) if first else (2, seq, head_dim)
    out_shape = [jax.ShapeDtypeStruct(shape, jnp.bfloat16) for shape in (resid.shape, cache, cache)]
    n_plane, n_swap, n_hop = dma((40,)), dma((21,)), dma((13,))
    if first:
        out_shape += [jax.ShapeDtypeStruct(shape, jnp.bfloat16) for shape in (next_shape, unit_b)]
        scratch = [n_plane, n_plane, n_swap, n_swap, n_swap, n_swap, n_plane, n_plane]
    else:
        scratch = [dma((2,)), dma((2,))]
    scratch += [
        pltpu.VMEM((n_wx, seq, d_model), jnp.bfloat16),
        pltpu.VMEM(wa_shape, jnp.bfloat16),
        pltpu.VMEM(wb_shape, jnp.bfloat16),
        pltpu.VMEM((n_wx, seq, n_unit * SUB + 2 * head_dim), jnp.bfloat16),
        pltpu.VMEM((n_wx, seq, 4 * head_dim), jnp.bfloat16),
        pltpu.VMEM((3, 2, 2, seq, head_dim), jnp.bfloat16),
        n_hop, n_hop, n_plane, n_plane, dma((4,)),
        pltpu.VMEM((N_COL,) + piece, jnp.float32),
        pltpu.VMEM((n_piece,) + piece, jnp.float32),
        pltpu.VMEM((n_piece,) + piece, jnp.float32),
        pltpu.VMEM((N_RING,) + piece, jnp.float32),
        dma((n_piece,)), dma((n_piece,)), dma((N_RING,)), dma((N_RING,)),
    ]
    return pl.pallas_call(
        functools.partial(layer_kernel, n_wx, first),
        out_shape=tuple(out_shape),
        in_specs=[vmem_spec] * 4 + [any_spec] * len(weights),
        out_specs=[vmem_spec] + [any_spec] * (len(out_shape) - 1),
        scratch_shapes=scratch,
        compiler_params=pltpu.CompilerParams(collective_id=int(first), has_side_effects=True, vmem_limit_bytes=VMEM_LIMIT),
        name='layer_0' if first else 'layer_1',
    )(resid, gamma, cos, sin, *weights)


def settle_kernel(*refs):
    n = len(refs) // 3
    srcs, dsts, held, sem = refs[:n], refs[n:2 * n], refs[2 * n:3 * n], refs[-1]
    loads = [pltpu.make_async_copy(src, mid, sem.at[num]) for num, (src, mid) in enumerate(zip(srcs, held))]
    stores = [pltpu.make_async_copy(mid, dst, sem.at[n + num]) for num, (mid, dst) in enumerate(zip(held, dsts))]
    for load in loads:
        load.start()
    for load, store in zip(loads, stores):
        load.wait()
        store.start()
    for store in stores:
        store.wait()


def settle(arrays):
    n = len(arrays)
    return pl.pallas_call(
        settle_kernel,
        out_shape=tuple(jax.ShapeDtypeStruct(a.shape, a.dtype) for a in arrays),
        in_specs=[pl.BlockSpec(memory_space=pl.ANY)] * n,
        out_specs=[pl.BlockSpec(memory_space=pl.ANY)] * n,
        scratch_shapes=[pltpu.VMEM(a.shape, a.dtype) for a in arrays] + [pltpu.SemaphoreType.DMA((2 * n,))],
        name='settle',
    )(*arrays)


def solution(mesh):
    batch_axes = ('dp', 'wy', 'wx')
    in_specs = (P(batch_axes), P(), P(None, 'wx', 'wy'), P(None, 'wx'), P(None, 'wx', None, 'wy'), P(None, 'wy', 'wx'), P(None, 'wy', 'wx'))
    out_specs = (P(batch_axes), P(None, batch_axes), P(None, batch_axes))
    n_wx = mesh.shape['wx']

    def device_step(x_tokens, gamma_ln, w_q, w_kv, w_gu, w_o, w_d):
        n_layers, d_loc = w_q.shape[:2]
        cos_tab, sin_tab = rope_tables(x_tokens.shape[1], w_kv.shape[-1])
        kv_half = lax.dynamic_index_in_dim(w_kv, lax.rem(lax.axis_index('wy'), 2), axis=2, keepdims=False)
        gu = jnp.transpose(w_gu.reshape(n_layers, d_loc, 2, n_wx, SUB), (0, 3, 1, 2, 4)).reshape(n_layers, n_wx, d_loc, 2 * SUB)
        resid, k_0, v_0, wa, unit_b = layer(x_tokens[0], gamma_ln, cos_tab, sin_tab, (gu, w_d, w_q, kv_half, w_o), n_wx, True)
        resid, k_all, v_all = settle(layer(resid, gamma_ln, cos_tab, sin_tab, (wa, unit_b, k_0, v_0), n_wx, False))
        return resid[None], k_all[:, None], v_all[:, None]

    return jax.shard_map(device_step, mesh=mesh, in_specs=in_specs, out_specs=out_specs, check_vma=False)
```
